8 devices in a mesh: dp: 1 (over z), ep: 8 (over y, x, core).
Axes of the slice: x: 2, y: 2, z: 1, core: 2. Of those that a mesh axis runs over, the one named last changes fastest.
Arguments:
- tokens: bfloat16 [8, 512, 2048], P(('dp', 'ep'))
- w_query: bfloat16 [2048, 32, 128], P('ep')
- w_key: bfloat16 [2048, 32, 128], P('ep')
- w_value: bfloat16 [2048, 32, 128], P('ep')
- w_out: bfloat16 [4096, 2048], P('ep')
- w_router: float32 [2048, 128], replicated
- w_one: bfloat16 [128, 2048, 768], P('ep')
- w_three: bfloat16 [128, 2048, 768], P('ep')
- w_two: bfloat16 [128, 768, 2048], P('ep')
- expert_ids: int32 [8, 512, 8], P(('dp', 'ep'))
Outputs:
- output: bfloat16 [8, 512, 2048], P(('dp', 'ep'))
All inputs are finite; a program needn't handle non-finite values.
Results may differ from the reference program's by a relative error of at most 0.00978195.
Values are sent between devices in bfloat16 or wider.
A program may use at most 1 GiB of HBM per device.

```python
import jax
import jax.numpy as jnp
import numpy as np
from jax import lax

D = 2048
HEADS = 32
HEAD = 128
EXPERTS = 128
TOP = 8
FF = 768
TOK_DEV = 512
SEQ = 512
GROUP = 8

TOKENS = TOK_DEV * GROUP
N_SEQ = TOKENS // SEQ
CAP = 2 * TOK_DEV * TOP // EXPERTS
WIDTH = HEADS * HEAD
EPS = 1e-6


def draw_routing(route_key):
    mean_load = TOK_DEV * TOP // EXPERTS
    ranks = np.arange(EXPERTS)
    loads = np.where(ranks < EXPERTS // 4, 2 * mean_load, np.where(ranks < EXPERTS // 2, mean_load, mean_load // 2))
    rank_of_pos = np.repeat(ranks, loads)
    order_key, device_key = jax.random.split(route_key)
    expert_order = jax.random.permutation(order_key, EXPERTS)
    grid = expert_order[rank_of_pos].reshape(TOP, TOK_DEV).T

    def one_device(dev_key):
        perm_key, shift_key = jax.random.split(dev_key)
        token_order = jax.random.permutation(perm_key, TOK_DEV)
        shift = jax.random.randint(shift_key, (TOK_DEV, 1), 0, TOP)
        columns = (jnp.arange(TOP)[None, :] + shift) % TOP
        return jnp.take_along_axis(grid[token_order], columns, axis=1)

    routes = jax.vmap(one_device)(jax.random.split(device_key, GROUP))
    return routes.reshape(N_SEQ, SEQ, TOP).astype(jnp.int32)


def setup_inputs(seed: int = 0, part: int = 0) -> dict:
    root_key = jax.random.key(seed)
    part_keys = jax.random.split(jax.random.fold_in(root_key, part), 3)
    weight_keys = jax.random.split(root_key, 8)

    def gaussian(index, shape, scale):
        return scale * jax.random.normal(weight_keys[index], shape, jnp.float32)

    seq_base = jax.random.normal(part_keys[0], (N_SEQ, 1, D), jnp.float32)
    noise = jax.random.normal(part_keys[1], (N_SEQ, SEQ, D), jnp.float32)
    return {
        'tokens': (0.6 * seq_base + 0.8 * noise).astype(jnp.bfloat16),
        'w_query': gaussian(0, (D, HEADS, HEAD), 1.5 * D ** -0.5).astype(jnp.bfloat16),
        'w_key': gaussian(1, (D, HEADS, HEAD), 1.5 * D ** -0.5).astype(jnp.bfloat16),
        'w_value': gaussian(2, (D, HEADS, HEAD), D ** -0.5).astype(jnp.bfloat16),
        'w_out': gaussian(3, (WIDTH, D), WIDTH ** -0.5).astype(jnp.bfloat16),
        'w_router': gaussian(4, (D, EXPERTS), D ** -0.5),
        'w_one': gaussian(5, (EXPERTS, D, FF), D ** -0.5).astype(jnp.bfloat16),
        'w_three': gaussian(6, (EXPERTS, D, FF), D ** -0.5).astype(jnp.bfloat16),
        'w_two': gaussian(7, (EXPERTS, FF, D), 2.0 * FF ** -0.5).astype(jnp.bfloat16),
        'expert_ids': draw_routing(part_keys[2]),
    }


def rms_norm(vals):
    wide = vals.astype(jnp.float32)
    return wide * lax.rsqrt(jnp.mean(wide * wide, axis=-1, keepdims=True) + EPS)


def reference(tokens, w_query, w_key, w_value, w_out, w_router, w_one, w_three, w_two, expert_ids):
    flat_query = w_query.reshape(D, WIDTH)
    flat_key = w_key.reshape(D, WIDTH)
    flat_value = w_value.reshape(D, WIDTH)
    causal = jnp.arange(SEQ)[:, None] >= jnp.arange(SEQ)[None, :]

    def one_sequence(seq_tokens):
        normed = rms_norm(seq_tokens).astype(jnp.bfloat16)
        query = jnp.dot(normed, flat_query, preferred_element_type=jnp.float32).astype(jnp.bfloat16)
        keys = jnp.dot(normed, flat_key, preferred_element_type=jnp.float32).astype(jnp.bfloat16)
        values = jnp.dot(normed, flat_value, preferred_element_type=jnp.float32).astype(jnp.bfloat16)
        query = query.astype(jnp.float32).reshape(SEQ, HEADS, HEAD)
        keys = keys.astype(jnp.float32).reshape(SEQ, HEADS, HEAD)
        values = values.astype(jnp.float32).reshape(SEQ, HEADS, HEAD)
        scores = jnp.einsum('qhk,shk->hqs', query, keys) * HEAD ** -0.5
        scores = jnp.where(causal, scores, -jnp.inf)
        attn_weights = jax.nn.softmax(scores, axis=-1).astype(jnp.bfloat16).astype(jnp.float32)
        context = jnp.einsum('hqs,shk->qhk', attn_weights, values).astype(jnp.bfloat16)
        attn_out = jnp.dot(context.reshape(SEQ, WIDTH), w_out, preferred_element_type=jnp.float32)
        return (seq_tokens.astype(jnp.float32) + attn_out).astype(jnp.bfloat16)

    hidden = lax.map(one_sequence, tokens).reshape(TOKENS, D)
    normed = rms_norm(hidden)
    logits = jnp.dot(normed, w_router, preferred_element_type=jnp.float32)
    ids_flat = expert_ids.reshape(TOKENS, TOP)
    gates = jax.nn.softmax(jnp.take_along_axis(logits, ids_flat, axis=1), axis=-1)
    padded = jnp.concatenate([normed.astype(jnp.bfloat16), jnp.zeros((1, D), jnp.bfloat16)], axis=0)
    limit = GROUP * CAP

    def one_expert(total_mix, expert_pack):
        expert, first_w, third_w, second_w = expert_pack
        match = ids_flat == expert
        weight = jnp.sum(jnp.where(match, gates, 0.0), axis=1)
        rows = jnp.nonzero(jnp.any(match, axis=1), size=limit, fill_value=TOKENS)[0]
        picked = padded[rows]
        first = jnp.dot(picked, first_w, preferred_element_type=jnp.float32)
        third = jnp.dot(picked, third_w, preferred_element_type=jnp.float32)
        activated = (jax.nn.silu(first) * third).astype(jnp.bfloat16)
        result = jnp.dot(activated, second_w, preferred_element_type=jnp.float32).astype(jnp.bfloat16)
        scale = jnp.concatenate([weight, jnp.zeros((1,), jnp.float32)])[rows]
        total_mix = total_mix.at[rows].add(scale[:, None] * result.astype(jnp.float32), mode='drop')
        return total_mix, None

    total_mix, _ = lax.scan(one_expert, jnp.zeros((TOKENS, D), jnp.float32), (jnp.arange(EXPERTS), w_one, w_three, w_two))
    layer_out = (hidden.astype(jnp.float32) + total_mix).astype(jnp.bfloat16)
    return layer_out.reshape(N_SEQ, SEQ, D)
```

```python
import jax
import jax.numpy as jnp
from jax import lax
from jax.sharding import PartitionSpec as P

EPS = 1e-6


def rms_norm(vals):
    wide = vals.astype(jnp.float32)
    return wide * lax.rsqrt(jnp.mean(wide * wide, axis=-1, keepdims=True) + EPS)


def attention_layer(tokens, w_query, w_key, w_value, w_out):
    seq_count = tokens.shape[0]
    seq_len = tokens.shape[1]
    head_dim = w_query.shape[2]
    normed = rms_norm(tokens).astype(jnp.bfloat16)
    query = jnp.einsum('bsd,dhk->bshk', normed, w_query, preferred_element_type=jnp.float32).astype(jnp.bfloat16)
    keys = jnp.einsum('bsd,dhk->bshk', normed, w_key, preferred_element_type=jnp.float32).astype(jnp.bfloat16)
    values = jnp.einsum('bsd,dhk->bshk', normed, w_value, preferred_element_type=jnp.float32).astype(jnp.bfloat16)
    scores = jnp.einsum('bqhk,bshk->bhqs', query, keys, preferred_element_type=jnp.float32) * head_dim ** -0.5
    causal = lax.broadcasted_iota(jnp.int32, (seq_len, seq_len), 0) >= lax.broadcasted_iota(jnp.int32, (seq_len, seq_len), 1)
    attn_weights = jax.nn.softmax(jnp.where(causal, scores, -jnp.inf), axis=-1).astype(jnp.bfloat16)
    context = jnp.einsum('bhqs,bshk->bqhk', attn_weights, values, preferred_element_type=jnp.float32).astype(jnp.bfloat16)
    attn_out = jnp.einsum('crd,de->cre', context.reshape(seq_count, seq_len, -1), w_out, preferred_element_type=jnp.float32)
    return (tokens.astype(jnp.float32) + attn_out).astype(jnp.bfloat16)


def router_gates(hidden, w_router, ids):
    normed = rms_norm(hidden)
    logits = jnp.einsum('td,de->te', normed, w_router, precision=lax.Precision.HIGHEST, preferred_element_type=jnp.float32)
    hit = ids[:, :, None] == jnp.arange(w_router.shape[1], dtype=jnp.int32)
    chosen = jnp.sum(jnp.where(hit, logits[:, None, :], 0.0), axis=2)
    return normed.astype(jnp.bfloat16), jax.nn.softmax(chosen, axis=-1)


def local_tables(all_ids, all_gates, first, count):
    wanted = first + jnp.arange(count, dtype=jnp.int32)
    hit = all_ids[:, :, :, None] == wanted
    member = jnp.sum(hit.astype(jnp.int32), axis=2)
    slot = jnp.cumsum(member, axis=1) - member
    gate = jnp.sum(jnp.where(hit, all_gates[:, :, :, None], 0.0), axis=2)
    return jnp.where(member > 0, slot, -1), gate


def expert_ffn(rows, w_one, w_three, w_two):
    first = jnp.einsum('end,edf->enf', rows, w_one, preferred_element_type=jnp.float32)
    third = jnp.einsum('end,edf->enf', rows, w_three, preferred_element_type=jnp.float32)
    activated = (jax.nn.silu(first) * third).astype(jnp.bfloat16)
    return jnp.einsum('enf,efd->end', activated, w_two, preferred_element_type=jnp.float32).astype(jnp.bfloat16)


def solution(mesh):
    tok_spec = P(('dp', 'ep'))
    row_spec = P('ep')

    def local_layer(tokens, w_query, w_key, w_value, w_out, w_router, w_one, w_three, w_two, expert_ids):
        seq_count, seq_len, model_dim = tokens.shape
        choices = expert_ids.shape[2]
        experts = w_router.shape[1]
        local_experts = w_one.shape[0]
        tok_count = seq_count * seq_len
        cap_rows = 2 * tok_count * choices // experts
        ids = expert_ids.reshape(tok_count, choices)
        all_ids = lax.all_gather(ids, 'ep', axis=0)
        full_query = lax.all_gather(w_query, 'ep', axis=0, tiled=True)
        full_key = lax.all_gather(w_key, 'ep', axis=0, tiled=True)
        full_value = lax.all_gather(w_value, 'ep', axis=0, tiled=True)
        full_out = lax.all_gather(w_out, 'ep', axis=0, tiled=True)
        hidden = attention_layer(tokens, full_query, full_key, full_value, full_out).reshape(tok_count, model_dim)
        normed, gates = router_gates(hidden, w_router, ids)
        all_normed = lax.all_gather(normed, 'ep', axis=0)
        all_gates = lax.all_gather(gates, 'ep', axis=0)
        first = lax.axis_index('ep') * local_experts
        slot, gate = local_tables(all_ids, all_gates, first, local_experts)
        place = slot[:, :, :, None] == jnp.arange(cap_rows, dtype=jnp.int32)
        rows = jnp.einsum('stec,std->secd', place.astype(jnp.bfloat16), all_normed, preferred_element_type=jnp.float32).astype(jnp.bfloat16)
        packed = rows.transpose(1, 0, 2, 3).reshape(local_experts, -1, model_dim)
        done = expert_ffn(packed, w_one, w_three, w_two)
        done = done.reshape(local_experts, -1, cap_rows, model_dim).transpose(1, 0, 2, 3)
        rest = jnp.where(place, gate[:, :, :, None], 0.0)
        mixed = 0.0
        for _ in range(3):
            part = lax.reduce_precision(rest, 8, 7)
            rest = rest - part
            mixed = mixed + jnp.einsum('stec,secd->std', part.astype(jnp.bfloat16), done, preferred_element_type=jnp.float32)
        total = lax.psum_scatter(mixed, 'ep', scatter_dimension=0, tiled=False)
        layer_out = (hidden.astype(jnp.float32) + total).astype(jnp.bfloat16)
        return layer_out.reshape(seq_count, seq_len, model_dim)

    return jax.shard_map(local_layer, mesh=mesh, in_specs=(tok_spec, row_spec, row_spec, row_spec, row_spec, P(), row_spec, row_spec, row_spec, tok_spec), out_specs=tok_spec, check_vma=False)
```

```python
import functools

import jax
import jax.numpy as jnp
from jax import lax
from jax.experimental import pallas as pl
from jax.experimental.pallas import tpu as pltpu
from jax.sharding import PartitionSpec as P

EPS = 1e-6
CAP = 64
UNIT = 16
VMEM_MAX = 67043328


def rms_norm(vals):
    wide = vals.astype(jnp.float32)
    return wide * lax.rsqrt(jnp.mean(wide * wide, axis=-1, keepdims=True) + EPS)


def attention_layer(tokens, w_query, w_key, w_value, w_out):
    seq_count = tokens.shape[0]
    seq_len = tokens.shape[1]
    head_dim = w_query.shape[2]
    normed = rms_norm(tokens).astype(jnp.bfloat16)
    query = jnp.einsum('bsd,dhk->bshk', normed, w_query, preferred_element_type=jnp.float32).astype(jnp.bfloat16)
    keys = jnp.einsum('bsd,dhk->bshk', normed, w_key, preferred_element_type=jnp.float32).astype(jnp.bfloat16)
    values = jnp.einsum('bsd,dhk->bshk', normed, w_value, preferred_element_type=jnp.float32).astype(jnp.bfloat16)
    scores = jnp.einsum('bqhk,bshk->bhqs', query, keys, preferred_element_type=jnp.float32) * head_dim ** -0.5
    causal = lax.broadcasted_iota(jnp.int32, (seq_len, seq_len), 0) >= lax.broadcasted_iota(jnp.int32, (seq_len, seq_len), 1)
    attn_weights = jax.nn.softmax(jnp.where(causal, scores, -jnp.inf), axis=-1).astype(jnp.bfloat16)
    context = jnp.einsum('bhqs,bshk->bqhk', attn_weights, values, preferred_element_type=jnp.float32).astype(jnp.bfloat16)
    attn_out = jnp.einsum('crd,de->cre', context.reshape(seq_count, seq_len, -1), w_out, preferred_element_type=jnp.float32)
    return (tokens.astype(jnp.float32) + attn_out).astype(jnp.bfloat16)


def router_gates(hidden, w_router, ids_t):
    normed = rms_norm(hidden)
    logits = jnp.einsum('td,de->et', normed, w_router, precision=lax.Precision.HIGHEST, preferred_element_type=jnp.float32)
    hit = ids_t[:, None, :] == jnp.arange(w_router.shape[1], dtype=jnp.int32)[None, :, None]
    chosen = jnp.sum(jnp.where(hit, logits[None], 0.0), axis=1)
    return normed.astype(jnp.bfloat16), jax.nn.softmax(chosen, axis=0)


def neighbours():
    me = lax.axis_index('ep')
    core, chip = lax.rem(me, 2), me // 2
    side, up = lax.rem(chip, 2), chip // 2
    return me, core, chip, 1 - side + 2 * up, side + 2 * (1 - up), 3 - chip


def greet(devices):
    barrier = pltpu.get_barrier_semaphore()
    for device in devices:
        pl.semaphore_signal(barrier, inc=1, device_id={'ep': device}, device_id_type=pl.DeviceIdType.MESH)
    pl.semaphore_wait(barrier, len(devices))


def remote(src, dst, send_sem, recv_sem, device):
    return pltpu.make_async_remote_copy(src_ref=src, dst_ref=dst, send_sem=send_sem, recv_sem=recv_sem, device_id={'ep': device}, device_id_type=pl.DeviceIdType.MESH)


def spread_kernel(u_hbm, g_hbm, slot_ref, x_hbm, gall_hbm, ubuf, hbuf, xbuf, own_sem, gown_sem, out_sem, x_send, y_send, d_send, recv, g_send, g_recv):
    me, core, chip, xn, yn, dg = neighbours()
    mate = me + 1 - 2 * core
    tok = ubuf.shape[1]
    part = tok // 4
    local_experts = slot_ref.shape[1]
    x_dev, y_dev, dg_dev = xn * 2 + core, yn * 2 + core, dg * 2 + core
    others = (x_dev, y_dev, mate, dg_dev, xn * 2 + 1 - core, yn * 2 + 1 - core, dg * 2 + 1 - core)
    greet(others)

    def rows(piece):
        return pl.ds(piece * part, part)

    def landed(source, piece):
        remote(ubuf.at[source, rows(piece)], ubuf.at[source, rows(piece)], d_send.at[0, 0], recv.at[source, piece], mate).wait_recv()

    def pass_on(order, source, piece):
        return remote(ubuf.at[source, rows(piece)], ubuf.at[source, rows(piece)], d_send.at[order, piece], recv.at[source, piece], mate)

    def across_x(slot, source, piece, src):
        return remote(src, ubuf.at[source, rows(piece)], x_send.at[slot], recv.at[source, piece], x_dev)

    def across_y(slot, source, piece, src):
        return remote(src, ubuf.at[source, rows(piece)], y_send.at[slot], recv.at[source, piece], y_dev)

    own = pltpu.make_async_copy(u_hbm, ubuf.at[me], own_sem)
    own.start()
    gown = pltpu.make_async_copy(g_hbm, gall_hbm.at[me], gown_sem)
    gown.start()
    for slot in range(4):
        across_x(slot, me, slot, u_hbm.at[rows(slot)]).start()
        across_y(slot, me, (slot + 2) % 4, u_hbm.at[rows((slot + 2) % 4)]).start()
    for piece in range(4):
        remote(u_hbm.at[rows(piece)], ubuf.at[me, rows(piece)], d_send.at[0, piece], recv.at[me, piece], mate).start()
    for slot, device in enumerate(others):
        remote(g_hbm, gall_hbm.at[me], g_send.at[slot], g_recv.at[me], device).start()
    own.wait()

    def out_copy(order, source):
        return pltpu.make_async_copy(xbuf.at[lax.rem(order, 2)], x_hbm.at[:, source], out_sem.at[lax.rem(order, 2)])

    def step(order, carry):
        kind = order // 2
        base = jnp.where(kind == 0, chip, jnp.where(kind == 1, xn, jnp.where(kind == 2, yn, dg)))
        odd = lax.rem(order, 2)
        source = base * 2 + core + odd * (1 - 2 * core)

        @pl.when(order == 2)
        def _():
            for piece in (0, 1):
                landed(x_dev, piece)
                across_y(4 + piece, x_dev, piece, ubuf.at[x_dev, rows(piece)]).start()
                pass_on(1, x_dev, piece).start()
                landed(y_dev, piece + 2)
                across_x(4 + piece, y_dev, piece + 2, ubuf.at[y_dev, rows(piece + 2)]).start()
                pass_on(2, y_dev, piece + 2).start()
            for piece in (0, 1):
                landed(x_dev, piece + 2)
                pass_on(1, x_dev, piece + 2).start()
                landed(y_dev, piece)
                pass_on(2, y_dev, piece).start()

        @pl.when(order == 6)
        def _():
            for piece in (0, 2, 1, 3):
                landed(dg_dev, piece)
                pass_on(3, dg_dev, piece).start()

        @pl.when(odd == 1)
        def _():
            for piece in range(4):
                landed(source, piece)

        @pl.when(order >= 2)
        def _():
            out_copy(order, source).wait()

        spot = lax.broadcasted_iota(jnp.int32, (CAP, tok), 0)
        for expert in range(local_experts):
            hit = slot_ref[source, expert:expert + 1, :] == spot
            hbuf[expert * CAP:(expert + 1) * CAP, :] = jnp.where(hit, 1.0, 0.0).astype(jnp.bfloat16)
        width = 256

        def tile(n, c):
            cols = pl.ds(pl.multiple_of(n * width, width), width)
            picked = jnp.dot(hbuf[...], ubuf[source, :, cols], preferred_element_type=jnp.float32)
            xbuf[odd, :, :, cols] = picked.astype(jnp.bfloat16).reshape(local_experts, CAP, width)
            return c

        lax.fori_loop(0, ubuf.shape[2] // width, tile, 0)
        out_copy(order, source).start()
        return carry

    lax.fori_loop(0, 8, step, 0)
    out_copy(0, me).wait()
    out_copy(1, me).wait()
    gown.wait()
    for slot in range(4):
        across_x(slot, me, slot, u_hbm.at[rows(slot)]).wait_send()
        across_y(slot, me, slot, u_hbm.at[rows(slot)]).wait_send()
    for piece in (0, 1):
        across_y(4 + piece, x_dev, piece, ubuf.at[x_dev, rows(piece)]).wait_send()
        across_x(4 + piece, y_dev, piece + 2, ubuf.at[y_dev, rows(piece + 2)]).wait_send()
    for order, source in enumerate((me, x_dev, y_dev, dg_dev)):
        for piece in range(4):
            pass_on(order, source, piece).wait_send()
    for slot, device in enumerate(others):
        remote(g_hbm, gall_hbm.at[me], g_send.at[slot], g_recv.at[me], device).wait_send()
        remote(g_hbm, gall_hbm.at[device], g_send.at[slot], g_recv.at[device], device).wait_recv()


def spread(u, gates, slots):
    devices, local_experts, tok = slots.shape
    dim = u.shape[1]
    return pl.pallas_call(
        spread_kernel,
        out_shape=(jax.ShapeDtypeStruct((local_experts, devices, CAP, dim), jnp.bfloat16), jax.ShapeDtypeStruct((devices,) + gates.shape, jnp.float32)),
        in_specs=[pl.BlockSpec(memory_space=pl.ANY), pl.BlockSpec(memory_space=pl.ANY), pl.BlockSpec(memory_space=pltpu.VMEM)],
        out_specs=(pl.BlockSpec(memory_space=pl.ANY), pl.BlockSpec(memory_space=pl.ANY)),
        scratch_shapes=[
            pltpu.VMEM((devices, tok, dim), jnp.bfloat16),
            pltpu.VMEM((local_experts * CAP, tok), jnp.bfloat16),
            pltpu.VMEM((2, local_experts, CAP, dim), jnp.bfloat16),
            pltpu.SemaphoreType.DMA, pltpu.SemaphoreType.DMA, pltpu.SemaphoreType.DMA((2,)),
            pltpu.SemaphoreType.DMA((6,)), pltpu.SemaphoreType.DMA((6,)), pltpu.SemaphoreType.DMA((4, 4)),
            pltpu.SemaphoreType.DMA((devices, 4)), pltpu.SemaphoreType.DMA((7,)), pltpu.SemaphoreType.DMA((devices,)),
        ],
        compiler_params=pltpu.CompilerParams(collective_id=1, has_side_effects=True, vmem_limit_bytes=VMEM_MAX),
        name='spread_rows',
    )(u, gates, slots)


def ffn_kernel(units_ref, x_ref, w1_ref, w3_ref, w2_ref, o_ref, packed, middle, done):
    expert = pl.program_id(0)
    devices = x_ref.shape[1]
    tile = 128
    total = 0
    for source in range(devices):
        count = units_ref[expert * devices + source]

        def pack(i, c, source=source, total=total):
            packed[pl.ds(pl.multiple_of((total + i) * UNIT, UNIT), UNIT), :] = x_ref[0, source, pl.ds(pl.multiple_of(i * UNIT, UNIT), UNIT), :]
            return c

        lax.fori_loop(0, count, pack, 0)
        total = total + count

    def run(t, c):
        rows = pl.ds(pl.multiple_of(t * tile, tile), tile)
        for n in range(w1_ref.shape[2] // 256):
            cols = slice(n * 256, (n + 1) * 256)
            first = jnp.dot(packed[rows, :], w1_ref[0, :, cols], preferred_element_type=jnp.float32)
            third = jnp.dot(packed[rows, :], w3_ref[0, :, cols], preferred_element_type=jnp.float32)
            middle[:, cols] = (first * jax.nn.sigmoid(first) * third).astype(jnp.bfloat16)
        for n in range(w2_ref.shape[2] // 512):
            cols = slice(n * 512, (n + 1) * 512)
            done[rows, cols] = jnp.dot(middle[...], w2_ref[0, :, cols], preferred_element_type=jnp.float32).astype(jnp.bfloat16)
        return c

    lax.fori_loop(0, (total * UNIT + tile - 1) // tile, run, 0)
    total = 0
    for source in range(devices):
        count = units_ref[expert * devices + source]

        def unpack(i, c, source=source, total=total):
            o_ref[0, source, pl.ds(pl.multiple_of(i * UNIT, UNIT), UNIT), :] = done[pl.ds(pl.multiple_of((total + i) * UNIT, UNIT), UNIT), :]
            return c

        def clear(i, c, source=source):
            o_ref[0, source, pl.ds(pl.multiple_of(i * UNIT, UNIT), UNIT), :] = jnp.zeros((UNIT, o_ref.shape[3]), jnp.bfloat16)
            return c

        lax.fori_loop(0, count, unpack, 0)
        lax.fori_loop(count, CAP // UNIT, clear, 0)
        total = total + count


def expert_ffn(units, x, w_one, w_three, w_two):
    experts, devices, _, dim = x.shape
    mid = w_one.shape[2]
    block = lambda *shape: pl.BlockSpec((1,) + shape, lambda e, units: (e,) + (0,) * len(shape))
    return pl.pallas_call(
        ffn_kernel,
        out_shape=jax.ShapeDtypeStruct(x.shape, jnp.bfloat16),
        grid_spec=pltpu.PrefetchScalarGridSpec(
            num_scalar_prefetch=1,
            grid=(experts,),
            in_specs=[block(devices, CAP, dim), block(dim, mid), block(dim, mid), block(mid, dim)],
            out_specs=block(devices, CAP, dim),
            scratch_shapes=[pltpu.VMEM((devices * CAP, dim), jnp.bfloat16), pltpu.VMEM((128, mid), jnp.bfloat16), pltpu.VMEM((devices * CAP, dim), jnp.bfloat16)],
        ),
        compiler_params=pltpu.CompilerParams(dimension_semantics=('arbitrary',), vmem_limit_bytes=VMEM_MAX),
        name='expert_mlp',
    )(units, x, w_one, w_three, w_two)


def combine_kernel(o_hbm, tab_hbm, h_hbm, y_ref, own, mate_rows, tab, gate3, p_one, r_one, p_two, r_two, p_last, r_last, own_sem, tab_sem, h_sem, mate_send, mate_recv, one_send, one_recv, two_send, two_recv, last_send, last_recv):
    me, core, chip, xn, yn, dg = neighbours()
    mate = me + 1 - 2 * core
    near = xn + core * (yn - xn)
    far = yn + core * (xn - yn)
    near_dev, far_dev = near * 2 + core, far * 2 + core
    half = own.shape[3]
    rows_n = p_one.shape[1]
    experts = own.shape[1]
    greet((near_dev, far_dev, mate))
    my_cols = pl.ds(pl.multiple_of(core * half, half), half)
    mate_cols = pl.ds(pl.multiple_of((1 - core) * half, half), half)

    def dest(i, first, second):
        pair = i // 2
        base = jnp.where(pair == 0, dg, jnp.where(pair == 1, first, jnp.where(pair == 2, second, chip)))
        return base

    def my_dest(i):
        odd = lax.rem(i, 2)
        return dest(i, near, far) * 2 + jnp.where(i < 6, odd, 1 - core + odd * (2 * core - 1))

    def mate_dest(i):
        odd = lax.rem(i, 2)
        return dest(i, far, near) * 2 + jnp.where(i < 6, odd, core + odd * (1 - 2 * core))

    def to_mate(i):
        return remote(o_hbm.at[:, mate_dest(i), :, mate_cols], mate_rows.at[i], mate_send.at[i], mate_recv.at[i], mate)

    def own_copy(i):
        return pltpu.make_async_copy(o_hbm.at[:, my_dest(i), :, my_cols], own.at[lax.rem(i, 2)], own_sem.at[lax.rem(i, 2)])

    def tab_copy(i):
        return pltpu.make_async_copy(tab_hbm.at[my_dest(i)], tab.at[lax.rem(i, 2)], tab_sem.at[lax.rem(i, 2)])

    def one_copy(n):
        return remote(p_one.at[n], r_one.at[n], one_send.at[n], one_recv.at[n], near_dev)

    def two_copy(n):
        return remote(p_two.at[n], r_two.at[n], two_send.at[n], two_recv.at[n], far_dev)

    def last_copy(n):
        return remote(p_last.at[n], r_last.at[n], last_send.at[n], last_recv.at[n], mate)

    own_copy(0).start()
    tab_copy(0).start()
    for i in range(8):
        to_mate(i).start()
    residual = pltpu.make_async_copy(h_hbm, y_ref, h_sem)
    residual.start()

    def open_dest(i):
        own_copy(i).wait()
        tab_copy(i).wait()
        to_mate(i).wait_recv()

        @pl.when(i < 7)
        def _():
            own_copy(i + 1).start()
            tab_copy(i + 1).start()

    def weights(i, part):
        slot = lax.rem(i, 2)
        cols = pl.ds(pl.multiple_of(part * rows_n, rows_n), rows_n)
        spot = lax.broadcasted_iota(jnp.int32, (2 * CAP, rows_n), 0)
        low = spot < CAP
        place = (spot - jnp.where(low, 0, CAP)).astype(jnp.float32)
        for pair in range(experts):
            at = tab[slot, 2 * pair:2 * pair + 2, cols]
            gate = tab[slot, 2 * experts + 2 * pair:2 * experts + 2 * pair + 2, cols]
            hit = jnp.where(low, at[0:1], at[1:2]) == place
            value = jnp.where(hit, jnp.where(low, gate[0:1], gate[1:2]), 0.0).T
            top = value.astype(jnp.bfloat16)
            rest = value - top.astype(jnp.float32)
            mid = rest.astype(jnp.bfloat16)
            low_part = (rest - mid.astype(jnp.float32)).astype(jnp.bfloat16)
            where = slice(pair * 2 * CAP, (pair + 1) * 2 * CAP)
            gate3[0:rows_n, where] = top
            gate3[rows_n:2 * rows_n, where] = mid
            gate3[2 * rows_n:3 * rows_n, where] = low_part

    def products(i, part, sink):
        weights(i, part)
        slot = lax.rem(i, 2)
        depth = experts * CAP
        width = 256

        def tile(n, c):
            cols = pl.ds(pl.multiple_of(n * width, width), width)
            mine = own[slot, :, :, cols].reshape(depth, width)
            other = mate_rows[i, :, :, cols].reshape(depth, width)
            out = jnp.dot(gate3[:, :depth], mine, preferred_element_type=jnp.float32) + jnp.dot(gate3[:, depth:], other, preferred_element_type=jnp.float32)
            sink(cols, out[0:rows_n] + out[rows_n:2 * rows_n] + out[2 * rows_n:3 * rows_n])
            return c

        lax.fori_loop(0, half // width, tile, 0)

    def phase_one(step, c):
        i, part = step // 2, lax.rem(step, 2)

        @pl.when(part == 0)
        def _():
            open_dest(i)

        def sink(cols, value):
            p_one[step, :, cols] = value

        products(i, part, sink)
        one_copy(step).start()
        return c

    lax.fori_loop(0, 8, phase_one, 0)

    def phase_two(step, c):
        i, part = 4 + step // 2, lax.rem(step, 2)

        @pl.when(part == 0)
        def _():
            open_dest(i)

        def sink(cols, value):
            p_two[step, :, cols] = value

        products(i, part, sink)
        one_copy(step).wait_recv()
        p_two[step] = p_two[step] + r_one[step]
        two_copy(step).start()
        return c

    lax.fori_loop(0, 4, phase_two, 0)
    residual.wait()

    def phase_three(step, c):
        i, part = 6 + step // 2, lax.rem(step, 2)

        @pl.when(part == 0)
        def _():
            open_dest(i)

        def sink(cols, value):
            p_last[step, :, cols] = value

        products(i, part, sink)
        target = jnp.where(step < 2, 1 - core, core)
        n = target * 2 + part
        one_copy(4 + n).wait_recv()
        two_copy(n).wait_recv()
        p_last[step] = p_last[step] + (r_one[4 + n] + r_two[n])

        @pl.when(step < 2)
        def _():
            last_copy(step).start()

        @pl.when(step >= 2)
        def _():
            rows = pl.ds(pl.multiple_of(part * rows_n, rows_n), rows_n)
            y_ref[rows, my_cols] = (y_ref[rows, my_cols].astype(jnp.float32) + p_last[step]).astype(jnp.bfloat16)

        return c

    lax.fori_loop(0, 4, phase_three, 0)
    for n in range(2):
        rows = pl.ds(n * rows_n, rows_n)
        last_copy(n).wait_recv()
        y_ref[rows, mate_cols] = (y_ref[rows, mate_cols].astype(jnp.float32) + r_last[n]).astype(jnp.bfloat16)
    for n in range(8):
        to_mate(n).wait_send()
        one_copy(n).wait_send()
    for n in range(4):
        two_copy(n).wait_send()
    for n in range(2):
        last_copy(n).wait_send()


def combine(done, tab, hidden):
    experts, devices, _, dim = done.shape
    tok = hidden.shape[0]
    half, part = dim // 2, tok // 2
    dma = pltpu.SemaphoreType.DMA
    return pl.pallas_call(
        combine_kernel,
        out_shape=jax.ShapeDtypeStruct((tok, dim), jnp.bfloat16),
        in_specs=[pl.BlockSpec(memory_space=pl.ANY)] * 3,
        out_specs=pl.BlockSpec(memory_space=pltpu.VMEM),
        scratch_shapes=[
            pltpu.VMEM((2, experts, CAP, half), jnp.bfloat16),
            pltpu.VMEM((devices, experts, CAP, half), jnp.bfloat16),
            pltpu.VMEM((2,) + tab.shape[1:], jnp.float32),
            pltpu.VMEM((3 * part, 2 * experts * CAP), jnp.bfloat16),
            pltpu.VMEM((8, part, half), jnp.float32),
            pltpu.VMEM((8, part, half), jnp.float32),
            pltpu.VMEM((4, part, half), jnp.float32),
            pltpu.VMEM((4, part, half), jnp.float32),
            pltpu.VMEM((4, part, half), jnp.float32),
            pltpu.VMEM((2, part, half), jnp.float32),
            dma((2,)), dma((2,)), dma, dma((8,)), dma((8,)), dma((8,)), dma((8,)), dma((4,)), dma((4,)), dma((2,)), dma((2,)),
        ],
        compiler_params=pltpu.CompilerParams(collective_id=2, has_side_effects=True, vmem_limit_bytes=VMEM_MAX),
        name='combine_rows',
    )(done, tab, hidden)


def solution(mesh):
    tok_spec = P(('dp', 'ep'))
    row_spec = P('ep')

    def local_layer(tokens, w_query, w_key, w_value, w_out, w_router, w_one, w_three, w_two, expert_ids):
        seq_count, seq_len, model_dim = tokens.shape
        choices = expert_ids.shape[2]
        local_experts = w_one.shape[0]
        tok_count = seq_count * seq_len
        ids_t = expert_ids.reshape(tok_count, choices).T
        all_ids = lax.all_gather(ids_t, 'ep', axis=0)
        me = lax.axis_index('ep')
        core = lax.rem(me, 2)
        local = jnp.arange(local_experts, dtype=jnp.int32)
        wanted = jnp.concatenate([me * local_experts + local, (me + 1 - 2 * core) * local_experts + local])
        hit = all_ids[:, :, None, :] == wanted[None, None, :, None]
        member = jnp.sum(hit.astype(jnp.int32), axis=1)
        before = jnp.arange(tok_count)[:, None] < jnp.arange(tok_count)[None, :]
        slot = jnp.einsum('set,tu->seu', member.astype(jnp.bfloat16), before.astype(jnp.bfloat16), preferred_element_type=jnp.float32)
        slot = jnp.where(member > 0, slot, -1.0)
        slots = slot[:, :local_experts].astype(jnp.int32)
        units = ((jnp.sum(member[:, :local_experts], axis=2) + UNIT - 1) // UNIT).T.reshape(-1)

        full_query = lax.all_gather(w_query, 'ep', axis=0, tiled=True)
        full_key = lax.all_gather(w_key, 'ep', axis=0, tiled=True)
        full_value = lax.all_gather(w_value, 'ep', axis=0, tiled=True)
        full_out = lax.all_gather(w_out, 'ep', axis=0, tiled=True)
        hidden = attention_layer(tokens, full_query, full_key, full_value, full_out).reshape(tok_count, model_dim)
        normed, gates = router_gates(hidden, w_router, ids_t)
        x, all_gates = spread(normed, gates, slots)
        gate = jnp.sum(jnp.where(hit, all_gates[:, :, None, :], 0.0), axis=1)
        tab = jnp.concatenate([slot, gate], axis=1)
        done = expert_ffn(units, x, w_one, w_three, w_two)
        layer_out = combine(done, tab, hidden)
        return layer_out.reshape(seq_count, seq_len, model_dim)

    return jax.shard_map(local_layer, mesh=mesh, in_specs=(tok_spec, row_spec, row_spec, row_spec, row_spec, P(), row_spec, row_spec, row_spec, tok_spec), out_specs=tok_spec, check_vma=False)
```

```python
import functools

import jax
import jax.numpy as jnp
from jax import lax
from jax.experimental import pallas as pl
from jax.experimental.pallas import tpu as pltpu
from jax.sharding import PartitionSpec as P

EPS = 1e-6
CAP = 64
UNIT = 16
VMEM_MAX = 67043328


def rms_norm(vals):
    wide = vals.astype(jnp.float32)
    return wide * lax.rsqrt(jnp.mean(wide * wide, axis=-1, keepdims=True) + EPS)


def router_gates(hidden, w_router, ids_t):
    normed = rms_norm(hidden)
    logits = jnp.einsum('td,de->et', normed, w_router, precision=lax.Precision.HIGHEST, preferred_element_type=jnp.float32)
    hit = ids_t[:, None, :] == jnp.arange(w_router.shape[1], dtype=jnp.int32)[None, :, None]
    chosen = jnp.sum(jnp.where(hit, logits[None], 0.0), axis=1)
    return normed.astype(jnp.bfloat16), jax.nn.softmax(chosen, axis=0)


def neighbours():
    me = lax.axis_index('ep')
    core, chip = lax.rem(me, 2), me // 2
    side, up = lax.rem(chip, 2), chip // 2
    return me, core, chip, 1 - side + 2 * up, side + 2 * (1 - up), 3 - chip


def greet(devices):
    barrier = pltpu.get_barrier_semaphore()
    for device in devices:
        pl.semaphore_signal(barrier, inc=1, device_id={'ep': device}, device_id_type=pl.DeviceIdType.MESH)
    pl.semaphore_wait(barrier, len(devices))


def remote(src, dst, send_sem, recv_sem, device):
    return pltpu.make_async_remote_copy(src_ref=src, dst_ref=dst, send_sem=send_sem, recv_sem=recv_sem, device_id={'ep': device}, device_id_type=pl.DeviceIdType.MESH)


def attend_kernel(tok_ref, ids_hbm, wq_hbm, wk_hbm, wv_hbm, wo_hbm, ctx_hbm, wfull_hbm, slots_ref, ids_ref, ids_buf, i_send, i_recv, i_own, nbuf, wbuf, wmate, qkv, cbuf, loc_sem, a_send, b_send, f_send, m_send, mf_send, w_recv, wm_recv, n_send, n_recv, c_send, c_recv, c_own, ox_send, oy_send, od_send, o_recv, o_own):
    me, core, chip, xn, yn, dg = neighbours()
    side = lax.rem(chip, 2)
    mate = me + 1 - 2 * core
    x_dev, y_dev, dg_dev, x_mate = xn * 2 + core, yn * 2 + core, dg * 2 + core, xn * 2 + 1 - core
    weights = (wq_hbm, wk_hbm, wv_hbm)
    seqs, tok, dim = nbuf.shape
    group = wbuf.shape[3]
    part = tok // 4
    others = (x_dev, y_dev, mate, x_mate, dg_dev, yn * 2 + 1 - core, dg * 2 + 1 - core)
    greet(others)

    def cols(on_side, on_core):
        return pl.ds(pl.multiple_of((2 * on_side + on_core) * group, group), group)

    def local_w(m):
        return pltpu.make_async_copy(weights[m].at[:, cols(side, core)], wbuf.at[m, me], loc_sem.at[m])

    def own_mate(m):
        return remote(weights[m].at[:, cols(side, 1 - core)], wbuf.at[m, me], m_send.at[m], w_recv.at[m, me], mate)

    def over_x(m):
        return (remote(weights[m].at[:, cols(1 - side, core)], wbuf.at[m, me], a_send.at[m, 0], w_recv.at[m, me], x_dev),
                remote(weights[m].at[:, cols(1 - side, 1 - core)], wmate.at[m, 0], a_send.at[m, 1], wm_recv.at[m, 0], x_dev))

    def over_y(m):
        return (remote(weights[m].at[:, cols(side, core)], wbuf.at[m, me], b_send.at[m, 0], w_recv.at[m, me], y_dev),
                remote(weights[m].at[:, cols(side, 1 - core)], wmate.at[m, 1], b_send.at[m, 1], wm_recv.at[m, 1], y_dev))

    def forward_y(m):
        return (remote(wbuf.at[m, x_dev], wbuf.at[m, x_dev], f_send.at[m, 0], w_recv.at[m, x_dev], y_dev),
                remote(wmate.at[m, 0], wmate.at[m, 2], f_send.at[m, 1], wm_recv.at[m, 2], y_dev))

    def to_mate(m, slot):
        source = (x_dev, y_dev, dg_dev)[slot]
        return remote(wmate.at[m, slot], wbuf.at[m, source], mf_send.at[m, slot], w_recv.at[m, source], mate)

    def landed(m, source):
        remote(wbuf.at[m, source], wbuf.at[m, source], m_send.at[m], w_recv.at[m, source], mate).wait_recv()

    def landed_mate(m, slot):
        to = wmate.at[m, slot]
        remote(to, to, m_send.at[m], wm_recv.at[m, slot], mate).wait_recv()

    def start(copies):
        for copy in copies:
            copy.start()

    def n_copy(slot):
        source, device = (0, 0, 0, 2)[slot], (mate, mate, x_dev, mate)[slot]
        return remote(nbuf.at[source], nbuf.at[slot], n_send.at[slot], n_recv.at[slot], device)

    def id_copy(slot, owner):
        return remote(ids_hbm, ids_buf.at[owner], i_send.at[slot], i_recv.at[owner], others[slot])

    def rows(piece):
        return pl.ds(piece * part, part)

    def wo_x(slot, source, piece, src):
        return remote(src, wfull_hbm.at[source, rows(piece)], ox_send.at[slot], o_recv.at[source, piece], x_dev)

    def wo_y(slot, source, piece, src):
        return remote(src, wfull_hbm.at[source, rows(piece)], oy_send.at[slot], o_recv.at[source, piece], y_dev)

    def wo_mate(order, source, piece, src):
        return remote(src, wfull_hbm.at[source, rows(piece)], od_send.at[order, piece], o_recv.at[source, piece], mate)

    def wo_landed(source, piece):
        to = wfull_hbm.at[source, rows(piece)]
        remote(to, to, od_send.at[0, 0], o_recv.at[source, piece], mate).wait_recv()

    for slot in range(7):
        id_copy(slot, me).start()
    id_own = pltpu.make_async_copy(ids_hbm, ids_buf.at[me], i_own)
    id_own.start()
    start(over_x(0))
    start(over_y(0))
    for m in range(3):
        local_w(m).start()
        own_mate(m).start()
    start(over_y(1))
    wide = tok_ref[...].astype(jnp.float32)
    nbuf[0] = (wide * lax.rsqrt(jnp.mean(wide * wide, axis=-1, keepdims=True) + EPS)).astype(jnp.bfloat16)
    n_copy(2).start()
    n_copy(1).start()
    start(over_x(1))
    start(over_x(2))
    for piece in range(4):
        wo_x(piece, me, piece, wo_hbm.at[rows(piece)]).start()
    for piece in range(4):
        wo_mate(0, me, piece, wo_hbm.at[rows(piece)]).start()
    wo_own = pltpu.make_async_copy(wo_hbm, wfull_hbm.at[me], o_own)
    wo_own.start()

    id_own.wait()
    for slot in range(7):
        id_copy(slot, others[slot]).wait_recv()
    order = lax.broadcasted_iota(jnp.int32, (tok, tok), 0) < lax.broadcasted_iota(jnp.int32, (tok, tok), 1)
    earlier = jnp.where(order, 1.0, 0.0).astype(jnp.bfloat16)
    experts = slots_ref.shape[1]
    spot = lax.broadcasted_iota(jnp.int32, (experts, tok), 0)
    local = experts // 2
    wanted = jnp.where(spot < local, me * local + spot, (mate - 1) * local + spot)

    def table(source, c):
        count = jnp.zeros((experts, tok), jnp.float32)
        for j in range(ids_buf.shape[1]):
            count = count + jnp.where(ids_buf[source, j:j + 1, :] == wanted, 1.0, 0.0)
        before = jnp.dot(count.astype(jnp.bfloat16), earlier, preferred_element_type=jnp.float32)
        slots_ref[source] = jnp.where(count > 0.0, before, -1.0)
        ids_ref[source] = ids_buf[source]
        return c

    lax.fori_loop(0, ids_buf.shape[0], table, 0)

    def arrive_x(m):
        landed(m, x_dev)
        landed_mate(m, 0)
        start(forward_y(m))
        to_mate(m, 0).start()

    def finish(m):
        landed_mate(m, 1)
        to_mate(m, 1).start()
        landed_mate(m, 2)
        to_mate(m, 2).start()
        local_w(m).wait()
        for source in (y_dev, dg_dev, mate, x_mate, yn * 2 + 1 - core, dg * 2 + 1 - core):
            landed(m, source)

    width = 256

    def project(m):
        def run(i, c):
            slot, n = i // (group // width), lax.rem(i, group // width)
            at = pl.ds(pl.multiple_of(n * width, width), width)
            out = jnp.dot(nbuf[slot], wbuf[m, :, :, at].reshape(dim, width), preferred_element_type=jnp.float32)
            qkv[m, slot, :, at] = out.astype(jnp.bfloat16)
            return c

        lax.fori_loop(0, seqs * (group // width), run, 0)

    arrive_x(0)
    start(over_y(2))
    n_copy(2).wait_recv()
    n_copy(3).start()
    finish(0)
    n_copy(1).wait_recv()
    n_copy(3).wait_recv()
    project(0)
    arrive_x(1)
    arrive_x(2)
    for slot, piece in enumerate((3, 0, 1, 2)):
        wo_y(slot, me, piece, wo_hbm.at[rows(piece)]).start()
    finish(1)
    project(1)
    finish(2)
    project(2)

    scale = 128 ** -0.5
    block = tok // 2
    pairs = group // 256

    def c_copy(slot, pair):
        at = pl.ds(pl.multiple_of(pair * 256, 256), 256)
        there = pl.ds(pl.multiple_of((2 * side + core) * group + pair * 256, 256), 256)
        src, dst = cbuf.at[slot, :, at], ctx_hbm.at[:, there]
        if slot == 0:
            return pltpu.make_async_copy(src, dst, c_own.at[pair])
        return remote(src, dst, c_send.at[slot - 1, pair], c_recv.at[slot - 1, pair], (mate, x_dev, x_mate)[slot - 1])

    def heads(pair, carry):
        def one_seq(slot, c):
            for h in range(2):
                at = pl.ds(pl.multiple_of(pair * 256 + h * 128, 128), 128)
                keys, values = qkv[1, slot, :, at], qkv[2, slot, :, at]
                for b in range(2):
                    query = qkv[0, slot, b * block:(b + 1) * block, at]
                    span = (b + 1) * block
                    s = lax.dot_general(query, keys[:span], (((1,), (1,)), ((), ())), preferred_element_type=jnp.float32) * scale
                    row = lax.broadcasted_iota(jnp.int32, (block, span), 0) + b * block
                    s = jnp.where(row >= lax.broadcasted_iota(jnp.int32, (block, span), 1), s, -jnp.inf)
                    e = jnp.exp(s - jnp.max(s, axis=-1, keepdims=True))
                    p = (e * (1.0 / jnp.sum(e, axis=-1, keepdims=True))).astype(jnp.bfloat16)
                    cbuf[slot, b * block:(b + 1) * block, at] = jnp.dot(p, values[:span], preferred_element_type=jnp.float32).astype(jnp.bfloat16)
            return c

        lax.fori_loop(0, seqs, one_seq, 0)
        for slot in (2, 3, 1, 0):
            c_copy(slot, pair).start()

        @pl.when(pair == 1)
        def _():
            for piece in range(4):
                wo_landed(x_dev, piece)
                wo_mate(1, x_dev, piece, wfull_hbm.at[x_dev, rows(piece)]).start()
                if piece < 3:
                    wo_y(4 + piece, x_dev, piece, wfull_hbm.at[x_dev, rows(piece)]).start()

        return carry

    lax.fori_loop(0, pairs, heads, 0)
    for piece in (3, 0, 1, 2):
        wo_landed(y_dev, piece)
        wo_mate(2, y_dev, piece, wfull_hbm.at[y_dev, rows(piece)]).start()
        if piece == 3:
            wo_x(4, y_dev, piece, wfull_hbm.at[y_dev, rows(piece)]).start()
    for piece in (0, 1, 2, 3):
        wo_landed(dg_dev, piece)
        wo_mate(3, dg_dev, piece, wfull_hbm.at[dg_dev, rows(piece)]).start()
    for slot in range(1, 4):
        for pair in range(4):
            at = pl.ds(pair * 256, 256)
            remote(cbuf.at[0, :, at], ctx_hbm.at[:, at], c_send.at[slot - 1, pair], c_recv.at[slot - 1, pair], mate).wait_recv()
    for source in (mate, x_mate, yn * 2 + 1 - core, dg * 2 + 1 - core):
        for piece in range(4):
            wo_landed(source, piece)
    for slot in range(7):
        id_copy(slot, me).wait_send()
    for m in range(3):
        own_mate(m).wait_send()
        for copy in over_x(m) + over_y(m) + forward_y(m):
            copy.wait_send()
        for slot in range(3):
            to_mate(m, slot).wait_send()
    for slot in range(1, 4):
        n_copy(slot).wait_send()
    for pair in range(4):
        c_copy(0, pair).wait()
        for slot in range(1, 4):
            c_copy(slot, pair).wait_send()
    wo_own.wait()
    for slot in range(5):
        wo_x(slot, me, 0, wo_hbm.at[rows(0)]).wait_send()
    for slot in range(7):
        wo_y(slot, me, 0, wo_hbm.at[rows(0)]).wait_send()
    for order in range(4):
        for piece in range(4):
            wo_mate(order, me, piece, wo_hbm.at[rows(piece)]).wait_send()


def attend(tokens, ids, w_query, w_key, w_value, w_out):
    tok, dim = tokens.shape
    depth, width = w_query.shape
    devices, group = 8, width // 4
    dma = pltpu.SemaphoreType.DMA
    any_spec = pl.BlockSpec(memory_space=pl.ANY)
    return pl.pallas_call(
        attend_kernel,
        out_shape=(jax.ShapeDtypeStruct((tok, width), jnp.bfloat16), jax.ShapeDtypeStruct((devices,) + w_out.shape, jnp.bfloat16), jax.ShapeDtypeStruct((devices, 32, tok), jnp.float32), jax.ShapeDtypeStruct((devices,) + ids.shape, jnp.int32)),
        in_specs=[pl.BlockSpec(memory_space=pltpu.VMEM)] + [any_spec] * 5,
        out_specs=(any_spec, any_spec, pl.BlockSpec(memory_space=pltpu.VMEM), pl.BlockSpec(memory_space=pltpu.VMEM)),
        scratch_shapes=[
            pltpu.VMEM((devices,) + ids.shape, jnp.int32), dma((7,)), dma((devices,)), dma,
            pltpu.VMEM((4, tok, dim), jnp.bfloat16),
            pltpu.VMEM((3, devices, depth, group), jnp.bfloat16),
            pltpu.VMEM((3, 3, depth, group), jnp.bfloat16),
            pltpu.VMEM((3, 4, tok, group), jnp.bfloat16),
            pltpu.VMEM((4, tok, group), jnp.bfloat16),
            dma((3,)), dma((3, 2)), dma((3, 2)), dma((3, 2)), dma((3,)), dma((3, 3)), dma((3, devices)), dma((3, 3)),
            dma((4,)), dma((4,)), dma((3, 4)), dma((3, 4)), dma((4,)),
            dma((5,)), dma((7,)), dma((4, 4)), dma((devices, 4)), dma,
        ],
        compiler_params=pltpu.CompilerParams(collective_id=3, has_side_effects=True, vmem_limit_bytes=VMEM_MAX),
        name='attend_heads',
    )(tokens, ids, w_query, w_key, w_value, w_out)


def spread_kernel(u_hbm, g_hbm, slot_ref, x_hbm, gall_hbm, ubuf, hbuf, xbuf, own_sem, gown_sem, out_sem, x_send, y_send, d_send, recv, g_send, g_recv):
    me, core, chip, xn, yn, dg = neighbours()
    mate = me + 1 - 2 * core
    tok = ubuf.shape[1]
    part = tok // 4
    local_experts = slot_ref.shape[1] // 2
    x_dev, y_dev, dg_dev = xn * 2 + core, yn * 2 + core, dg * 2 + core
    others = (x_dev, y_dev, mate, dg_dev, xn * 2 + 1 - core, yn * 2 + 1 - core, dg * 2 + 1 - core)
    greet(others)

    def rows(piece):
        return pl.ds(piece * part, part)

    def landed(source, piece):
        remote(ubuf.at[source, rows(piece)], ubuf.at[source, rows(piece)], d_send.at[0, 0], recv.at[source, piece], mate).wait_recv()

    def pass_on(order, source, piece):
        return remote(ubuf.at[source, rows(piece)], ubuf.at[source, rows(piece)], d_send.at[order, piece], recv.at[source, piece], mate)

    def across_x(slot, source, piece, src):
        return remote(src, ubuf.at[source, rows(piece)], x_send.at[slot], recv.at[source, piece], x_dev)

    def across_y(slot, source, piece, src):
        return remote(src, ubuf.at[source, rows(piece)], y_send.at[slot], recv.at[source, piece], y_dev)

    own = pltpu.make_async_copy(u_hbm, ubuf.at[me], own_sem)
    own.start()
    gown = pltpu.make_async_copy(g_hbm, gall_hbm.at[me], gown_sem)
    gown.start()
    for slot in range(4):
        across_x(slot, me, slot, u_hbm.at[rows(slot)]).start()
        across_y(slot, me, (slot + 2) % 4, u_hbm.at[rows((slot + 2) % 4)]).start()
    for piece in range(4):
        remote(u_hbm.at[rows(piece)], ubuf.at[me, rows(piece)], d_send.at[0, piece], recv.at[me, piece], mate).start()
    for slot, device in enumerate(others):
        remote(g_hbm, gall_hbm.at[me], g_send.at[slot], g_recv.at[me], device).start()
    own.wait()

    def out_copy(order, source):
        return pltpu.make_async_copy(xbuf.at[lax.rem(order, 2)], x_hbm.at[:, source], out_sem.at[lax.rem(order, 2)])

    def step(order, carry):
        kind = order // 2
        base = jnp.where(kind == 0, chip, jnp.where(kind == 1, xn, jnp.where(kind == 2, yn, dg)))
        odd = lax.rem(order, 2)
        source = base * 2 + core + odd * (1 - 2 * core)

        @pl.when(order == 2)
        def _():
            for piece in (0, 1):
                landed(x_dev, piece)
                across_y(4 + piece, x_dev, piece, ubuf.at[x_dev, rows(piece)]).start()
                pass_on(1, x_dev, piece).start()
                landed(y_dev, piece + 2)
                across_x(4 + piece, y_dev, piece + 2, ubuf.at[y_dev, rows(piece + 2)]).start()
                pass_on(2, y_dev, piece + 2).start()
            for piece in (0, 1):
                landed(x_dev, piece + 2)
                pass_on(1, x_dev, piece + 2).start()
                landed(y_dev, piece)
                pass_on(2, y_dev, piece).start()

        @pl.when(order == 6)
        def _():
            for piece in (0, 2, 1, 3):
                landed(dg_dev, piece)
                pass_on(3, dg_dev, piece).start()

        @pl.when(odd == 1)
        def _():
            for piece in range(4):
                landed(source, piece)

        @pl.when(order >= 2)
        def _():
            out_copy(order, source).wait()

        spot = lax.broadcasted_iota(jnp.int32, (CAP, tok), 0).astype(jnp.float32)
        for expert in range(local_experts):
            hit = slot_ref[source, expert:expert + 1, :] == spot
            hbuf[expert * CAP:(expert + 1) * CAP, :] = jnp.where(hit, 1.0, 0.0).astype(jnp.bfloat16)
        width = 256

        def tile(n, c):
            cols = pl.ds(pl.multiple_of(n * width, width), width)
            picked = jnp.dot(hbuf[...], ubuf[source, :, cols], preferred_element_type=jnp.float32)
            xbuf[odd, :, :, cols] = picked.astype(jnp.bfloat16).reshape(local_experts, CAP, width)
            return c

        lax.fori_loop(0, ubuf.shape[2] // width, tile, 0)
        out_copy(order, source).start()
        return carry

    lax.fori_loop(0, 8, step, 0)
    out_copy(0, me).wait()
    out_copy(1, me).wait()
    gown.wait()
    for slot in range(4):
        across_x(slot, me, slot, u_hbm.at[rows(slot)]).wait_send()
        across_y(slot, me, slot, u_hbm.at[rows(slot)]).wait_send()
    for piece in (0, 1):
        across_y(4 + piece, x_dev, piece, ubuf.at[x_dev, rows(piece)]).wait_send()
        across_x(4 + piece, y_dev, piece + 2, ubuf.at[y_dev, rows(piece + 2)]).wait_send()
    for order, source in enumerate((me, x_dev, y_dev, dg_dev)):
        for piece in range(4):
            pass_on(order, source, piece).wait_send()
    for slot, device in enumerate(others):
        remote(g_hbm, gall_hbm.at[me], g_send.at[slot], g_recv.at[me], device).wait_send()
        remote(g_hbm, gall_hbm.at[device], g_send.at[slot], g_recv.at[device], device).wait_recv()


def spread(u, gates, slots):
    devices, pair_experts, tok = slots.shape
    local_experts = pair_experts // 2
    dim = u.shape[1]
    return pl.pallas_call(
        spread_kernel,
        out_shape=(jax.ShapeDtypeStruct((local_experts, devices, CAP, dim), jnp.bfloat16), jax.ShapeDtypeStruct((devices,) + gates.shape, jnp.float32)),
        in_specs=[pl.BlockSpec(memory_space=pl.ANY), pl.BlockSpec(memory_space=pl.ANY), pl.BlockSpec(memory_space=pltpu.VMEM)],
        out_specs=(pl.BlockSpec(memory_space=pl.ANY), pl.BlockSpec(memory_space=pl.ANY)),
        scratch_shapes=[
            pltpu.VMEM((devices, tok, dim), jnp.bfloat16),
            pltpu.VMEM((local_experts * CAP, tok), jnp.bfloat16),
            pltpu.VMEM((2, local_experts, CAP, dim), jnp.bfloat16),
            pltpu.SemaphoreType.DMA, pltpu.SemaphoreType.DMA, pltpu.SemaphoreType.DMA((2,)),
            pltpu.SemaphoreType.DMA((6,)), pltpu.SemaphoreType.DMA((6,)), pltpu.SemaphoreType.DMA((4, 4)),
            pltpu.SemaphoreType.DMA((devices, 4)), pltpu.SemaphoreType.DMA((7,)), pltpu.SemaphoreType.DMA((devices,)),
        ],
        compiler_params=pltpu.CompilerParams(collective_id=1, has_side_effects=True, vmem_limit_bytes=VMEM_MAX),
        name='spread_rows',
    )(u, gates, slots)


def ffn_kernel(units_ref, x_ref, w1_ref, w3_ref, w2_ref, o_ref, packed, middle, done):
    expert = pl.program_id(0)
    devices = x_ref.shape[1]
    tile = 128
    total = 0
    for source in range(devices):
        count = units_ref[expert * devices + source]

        def pack(i, c, source=source, total=total):
            packed[pl.ds(pl.multiple_of((total + i) * UNIT, UNIT), UNIT), :] = x_ref[0, source, pl.ds(pl.multiple_of(i * UNIT, UNIT), UNIT), :]
            return c

        lax.fori_loop(0, count, pack, 0)
        total = total + count

    def run(t, c):
        rows = pl.ds(pl.multiple_of(t * tile, tile), tile)
        for n in range(w1_ref.shape[2] // 256):
            cols = slice(n * 256, (n + 1) * 256)
            first = jnp.dot(packed[rows, :], w1_ref[0, :, cols], preferred_element_type=jnp.float32)
            third = jnp.dot(packed[rows, :], w3_ref[0, :, cols], preferred_element_type=jnp.float32)
            middle[:, cols] = (first * jax.nn.sigmoid(first) * third).astype(jnp.bfloat16)
        for n in range(w2_ref.shape[2] // 512):
            cols = slice(n * 512, (n + 1) * 512)
            done[rows, cols] = jnp.dot(middle[...], w2_ref[0, :, cols], preferred_element_type=jnp.float32).astype(jnp.bfloat16)
        return c

    lax.fori_loop(0, (total * UNIT + tile - 1) // tile, run, 0)
    total = 0
    for source in range(devices):
        count = units_ref[expert * devices + source]

        def unpack(i, c, source=source, total=total):
            o_ref[0, source, pl.ds(pl.multiple_of(i * UNIT, UNIT), UNIT), :] = done[pl.ds(pl.multiple_of((total + i) * UNIT, UNIT), UNIT), :]
            return c

        def clear(i, c, source=source):
            o_ref[0, source, pl.ds(pl.multiple_of(i * UNIT, UNIT), UNIT), :] = jnp.zeros((UNIT, o_ref.shape[3]), jnp.bfloat16)
            return c

        lax.fori_loop(0, count, unpack, 0)
        lax.fori_loop(count, CAP // UNIT, clear, 0)
        total = total + count


def expert_ffn(units, x, w_one, w_three, w_two):
    experts, devices, _, dim = x.shape
    mid = w_one.shape[2]
    block = lambda *shape: pl.BlockSpec((1,) + shape, lambda e, units: (e,) + (0,) * len(shape))
    return pl.pallas_call(
        ffn_kernel,
        out_shape=jax.ShapeDtypeStruct(x.shape, jnp.bfloat16),
        grid_spec=pltpu.PrefetchScalarGridSpec(
            num_scalar_prefetch=1,
            grid=(experts,),
            in_specs=[block(devices, CAP, dim), block(dim, mid), block(dim, mid), block(mid, dim)],
            out_specs=block(devices, CAP, dim),
            scratch_shapes=[pltpu.VMEM((devices * CAP, dim), jnp.bfloat16), pltpu.VMEM((128, mid), jnp.bfloat16), pltpu.VMEM((devices * CAP, dim), jnp.bfloat16)],
        ),
        compiler_params=pltpu.CompilerParams(dimension_semantics=('arbitrary',), vmem_limit_bytes=VMEM_MAX),
        name='expert_mlp',
    )(units, x, w_one, w_three, w_two)


def combine_kernel(o_hbm, tab_hbm, h_hbm, y_ref, own, mate_rows, tab, gate3, p_one, r_one, p_two, r_two, p_last, r_last, own_sem, tab_sem, h_sem, mate_send, mate_recv, one_send, one_recv, two_send, two_recv, last_send, last_recv):
    me, core, chip, xn, yn, dg = neighbours()
    mate = me + 1 - 2 * core
    near = xn + core * (yn - xn)
    far = yn + core * (xn - yn)
    near_dev, far_dev = near * 2 + core, far * 2 + core
    half = own.shape[3]
    rows_n = p_one.shape[1]
    experts = own.shape[1]
    greet((near_dev, far_dev, mate))
    my_cols = pl.ds(pl.multiple_of(core * half, half), half)
    mate_cols = pl.ds(pl.multiple_of((1 - core) * half, half), half)

    def dest(i, first, second):
        pair = i // 2
        base = jnp.where(pair == 0, dg, jnp.where(pair == 1, first, jnp.where(pair == 2, second, chip)))
        return base

    def my_dest(i):
        odd = lax.rem(i, 2)
        return dest(i, near, far) * 2 + jnp.where(i < 6, odd, 1 - core + odd * (2 * core - 1))

    def mate_dest(i):
        odd = lax.rem(i, 2)
        return dest(i, far, near) * 2 + jnp.where(i < 6, odd, core + odd * (1 - 2 * core))

    def to_mate(i):
        return remote(o_hbm.at[:, mate_dest(i), :, mate_cols], mate_rows.at[i], mate_send.at[i], mate_recv.at[i], mate)

    def own_copy(i):
        return pltpu.make_async_copy(o_hbm.at[:, my_dest(i), :, my_cols], own.at[lax.rem(i, 2)], own_sem.at[lax.rem(i, 2)])

    def tab_copy(i):
        return pltpu.make_async_copy(tab_hbm.at[my_dest(i)], tab.at[lax.rem(i, 2)], tab_sem.at[lax.rem(i, 2)])

    def one_copy(n):
        return remote(p_one.at[n], r_one.at[n], one_send.at[n], one_recv.at[n], near_dev)

    def two_copy(n):
        return remote(p_two.at[n], r_two.at[n], two_send.at[n], two_recv.at[n], far_dev)

    def last_copy(n):
        return remote(p_last.at[n], r_last.at[n], last_send.at[n], last_recv.at[n], mate)

    own_copy(0).start()
    tab_copy(0).start()
    for i in range(8):
        to_mate(i).start()
    residual = pltpu.make_async_copy(h_hbm, y_ref, h_sem)
    residual.start()

    def open_dest(i):
        own_copy(i).wait()
        tab_copy(i).wait()
        to_mate(i).wait_recv()

        @pl.when(i < 7)
        def _():
            own_copy(i + 1).start()
            tab_copy(i + 1).start()

    def weights(i, part):
        slot = lax.rem(i, 2)
        cols = pl.ds(pl.multiple_of(part * rows_n, rows_n), rows_n)
        spot = lax.broadcasted_iota(jnp.int32, (2 * CAP, rows_n), 0)
        low = spot < CAP
        place = (spot - jnp.where(low, 0, CAP)).astype(jnp.float32)
        for pair in range(experts):
            at = tab[slot, 2 * pair:2 * pair + 2, cols]
            gate = tab[slot, 2 * experts + 2 * pair:2 * experts + 2 * pair + 2, cols]
            hit = jnp.where(low, at[0:1], at[1:2]) == place
            value = jnp.where(hit, jnp.where(low, gate[0:1], gate[1:2]), 0.0).T
            top = value.astype(jnp.bfloat16)
            rest = value - top.astype(jnp.float32)
            mid = rest.astype(jnp.bfloat16)
            low_part = (rest - mid.astype(jnp.float32)).astype(jnp.bfloat16)
            where = slice(pair * 2 * CAP, (pair + 1) * 2 * CAP)
            gate3[0:rows_n, where] = top
            gate3[rows_n:2 * rows_n, where] = mid
            gate3[2 * rows_n:3 * rows_n, where] = low_part

    def products(i, part, sink):
        weights(i, part)
        slot = lax.rem(i, 2)
        depth = experts * CAP
        width = 256

        def tile(n, c):
            cols = pl.ds(pl.multiple_of(n * width, width), width)
            mine = own[slot, :, :, cols].reshape(depth, width)
            other = mate_rows[i, :, :, cols].reshape(depth, width)
            out = jnp.dot(gate3[:, :depth], mine, preferred_element_type=jnp.float32) + jnp.dot(gate3[:, depth:], other, preferred_element_type=jnp.float32)
            sink(cols, out[0:rows_n] + out[rows_n:2 * rows_n] + out[2 * rows_n:3 * rows_n])
            return c

        lax.fori_loop(0, half // width, tile, 0)

    def phase_one(step, c):
        i, part = step // 2, lax.rem(step, 2)

        @pl.when(part == 0)
        def _():
            open_dest(i)

        def sink(cols, value):
            p_one[step, :, cols] = value

        products(i, part, sink)
        one_copy(step).start()
        return c

    lax.fori_loop(0, 8, phase_one, 0)

    def phase_two(step, c):
        i, part = 4 + step // 2, lax.rem(step, 2)

        @pl.when(part == 0)
        def _():
            open_dest(i)

        def sink(cols, value):
            p_two[step, :, cols] = value

        products(i, part, sink)
        one_copy(step).wait_recv()
        p_two[step] = p_two[step] + r_one[step]
        two_copy(step).start()
        return c

    lax.fori_loop(0, 4, phase_two, 0)
    residual.wait()

    def phase_three(step, c):
        i, part = 6 + step // 2, lax.rem(step, 2)

        @pl.when(part == 0)
        def _():
            open_dest(i)

        def sink(cols, value):
            p_last[step, :, cols] = value

        products(i, part, sink)
        target = jnp.where(step < 2, 1 - core, core)
        n = target * 2 + part
        one_copy(4 + n).wait_recv()
        two_copy(n).wait_recv()
        p_last[step] = p_last[step] + (r_one[4 + n] + r_two[n])

        @pl.when(step < 2)
        def _():
            last_copy(step).start()

        @pl.when(step >= 2)
        def _():
            rows = pl.ds(pl.multiple_of(part * rows_n, rows_n), rows_n)
            y_ref[rows, my_cols] = (y_ref[rows, my_cols].astype(jnp.float32) + p_last[step]).astype(jnp.bfloat16)

        return c

    lax.fori_loop(0, 4, phase_three, 0)
    for n in range(2):
        rows = pl.ds(n * rows_n, rows_n)
        last_copy(n).wait_recv()
        y_ref[rows, mate_cols] = (y_ref[rows, mate_cols].astype(jnp.float32) + r_last[n]).astype(jnp.bfloat16)
    for n in range(8):
        to_mate(n).wait_send()
        one_copy(n).wait_send()
    for n in range(4):
        two_copy(n).wait_send()
    for n in range(2):
        last_copy(n).wait_send()


def combine(done, tab, hidden):
    experts, devices, _, dim = done.shape
    tok = hidden.shape[0]
    half, part = dim // 2, tok // 2
    dma = pltpu.SemaphoreType.DMA
    return pl.pallas_call(
        combine_kernel,
        out_shape=jax.ShapeDtypeStruct((tok, dim), jnp.bfloat16),
        in_specs=[pl.BlockSpec(memory_space=pl.ANY)] * 3,
        out_specs=pl.BlockSpec(memory_space=pltpu.VMEM),
        scratch_shapes=[
            pltpu.VMEM((2, experts, CAP, half), jnp.bfloat16),
            pltpu.VMEM((devices, experts, CAP, half), jnp.bfloat16),
            pltpu.VMEM((2,) + tab.shape[1:], jnp.float32),
            pltpu.VMEM((3 * part, 2 * experts * CAP), jnp.bfloat16),
            pltpu.VMEM((8, part, half), jnp.float32),
            pltpu.VMEM((8, part, half), jnp.float32),
            pltpu.VMEM((4, part, half), jnp.float32),
            pltpu.VMEM((4, part, half), jnp.float32),
            pltpu.VMEM((4, part, half), jnp.float32),
            pltpu.VMEM((2, part, half), jnp.float32),
            dma((2,)), dma((2,)), dma, dma((8,)), dma((8,)), dma((8,)), dma((8,)), dma((4,)), dma((4,)), dma((2,)), dma((2,)),
        ],
        compiler_params=pltpu.CompilerParams(collective_id=2, has_side_effects=True, vmem_limit_bytes=VMEM_MAX),
        name='combine_rows',
    )(done, tab, hidden)


def solution(mesh):
    tok_spec = P(('dp', 'ep'))
    row_spec = P('ep')

    def local_layer(tokens, w_query, w_key, w_value, w_out, w_router, w_one, w_three, w_two, expert_ids):
        seq_count, seq_len, model_dim = tokens.shape
        choices = expert_ids.shape[2]
        local_experts = w_one.shape[0]
        tok_count = seq_count * seq_len
        ids_t = expert_ids.reshape(tok_count, choices).T
        flat = tokens.reshape(tok_count, model_dim)
        w_flat = [w.reshape(w.shape[0], -1) for w in (w_query, w_key, w_value)]
        context, full_out, slot, all_ids = attend(flat, ids_t, *w_flat, w_out)
        units = ((jnp.max(slot[:, :local_experts], axis=2).astype(jnp.int32) + UNIT) // UNIT).T.reshape(-1)
        mixed = jnp.dot(context, full_out.reshape(-1, model_dim), preferred_element_type=jnp.float32)
        hidden = (flat.astype(jnp.float32) + mixed).astype(jnp.bfloat16)
        normed, gates = router_gates(hidden, w_router, ids_t)
        x, all_gates = spread(normed, gates, slot)
        me = lax.axis_index('ep')
        local = jnp.arange(local_experts, dtype=jnp.int32)
        wanted = jnp.concatenate([me * local_experts + local, (me + 1 - 2 * lax.rem(me, 2)) * local_experts + local])
        hit = all_ids[:, :, None, :] == wanted[None, None, :, None]
        gate = jnp.sum(jnp.where(hit, all_gates[:, :, None, :], 0.0), axis=1)
        tab = jnp.concatenate([slot, gate], axis=1)
        done = expert_ffn(units, x, w_one, w_three, w_two)
        layer_out = combine(done, tab, hidden)
        return layer_out.reshape(seq_count, seq_len, model_dim)

    return jax.shard_map(local_layer, mesh=mesh, in_specs=(tok_spec, row_spec, row_spec, row_spec, row_spec, P(), row_spec, row_spec, row_spec, tok_spec), out_specs=tok_spec, check_vma=False)
```

```python
import functools

import jax
import jax.numpy as jnp
from jax import lax
from jax.experimental import pallas as pl
from jax.experimental.pallas import tpu as pltpu
from jax.sharding import PartitionSpec as P

EPS = 1e-6
CAP = 64
UNIT = 16
VMEM_MAX = 67043328
LANES = 128
TILE = 256
CORES = 2
PARTS = 4
ANY = pl.BlockSpec(memory_space=pl.ANY)
WHOLE = pl.BlockSpec(memory_space=pltpu.VMEM)


def strips(size, width):
    return [slice(at, at + width) for at in range(0, size, width)]


def start(copies):
    for copy in copies:
        copy.start()


def finish_send(copies):
    for copy in copies:
        copy.wait_send()


def rms_norm(vals):
    wide = vals.astype(jnp.float32)
    return wide * lax.rsqrt(jnp.mean(wide * wide, axis=-1, keepdims=True) + EPS)


def router_gates(hidden, w_router, ids_t):
    normed = rms_norm(hidden)
    logits = jnp.einsum('td,de->et', normed, w_router, precision=lax.Precision.HIGHEST, preferred_element_type=jnp.float32)
    hit = ids_t[:, None, :] == jnp.arange(w_router.shape[1], dtype=jnp.int32)[None, :, None]
    chosen = jnp.sum(jnp.where(hit, logits[None], 0.0), axis=1)
    return normed.astype(jnp.bfloat16), jax.nn.softmax(chosen, axis=0)


def neighbours():
    me = lax.axis_index('ep')
    core, chip = lax.rem(me, 2), me // 2
    side, up = lax.rem(chip, 2), chip // 2
    return me, core, chip, 1 - side + 2 * up, side + 2 * (1 - up), 3 - chip


def greet(devices):
    barrier = pltpu.get_barrier_semaphore()
    for device in devices:
        pl.semaphore_signal(barrier, inc=1, device_id={'ep': device}, device_id_type=pl.DeviceIdType.MESH)
    pl.semaphore_wait(barrier, len(devices))


def remote(src, dst, send_sem, recv_sem, device):
    return pltpu.make_async_remote_copy(src_ref=src, dst_ref=dst, send_sem=send_sem, recv_sem=recv_sem, device_id={'ep': device}, device_id_type=pl.DeviceIdType.MESH)


def attend_kernel(tok_ref, ids_hbm, wq_hbm, wk_hbm, wv_hbm, wo_hbm, ctx_hbm, wfull_hbm, slots_ref, ids_ref, ids_buf, i_send, i_recv, i_own, nbuf, wbuf, wmate, qkv, cbuf, loc_sem, a_send, b_send, f_send, m_send, mf_send, w_recv, wm_recv, n_send, n_recv, c_send, c_recv, c_own, ox_send, oy_send, od_send, o_recv, o_own):
    me, core, chip, xn, yn, dg = neighbours()
    side = lax.rem(chip, 2)
    mate = me + 1 - 2 * core
    x_dev, y_dev, dg_dev, x_mate = xn * CORES + core, yn * CORES + core, dg * CORES + core, xn * CORES + 1 - core
    weights = (wq_hbm, wk_hbm, wv_hbm)
    seqs, tok, dim = nbuf.shape
    group = wbuf.shape[3]
    part = tok // 4
    others = (x_dev, y_dev, mate, x_mate, dg_dev, yn * CORES + 1 - core, dg * CORES + 1 - core)
    greet(others)

    def cols(on_side, on_core):
        return pl.ds(pl.multiple_of((2 * on_side + on_core) * group, group), group)

    def local_w(m):
        return pltpu.make_async_copy(weights[m].at[:, cols(side, core)], wbuf.at[m, me], loc_sem.at[m])

    def own_mate(m):
        return remote(weights[m].at[:, cols(side, 1 - core)], wbuf.at[m, me], m_send.at[m], w_recv.at[m, me], mate)

    def over_x(m):
        return (remote(weights[m].at[:, cols(1 - side, core)], wbuf.at[m, me], a_send.at[m, 0], w_recv.at[m, me], x_dev),
                remote(weights[m].at[:, cols(1 - side, 1 - core)], wmate.at[m, 0], a_send.at[m, 1], wm_recv.at[m, 0], x_dev))

    def over_y(m):
        return (remote(weights[m].at[:, cols(side, core)], wbuf.at[m, me], b_send.at[m, 0], w_recv.at[m, me], y_dev),
                remote(weights[m].at[:, cols(side, 1 - core)], wmate.at[m, 1], b_send.at[m, 1], wm_recv.at[m, 1], y_dev))

    def forward_y(m):
        return (remote(wbuf.at[m, x_dev], wbuf.at[m, x_dev], f_send.at[m, 0], w_recv.at[m, x_dev], y_dev),
                remote(wmate.at[m, 0], wmate.at[m, 2], f_send.at[m, 1], wm_recv.at[m, 2], y_dev))

    def to_mate(m, slot):
        source = (x_dev, y_dev, dg_dev)[slot]
        return remote(wmate.at[m, slot], wbuf.at[m, source], mf_send.at[m, slot], w_recv.at[m, source], mate)

    def landed(m, source):
        remote(wbuf.at[m, source], wbuf.at[m, source], m_send.at[m], w_recv.at[m, source], mate).wait_recv()

    def landed_mate(m, slot):
        to = wmate.at[m, slot]
        remote(to, to, m_send.at[m], wm_recv.at[m, slot], mate).wait_recv()

    def n_copy(slot):
        source, device = (0, 0, 0, 2)[slot], (mate, mate, x_dev, mate)[slot]
        return remote(nbuf.at[source], nbuf.at[slot], n_send.at[slot], n_recv.at[slot], device)

    def id_copy(slot, owner):
        return remote(ids_hbm, ids_buf.at[owner], i_send.at[slot], i_recv.at[owner], others[slot])

    def rows(piece):
        return pl.ds(piece * part, part)

    def wo_x(slot, source, piece, src):
        return remote(src, wfull_hbm.at[source, rows(piece)], ox_send.at[slot], o_recv.at[source, piece], x_dev)

    def wo_y(slot, source, piece, src):
        return remote(src, wfull_hbm.at[source, rows(piece)], oy_send.at[slot], o_recv.at[source, piece], y_dev)

    def wo_mate(order, source, piece, src):
        return remote(src, wfull_hbm.at[source, rows(piece)], od_send.at[order, piece], o_recv.at[source, piece], mate)

    def wo_landed(source, piece):
        to = wfull_hbm.at[source, rows(piece)]
        remote(to, to, od_send.at[0, 0], o_recv.at[source, piece], mate).wait_recv()

    for slot in range(7):
        id_copy(slot, me).start()
    id_own = pltpu.make_async_copy(ids_hbm, ids_buf.at[me], i_own)
    id_own.start()
    start(over_x(0))
    start(over_y(0))
    for m in range(3):
        local_w(m).start()
        own_mate(m).start()
    start(over_y(1))
    wide = tok_ref[...].astype(jnp.float32)
    nbuf[0] = (wide * lax.rsqrt(jnp.mean(wide * wide, axis=-1, keepdims=True) + EPS)).astype(jnp.bfloat16)
    n_copy(2).start()
    n_copy(1).start()
    start(over_x(1))
    start(over_x(2))
    for piece in range(PARTS):
        wo_x(piece, me, piece, wo_hbm.at[rows(piece)]).start()
    for piece in range(PARTS):
        wo_mate(0, me, piece, wo_hbm.at[rows(piece)]).start()
    wo_own = pltpu.make_async_copy(wo_hbm, wfull_hbm.at[me], o_own)
    wo_own.start()

    id_own.wait()
    for slot in range(7):
        id_copy(slot, others[slot]).wait_recv()
    order = lax.broadcasted_iota(jnp.int32, (tok, tok), 0) < lax.broadcasted_iota(jnp.int32, (tok, tok), 1)
    earlier = jnp.where(order, 1.0, 0.0).astype(jnp.bfloat16)
    experts = slots_ref.shape[1]
    spot = lax.broadcasted_iota(jnp.int32, (experts, tok), 0)
    local = experts // 2
    wanted = jnp.where(spot < local, me * local + spot, (mate - 1) * local + spot)

    def table(source, c):
        count = jnp.zeros((experts, tok), jnp.float32)
        for j in range(ids_buf.shape[1]):
            count = count + jnp.where(ids_buf[source, j:j + 1, :] == wanted, 1.0, 0.0)
        before = jnp.dot(count.astype(jnp.bfloat16), earlier, preferred_element_type=jnp.float32)
        slots_ref[source] = jnp.where(count > 0.0, before, -1.0)
        ids_ref[source] = ids_buf[source]
        return c

    lax.fori_loop(0, ids_buf.shape[0], table, 0)

    def arrive_x(m):
        landed(m, x_dev)
        landed_mate(m, 0)
        start(forward_y(m))
        to_mate(m, 0).start()

    def finish(m):
        landed_mate(m, 1)
        to_mate(m, 1).start()
        landed_mate(m, 2)
        to_mate(m, 2).start()
        local_w(m).wait()
        for source in (y_dev, dg_dev, mate, x_mate, yn * CORES + 1 - core, dg * CORES + 1 - core):
            landed(m, source)

    width = 256

    def project(m):
        def run(i, c):
            slot, n = i // (group // width), lax.rem(i, group // width)
            at = pl.ds(pl.multiple_of(n * width, width), width)
            out = jnp.dot(nbuf[slot], wbuf[m, :, :, at].reshape(dim, width), preferred_element_type=jnp.float32)
            qkv[m, slot, :, at] = out.astype(jnp.bfloat16)
            return c

        lax.fori_loop(0, seqs * (group // width), run, 0)

    arrive_x(0)
    start(over_y(2))
    n_copy(2).wait_recv()
    n_copy(3).start()
    finish(0)
    n_copy(1).wait_recv()
    n_copy(3).wait_recv()
    project(0)
    arrive_x(1)
    arrive_x(2)
    for slot, piece in enumerate((3, 0, 1, 2)):
        wo_y(slot, me, piece, wo_hbm.at[rows(piece)]).start()
    finish(1)
    project(1)
    finish(2)
    project(2)

    scale = 128 ** -0.5
    block = tok // 2
    pairs = group // 256

    def c_copy(slot, pair):
        at = pl.ds(pl.multiple_of(pair * 256, 256), 256)
        there = pl.ds(pl.multiple_of((2 * side + core) * group + pair * 256, 256), 256)
        src, dst = cbuf.at[slot, :, at], ctx_hbm.at[:, there]
        if slot == 0:
            return pltpu.make_async_copy(src, dst, c_own.at[pair])
        return remote(src, dst, c_send.at[slot - 1, pair], c_recv.at[slot - 1, pair], (mate, x_dev, x_mate)[slot - 1])

    def heads(pair, carry):
        def one_seq(slot, c):
            for h in range(2):
                at = pl.ds(pl.multiple_of(pair * 256 + h * 128, 128), 128)
                keys, values = qkv[1, slot, :, at], qkv[2, slot, :, at]
                for b in range(2):
                    query = qkv[0, slot, b * block:(b + 1) * block, at]
                    span = (b + 1) * block
                    s = lax.dot_general(query, keys[:span], (((1,), (1,)), ((), ())), preferred_element_type=jnp.float32) * scale
                    row = lax.broadcasted_iota(jnp.int32, (block, span), 0) + b * block
                    s = jnp.where(row >= lax.broadcasted_iota(jnp.int32, (block, span), 1), s, -jnp.inf)
                    e = jnp.exp(s - jnp.max(s, axis=-1, keepdims=True))
                    p = (e * (1.0 / jnp.sum(e, axis=-1, keepdims=True))).astype(jnp.bfloat16)
                    cbuf[slot, b * block:(b + 1) * block, at] = jnp.dot(p, values[:span], preferred_element_type=jnp.float32).astype(jnp.bfloat16)
            return c

        lax.fori_loop(0, seqs, one_seq, 0)
        for slot in (2, 3, 1, 0):
            c_copy(slot, pair).start()

        @pl.when(pair == 1)
        def _():
            for piece in range(PARTS):
                wo_landed(x_dev, piece)
                wo_mate(1, x_dev, piece, wfull_hbm.at[x_dev, rows(piece)]).start()
                if piece < 3:
                    wo_y(4 + piece, x_dev, piece, wfull_hbm.at[x_dev, rows(piece)]).start()

        return carry

    lax.fori_loop(0, pairs, heads, 0)
    for piece in (3, 0, 1, 2):
        wo_landed(y_dev, piece)
        wo_mate(2, y_dev, piece, wfull_hbm.at[y_dev, rows(piece)]).start()
        if piece == 3:
            wo_x(4, y_dev, piece, wfull_hbm.at[y_dev, rows(piece)]).start()
    for piece in (0, 1, 2, 3):
        wo_landed(dg_dev, piece)
        wo_mate(3, dg_dev, piece, wfull_hbm.at[dg_dev, rows(piece)]).start()
    for slot in range(1, 4):
        for pair in range(PARTS):
            at = pl.ds(pair * 256, 256)
            remote(cbuf.at[0, :, at], ctx_hbm.at[:, at], c_send.at[slot - 1, pair], c_recv.at[slot - 1, pair], mate).wait_recv()
    for source in (mate, x_mate, yn * CORES + 1 - core, dg * CORES + 1 - core):
        for piece in range(PARTS):
            wo_landed(source, piece)
    for slot in range(7):
        id_copy(slot, me).wait_send()
    for m in range(3):
        own_mate(m).wait_send()
        for copy in over_x(m) + over_y(m) + forward_y(m):
            copy.wait_send()
        for slot in range(3):
            to_mate(m, slot).wait_send()
    for slot in range(1, 4):
        n_copy(slot).wait_send()
    for pair in range(PARTS):
        c_copy(0, pair).wait()
        for slot in range(1, 4):
            c_copy(slot, pair).wait_send()
    wo_own.wait()
    for slot in range(5):
        wo_x(slot, me, 0, wo_hbm.at[rows(0)]).wait_send()
    for slot in range(7):
        wo_y(slot, me, 0, wo_hbm.at[rows(0)]).wait_send()
    for order in range(PARTS):
        for piece in range(PARTS):
            wo_mate(order, me, piece, wo_hbm.at[rows(piece)]).wait_send()


def attend(tokens, ids, w_query, w_key, w_value, w_out):
    tok, dim = tokens.shape
    depth, width = w_query.shape
    devices, group = 8, width // 4
    dma = pltpu.SemaphoreType.DMA
    return pl.pallas_call(
        attend_kernel,
        out_shape=(jax.ShapeDtypeStruct((tok, width), jnp.bfloat16), jax.ShapeDtypeStruct((devices,) + w_out.shape, jnp.bfloat16), jax.ShapeDtypeStruct((devices, 32, tok), jnp.float32), jax.ShapeDtypeStruct((devices,) + ids.shape, jnp.int32)),
        in_specs=[WHOLE] + [ANY] * 5,
        out_specs=(ANY, ANY, WHOLE, WHOLE),
        scratch_shapes=[
            pltpu.VMEM((devices,) + ids.shape, jnp.int32), dma((7,)), dma((devices,)), dma,
            pltpu.VMEM((4, tok, dim), jnp.bfloat16),
            pltpu.VMEM((3, devices, depth, group), jnp.bfloat16),
            pltpu.VMEM((3, 3, depth, group), jnp.bfloat16),
            pltpu.VMEM((3, 4, tok, group), jnp.bfloat16),
            pltpu.VMEM((4, tok, group), jnp.bfloat16),
            dma((3,)), dma((3, 2)), dma((3, 2)), dma((3, 2)), dma((3,)), dma((3, 3)), dma((3, devices)), dma((3, 3)),
            dma((4,)), dma((4,)), dma((3, 4)), dma((3, 4)), dma((4,)),
            dma((5,)), dma((7,)), dma((4, 4)), dma((devices, 4)), dma,
        ],
        compiler_params=pltpu.CompilerParams(collective_id=3, has_side_effects=True, vmem_limit_bytes=VMEM_MAX),
        name='attend_heads',
    )(tokens, ids, w_query, w_key, w_value, w_out)


def spread_kernel(u_hbm, g_hbm, slot_ref, x_hbm, gall_hbm, ubuf, hbuf, xbuf, own_sem, gown_sem, out_sem, x_send, y_send, d_send, recv, g_send, g_recv):
    me, core, chip, xn, yn, dg = neighbours()
    mate = me + 1 - 2 * core
    tok = ubuf.shape[1]
    part = tok // 4
    local_experts = slot_ref.shape[1] // 2
    x_dev, y_dev, dg_dev = xn * CORES + core, yn * CORES + core, dg * CORES + core
    others = (x_dev, y_dev, mate, dg_dev, xn * CORES + 1 - core, yn * CORES + 1 - core, dg * CORES + 1 - core)
    greet(others)

    def rows(piece):
        return pl.ds(piece * part, part)

    def landed(source, piece):
        remote(ubuf.at[source, rows(piece)], ubuf.at[source, rows(piece)], d_send.at[0, 0], recv.at[source, piece], mate).wait_recv()

    def pass_on(order, source, piece):
        return remote(ubuf.at[source, rows(piece)], ubuf.at[source, rows(piece)], d_send.at[order, piece], recv.at[source, piece], mate)

    def across_x(slot, source, piece, src):
        return remote(src, ubuf.at[source, rows(piece)], x_send.at[slot], recv.at[source, piece], x_dev)

    def across_y(slot, source, piece, src):
        return remote(src, ubuf.at[source, rows(piece)], y_send.at[slot], recv.at[source, piece], y_dev)

    own = pltpu.make_async_copy(u_hbm, ubuf.at[me], own_sem)
    own.start()
    gown = pltpu.make_async_copy(g_hbm, gall_hbm.at[me], gown_sem)
    gown.start()
    for slot in range(PARTS):
        across_x(slot, me, slot, u_hbm.at[rows(slot)]).start()
        across_y(slot, me, (slot + 2) % 4, u_hbm.at[rows((slot + 2) % 4)]).start()
    for piece in range(PARTS):
        remote(u_hbm.at[rows(piece)], ubuf.at[me, rows(piece)], d_send.at[0, piece], recv.at[me, piece], mate).start()
    for slot, device in enumerate(others):
        remote(g_hbm, gall_hbm.at[me], g_send.at[slot], g_recv.at[me], device).start()
    own.wait()

    def out_copy(order, source):
        return pltpu.make_async_copy(xbuf.at[lax.rem(order, 2)], x_hbm.at[:, source], out_sem.at[lax.rem(order, 2)])

    def step(order, carry):
        kind = order // 2
        base = jnp.where(kind == 0, chip, jnp.where(kind == 1, xn, jnp.where(kind == 2, yn, dg)))
        odd = lax.rem(order, 2)
        source = base * 2 + core + odd * (1 - 2 * core)

        @pl.when(order == 2)
        def _():
            for piece in (0, 1):
                landed(x_dev, piece)
                across_y(4 + piece, x_dev, piece, ubuf.at[x_dev, rows(piece)]).start()
                pass_on(1, x_dev, piece).start()
                landed(y_dev, piece + 2)
                across_x(4 + piece, y_dev, piece + 2, ubuf.at[y_dev, rows(piece + 2)]).start()
                pass_on(2, y_dev, piece + 2).start()
            for piece in (0, 1):
                landed(x_dev, piece + 2)
                pass_on(1, x_dev, piece + 2).start()
                landed(y_dev, piece)
                pass_on(2, y_dev, piece).start()

        @pl.when(order == 6)
        def _():
            for piece in (0, 2, 1, 3):
                landed(dg_dev, piece)
                pass_on(3, dg_dev, piece).start()

        @pl.when(odd == 1)
        def _():
            for piece in range(PARTS):
                landed(source, piece)

        @pl.when(order >= 2)
        def _():
            out_copy(order, source).wait()

        spot = lax.broadcasted_iota(jnp.int32, (CAP, tok), 0).astype(jnp.float32)
        for expert in range(local_experts):
            hit = slot_ref[source, expert:expert + 1, :] == spot
            hbuf[expert * CAP:(expert + 1) * CAP, :] = jnp.where(hit, 1.0, 0.0).astype(jnp.bfloat16)
        width = 256

        def tile(n, c):
            cols = pl.ds(pl.multiple_of(n * width, width), width)
            picked = jnp.dot(hbuf[...], ubuf[source, :, cols], preferred_element_type=jnp.float32)
            xbuf[odd, :, :, cols] = picked.astype(jnp.bfloat16).reshape(local_experts, CAP, width)
            return c

        lax.fori_loop(0, ubuf.shape[2] // width, tile, 0)
        out_copy(order, source).start()
        return carry

    lax.fori_loop(0, 8, step, 0)
    out_copy(0, me).wait()
    out_copy(1, me).wait()
    gown.wait()
    for slot in range(PARTS):
        across_x(slot, me, slot, u_hbm.at[rows(slot)]).wait_send()
        across_y(slot, me, slot, u_hbm.at[rows(slot)]).wait_send()
    for piece in (0, 1):
        across_y(4 + piece, x_dev, piece, ubuf.at[x_dev, rows(piece)]).wait_send()
        across_x(4 + piece, y_dev, piece + 2, ubuf.at[y_dev, rows(piece + 2)]).wait_send()
    for order, source in enumerate((me, x_dev, y_dev, dg_dev)):
        for piece in range(PARTS):
            pass_on(order, source, piece).wait_send()
    for slot, device in enumerate(others):
        remote(g_hbm, gall_hbm.at[me], g_send.at[slot], g_recv.at[me], device).wait_send()
        remote(g_hbm, gall_hbm.at[device], g_send.at[slot], g_recv.at[device], device).wait_recv()


def spread(u, gates, slots):
    devices, pair_experts, tok = slots.shape
    local_experts = pair_experts // 2
    dim = u.shape[1]
    return pl.pallas_call(
        spread_kernel,
        out_shape=(jax.ShapeDtypeStruct((local_experts, devices, CAP, dim), jnp.bfloat16), jax.ShapeDtypeStruct((devices,) + gates.shape, jnp.float32)),
        in_specs=[ANY, ANY, WHOLE],
        out_specs=(ANY, ANY),
        scratch_shapes=[
            pltpu.VMEM((devices, tok, dim), jnp.bfloat16),
            pltpu.VMEM((local_experts * CAP, tok), jnp.bfloat16),
            pltpu.VMEM((2, local_experts, CAP, dim), jnp.bfloat16),
            pltpu.SemaphoreType.DMA, pltpu.SemaphoreType.DMA, pltpu.SemaphoreType.DMA((2,)),
            pltpu.SemaphoreType.DMA((6,)), pltpu.SemaphoreType.DMA((6,)), pltpu.SemaphoreType.DMA((4, 4)),
            pltpu.SemaphoreType.DMA((devices, 4)), pltpu.SemaphoreType.DMA((7,)), pltpu.SemaphoreType.DMA((devices,)),
        ],
        compiler_params=pltpu.CompilerParams(collective_id=1, has_side_effects=True, vmem_limit_bytes=VMEM_MAX),
        name='spread_rows',
    )(u, gates, slots)


def ffn_kernel(units_ref, x_ref, w1_hbm, w3_hbm, w2_hbm, o_ref, packed, middle, done, w1_buf, w3_buf, w2_buf, w_sem):
    expert = pl.program_id(0)
    last = pl.num_programs(0)
    devices = x_ref.shape[1]
    depth = w1_buf.shape[0]
    ahead = depth - 1

    def fetch(e):
        slot = lax.rem(e, depth)
        moves = ((w1_hbm, w1_buf), (w3_hbm, w3_buf), (w2_hbm, w2_buf))
        return [pltpu.make_async_copy(src.at[e], dst.at[slot], w_sem.at[slot, i]) for i, (src, dst) in enumerate(moves)]

    @pl.when(expert == 0)
    def _():
        for e in range(ahead):
            start(fetch(e))
        packed[...] = jnp.zeros_like(packed)
        done[...] = jnp.zeros_like(done)

    @pl.when(expert + ahead < last)
    def _():
        start(fetch(expert + ahead))

    begins, counts = [], [units_ref[expert * devices + source] * UNIT for source in range(devices)]
    total = 0
    for source in range(devices):
        begins.append(pl.multiple_of(total, UNIT))
        packed[pl.ds(begins[-1], CAP), :] = x_ref[0, source]
        total = total + counts[source]
    for copy in fetch(expert):
        copy.wait()
    slot = lax.rem(expert, depth)
    small, big = LANES, TILE

    def run(begin, size):
        rows = pl.ds(pl.multiple_of(begin, small), size)
        for at in strips(w1_buf.shape[2], TILE):
            first = jnp.dot(packed[rows, :], w1_buf[slot, :, at], preferred_element_type=jnp.float32)
            third = jnp.dot(packed[rows, :], w3_buf[slot, :, at], preferred_element_type=jnp.float32)
            middle[:size, at] = (first * jax.nn.sigmoid(first) * third).astype(jnp.bfloat16)
        for at in strips(w2_buf.shape[2], 2 * TILE):
            done[rows, at] = jnp.dot(middle[:size], w2_buf[slot, :, at], preferred_element_type=jnp.float32).astype(jnp.bfloat16)

    full = (total + small - 1) // big

    def run_big(t, c):
        run(t * big, big)
        return c

    lax.fori_loop(0, full, run_big, 0)

    @pl.when(full * big < total)
    def _():
        run(full * big, small)

    spot = lax.broadcasted_iota(jnp.int32, (CAP, o_ref.shape[3]), 0)
    for source in range(devices):
        o_ref[0, source] = jnp.where(spot < counts[source], done[pl.ds(begins[source], CAP), :], jnp.zeros((), jnp.bfloat16))


def expert_ffn(units, x, w_one, w_three, w_two):
    experts, devices, _, dim = x.shape
    mid = w_one.shape[2]
    depth = 3
    block = pl.BlockSpec((1, devices, CAP, dim), lambda e, units: (e, 0, 0, 0))
    ring = [pltpu.VMEM((depth,) + w.shape[1:], jnp.bfloat16) for w in (w_one, w_three, w_two)]
    lines = pltpu.VMEM(((devices + 1) * CAP, dim), jnp.bfloat16)
    return pl.pallas_call(
        ffn_kernel,
        out_shape=jax.ShapeDtypeStruct(x.shape, jnp.bfloat16),
        grid_spec=pltpu.PrefetchScalarGridSpec(
            num_scalar_prefetch=1,
            grid=(experts,),
            in_specs=[block] + [ANY] * 3,
            out_specs=block,
            scratch_shapes=[lines, pltpu.VMEM((TILE, mid), jnp.bfloat16), lines] + ring + [pltpu.SemaphoreType.DMA((depth, 3))],
        ),
        compiler_params=pltpu.CompilerParams(dimension_semantics=('arbitrary',), vmem_limit_bytes=VMEM_MAX),
        name='expert_mlp',
    )(units, x, w_one, w_three, w_two)


def combine_kernel(o_hbm, slots_ref, ids_ref, gates_ref, h_hbm, y_ref, own, mate_rows, gate_tab, gate3, p_one, r_one, p_two, r_two, p_last, r_last, own_sem, h_sem, mate_send, mate_recv, one_send, one_recv, two_send, two_recv, last_send, last_recv):
    me, core, chip, xn, yn, dg = neighbours()
    mate = me + 1 - CORES * core
    near = xn + core * (yn - xn)
    far = yn + core * (xn - yn)
    near_dev, far_dev = near * CORES + core, far * CORES + core
    half = own.shape[3]
    rows_n = p_one.shape[1]
    experts = own.shape[1]
    greet((near_dev, far_dev, mate))
    my_cols = pl.ds(pl.multiple_of(core * half, half), half)
    mate_cols = pl.ds(pl.multiple_of((1 - core) * half, half), half)
    spot = lax.broadcasted_iota(jnp.int32, gate_tab.shape, 0)
    wanted = jnp.where(spot < experts, me * experts + spot, (mate - 1) * experts + spot)

    def dest(i, first, second, front):
        pair, odd = i // CORES, lax.rem(i, CORES)
        base = jnp.where(pair == 0, dg, jnp.where(pair == 1, first, jnp.where(pair == 2, second, chip)))
        return base * CORES + jnp.where(pair < 3, odd, front + odd * (1 - CORES * front))

    def my_dest(i):
        return dest(i, near, far, 1 - core)

    def to_mate(i):
        return remote(o_hbm.at[:, dest(i, far, near, core), :, mate_cols], mate_rows.at[i], mate_send.at[i], mate_recv.at[i], mate)

    def own_copy(i):
        slot = lax.rem(i, CORES)
        return pltpu.make_async_copy(o_hbm.at[:, my_dest(i), :, my_cols], own.at[slot], own_sem.at[slot])

    def one_copy(n):
        return remote(p_one.at[n], r_one.at[n], one_send.at[n], one_recv.at[n], near_dev)

    def two_copy(n):
        return remote(p_two.at[n], r_two.at[n], two_send.at[n], two_recv.at[n], far_dev)

    def last_copy(n):
        return remote(p_last.at[n], r_last.at[n], last_send.at[n], last_recv.at[n], mate)

    own_copy(0).start()
    for i in range(8):
        to_mate(i).start()
    residual = pltpu.make_async_copy(h_hbm, y_ref, h_sem)
    residual.start()

    def open_dest(i):
        gate = jnp.zeros(gate_tab.shape, jnp.float32)
        target = my_dest(i)
        for j in range(ids_ref.shape[1]):
            gate = gate + jnp.where(ids_ref[target, j:j + 1, :] == wanted, gates_ref[target, j:j + 1, :], 0.0)
        gate_tab[...] = gate
        own_copy(i).wait()
        to_mate(i).wait_recv()

        @pl.when(i < 7)
        def _():
            own_copy(i + 1).start()

    def weights(i, part):
        target = my_dest(i)
        cols = pl.ds(pl.multiple_of(part * rows_n, rows_n), rows_n)
        line = lax.broadcasted_iota(jnp.int32, (2 * CAP, rows_n), 0)
        low = line < CAP
        place = (line - jnp.where(low, 0, CAP)).astype(jnp.float32)
        for pair, where in enumerate(strips(gate3.shape[1], 2 * CAP)):
            one, two = slice(2 * pair, 2 * pair + 1), slice(2 * pair + 1, 2 * pair + 2)
            hit = jnp.where(low, slots_ref[target, one, cols], slots_ref[target, two, cols]) == place
            rest = jnp.where(hit, jnp.where(low, gate_tab[one, cols], gate_tab[two, cols]), 0.0).T
            for rows in strips(gate3.shape[0], rows_n):
                term = rest.astype(jnp.bfloat16)
                gate3[rows, where] = term
                rest = rest - term.astype(jnp.float32)

    def products(i, part, sink):
        @pl.when(part == 0)
        def _():
            open_dest(i)

        weights(i, part)
        slot = lax.rem(i, CORES)
        depth = experts * CAP

        def tile(n, c):
            cols = pl.ds(pl.multiple_of(n * TILE, TILE), TILE)
            mine = own[slot, :, :, cols].reshape(depth, TILE)
            other = mate_rows[i, :, :, cols].reshape(depth, TILE)
            out = jnp.dot(gate3[:, :depth], mine, preferred_element_type=jnp.float32) + jnp.dot(gate3[:, depth:], other, preferred_element_type=jnp.float32)
            sink[:, cols] = sum(out[rows] for rows in strips(out.shape[0], rows_n))
            return c

        lax.fori_loop(0, half // TILE, tile, 0)

    lead, pair_n, part_n = p_one.shape[0], p_two.shape[0], p_two.shape[0] // CORES

    def phase_one(step, c):
        products(step // part_n, lax.rem(step, part_n), p_one.at[step])
        one_copy(step).start()
        return c

    lax.fori_loop(0, lead, phase_one, 0)

    def phase_two(step, c):
        products(4 + step // part_n, lax.rem(step, part_n), p_two.at[step])
        one_copy(step).wait_recv()
        p_two[step] = p_two[step] + r_one[step]
        two_copy(step).start()
        return c

    lax.fori_loop(0, pair_n, phase_two, 0)
    residual.wait()

    def phase_three(step, c):
        part = lax.rem(step, part_n)
        products(6 + step // part_n, part, p_last.at[step])
        n = jnp.where(step < part_n, 1 - core, core) * part_n + part
        one_copy(pair_n + n).wait_recv()
        two_copy(n).wait_recv()
        p_last[step] = p_last[step] + (r_one[pair_n + n] + r_two[n])

        @pl.when(step < part_n)
        def _():
            last_copy(step).start()

        @pl.when(step >= part_n)
        def _():
            rows = pl.ds(pl.multiple_of(part * rows_n, rows_n), rows_n)
            y_ref[rows, my_cols] = (y_ref[rows, my_cols].astype(jnp.float32) + p_last[step]).astype(jnp.bfloat16)

        return c

    lax.fori_loop(0, pair_n, phase_three, 0)
    for n in range(part_n):
        rows = pl.ds(n * rows_n, rows_n)
        last_copy(n).wait_recv()
        y_ref[rows, mate_cols] = (y_ref[rows, mate_cols].astype(jnp.float32) + r_last[n]).astype(jnp.bfloat16)
    finish_send(to_mate(n) for n in range(8))
    finish_send(one_copy(n) for n in range(lead))
    finish_send(two_copy(n) for n in range(pair_n))
    finish_send(last_copy(n) for n in range(part_n))


def combine(done, slots, ids, gates, hidden):
    experts, devices, _, dim = done.shape
    tok = hidden.shape[0]
    half, part = dim // CORES, tok // PARTS
    pair_n = CORES * PARTS
    dma = pltpu.SemaphoreType.DMA
    floats = lambda n: pltpu.VMEM((n, part, half), jnp.float32)
    rows = lambda n: pltpu.VMEM((n, experts, CAP, half), jnp.bfloat16)
    sizes = [CORES * pair_n, CORES * pair_n, pair_n, pair_n, pair_n, PARTS]
    sems = [dma((n,)) for n in (devices, devices, 2 * pair_n, 2 * pair_n, pair_n, pair_n, PARTS, PARTS)]
    return pl.pallas_call(
        combine_kernel,
        out_shape=jax.ShapeDtypeStruct((tok, dim), jnp.bfloat16),
        in_specs=[ANY, WHOLE, WHOLE, WHOLE, ANY],
        out_specs=WHOLE,
        scratch_shapes=[rows(CORES), rows(devices), pltpu.VMEM(slots.shape[1:], jnp.float32), pltpu.VMEM((3 * part, CORES * experts * CAP), jnp.bfloat16)] + [floats(n) for n in sizes] + [dma((CORES,)), dma] + sems,
        compiler_params=pltpu.CompilerParams(collective_id=2, has_side_effects=True, vmem_limit_bytes=VMEM_MAX),
        name='combine_rows',
    )(done, slots, ids, gates, hidden)


def solution(mesh):
    tok_spec = P(('dp', 'ep'))
    row_spec = P('ep')

    def local_layer(tokens, w_query, w_key, w_value, w_out, w_router, w_one, w_three, w_two, expert_ids):
        seq_count, seq_len, model_dim = tokens.shape
        choices = expert_ids.shape[2]
        local_experts = w_one.shape[0]
        tok_count = seq_count * seq_len
        ids_t = expert_ids.reshape(tok_count, choices).T
        flat = tokens.reshape(tok_count, model_dim)
        w_flat = [w.reshape(w.shape[0], -1) for w in (w_query, w_key, w_value)]
        context, full_out, slot, all_ids = attend(flat, ids_t, *w_flat, w_out)
        units = ((jnp.max(slot[:, :local_experts], axis=2).astype(jnp.int32) + UNIT) // UNIT).T.reshape(-1)
        mixed = jnp.dot(context, full_out.reshape(-1, model_dim), preferred_element_type=jnp.float32)
        hidden = (flat.astype(jnp.float32) + mixed).astype(jnp.bfloat16)
        normed, gates = router_gates(hidden, w_router, ids_t)
        x, all_gates = spread(normed, gates, slot)
        done = expert_ffn(units, x, w_one, w_three, w_two)
        layer_out = combine(done, slot, all_ids, all_gates, hidden)
        return layer_out.reshape(seq_count, seq_len, model_dim)

    return jax.shard_map(local_layer, mesh=mesh, in_specs=(tok_spec, row_spec, row_spec, row_spec, row_spec, P(), row_spec, row_spec, row_spec, tok_spec), out_specs=tok_spec, check_vma=False)
```

```python
import functools

import jax
import jax.numpy as jnp
from jax import lax
from jax.experimental import pallas as pl
from jax.experimental.pallas import tpu as pltpu
from jax.sharding import PartitionSpec as P

EPS = 1e-6
CAP = 64
UNIT = 16
VMEM_MAX = 67043328
LANES = 128
TILE = 256
CORES = 2
PARTS = 4
ANY = pl.BlockSpec(memory_space=pl.ANY)
WHOLE = pl.BlockSpec(memory_space=pltpu.VMEM)


def strips(size, width):
    return [slice(at, at + width) for at in range(0, size, width)]


def start(copies):
    for copy in copies:
        copy.start()


def finish_send(copies):
    for copy in copies:
        copy.wait_send()


def neighbours():
    me = lax.axis_index('ep')
    core, chip = lax.rem(me, 2), me // 2
    side, up = lax.rem(chip, 2), chip // 2
    return me, core, chip, 1 - side + 2 * up, side + 2 * (1 - up), 3 - chip


def greet(devices):
    barrier = pltpu.get_barrier_semaphore()
    for device in devices:
        pl.semaphore_signal(barrier, inc=1, device_id={'ep': device}, device_id_type=pl.DeviceIdType.MESH)
    pl.semaphore_wait(barrier, len(devices))


def remote(src, dst, send_sem, recv_sem, device):
    return pltpu.make_async_remote_copy(src_ref=src, dst_ref=dst, send_sem=send_sem, recv_sem=recv_sem, device_id={'ep': device}, device_id_type=pl.DeviceIdType.MESH)


def attend_kernel(tok_ref, ids_hbm, wq_hbm, wk_hbm, wv_hbm, wo_hbm, h_hbm, u_hbm, wfull_hbm, slots_ref, ids_ref, ctx, total, out_sem, ring_sem, ids_buf, i_send, i_recv, i_own, nbuf, wbuf, wmate, qkv, cbuf, loc_sem, a_send, b_send, f_send, m_send, mf_send, w_recv, wm_recv, n_send, n_recv, c_send, c_recv, c_own, ox_send, oy_send, od_send, o_recv, o_own):
    me, core, chip, xn, yn, dg = neighbours()
    side = lax.rem(chip, 2)
    mate = me + 1 - 2 * core
    x_dev, y_dev, dg_dev, x_mate = xn * CORES + core, yn * CORES + core, dg * CORES + core, xn * CORES + 1 - core
    weights = (wq_hbm, wk_hbm, wv_hbm)
    seqs, tok, dim = nbuf.shape
    group = wbuf.shape[3]
    part = tok // 4
    others = (x_dev, y_dev, mate, x_mate, dg_dev, yn * CORES + 1 - core, dg * CORES + 1 - core)
    greet(others)

    def cols(on_side, on_core):
        return pl.ds(pl.multiple_of((2 * on_side + on_core) * group, group), group)

    def local_w(m):
        return pltpu.make_async_copy(weights[m].at[:, cols(side, core)], wbuf.at[m, me], loc_sem.at[m])

    def own_mate(m):
        return remote(weights[m].at[:, cols(side, 1 - core)], wbuf.at[m, me], m_send.at[m], w_recv.at[m, me], mate)

    def over_x(m):
        return (remote(weights[m].at[:, cols(1 - side, core)], wbuf.at[m, me], a_send.at[m, 0], w_recv.at[m, me], x_dev),
                remote(weights[m].at[:, cols(1 - side, 1 - core)], wmate.at[m, 0], a_send.at[m, 1], wm_recv.at[m, 0], x_dev))

    def over_y(m):
        return (remote(weights[m].at[:, cols(side, core)], wbuf.at[m, me], b_send.at[m, 0], w_recv.at[m, me], y_dev),
                remote(weights[m].at[:, cols(side, 1 - core)], wmate.at[m, 1], b_send.at[m, 1], wm_recv.at[m, 1], y_dev))

    def forward_y(m):
        return (remote(wbuf.at[m, x_dev], wbuf.at[m, x_dev], f_send.at[m, 0], w_recv.at[m, x_dev], y_dev),
                remote(wmate.at[m, 0], wmate.at[m, 2], f_send.at[m, 1], wm_recv.at[m, 2], y_dev))

    def to_mate(m, slot):
        source = (x_dev, y_dev, dg_dev)[slot]
        return remote(wmate.at[m, slot], wbuf.at[m, source], mf_send.at[m, slot], w_recv.at[m, source], mate)

    def landed(m, source):
        remote(wbuf.at[m, source], wbuf.at[m, source], m_send.at[m], w_recv.at[m, source], mate).wait_recv()

    def landed_mate(m, slot):
        to = wmate.at[m, slot]
        remote(to, to, m_send.at[m], wm_recv.at[m, slot], mate).wait_recv()

    def n_copy(slot):
        source, device = (0, 0, 0, 2)[slot], (mate, mate, x_dev, mate)[slot]
        return remote(nbuf.at[source], nbuf.at[slot], n_send.at[slot], n_recv.at[slot], device)

    def id_copy(slot, owner):
        return remote(ids_hbm, ids_buf.at[owner], i_send.at[slot], i_recv.at[owner], others[slot])

    def rows(piece):
        return pl.ds(piece * part, part)

    def wo_x(slot, source, piece, src):
        return remote(src, wfull_hbm.at[source, rows(piece)], ox_send.at[slot], o_recv.at[source, piece], x_dev)

    def wo_y(slot, source, piece, src):
        return remote(src, wfull_hbm.at[source, rows(piece)], oy_send.at[slot], o_recv.at[source, piece], y_dev)

    def wo_mate(order, source, piece, src):
        return remote(src, wfull_hbm.at[source, rows(piece)], od_send.at[order, piece], o_recv.at[source, piece], mate)

    def wo_landed(source, piece):
        to = wfull_hbm.at[source, rows(piece)]
        remote(to, to, od_send.at[0, 0], o_recv.at[source, piece], mate).wait_recv()

    for slot in range(7):
        id_copy(slot, me).start()
    id_own = pltpu.make_async_copy(ids_hbm, ids_buf.at[me], i_own)
    id_own.start()
    start(over_x(0))
    start(over_y(0))
    for m in range(3):
        local_w(m).start()
        own_mate(m).start()
    start(over_y(1))
    wide = tok_ref[...].astype(jnp.float32)
    nbuf[0] = (wide * lax.rsqrt(jnp.mean(wide * wide, axis=-1, keepdims=True) + EPS)).astype(jnp.bfloat16)
    n_copy(2).start()
    n_copy(1).start()
    start(over_x(1))
    start(over_x(2))
    for piece in range(PARTS):
        wo_x(piece, me, piece, wo_hbm.at[rows(piece)]).start()
    for piece in range(PARTS):
        wo_mate(0, me, piece, wo_hbm.at[rows(piece)]).start()
    wo_own = pltpu.make_async_copy(wo_hbm, wfull_hbm.at[me], o_own)
    wo_own.start()

    id_own.wait()
    for slot in range(7):
        id_copy(slot, others[slot]).wait_recv()
    order = lax.broadcasted_iota(jnp.int32, (tok, tok), 0) < lax.broadcasted_iota(jnp.int32, (tok, tok), 1)
    earlier = jnp.where(order, 1.0, 0.0).astype(jnp.bfloat16)
    experts = slots_ref.shape[1]
    spot = lax.broadcasted_iota(jnp.int32, (experts, tok), 0)
    local = experts // 2
    wanted = jnp.where(spot < local, me * local + spot, (mate - 1) * local + spot)

    def table(source, c):
        count = jnp.zeros((experts, tok), jnp.float32)
        for j in range(ids_buf.shape[1]):
            count = count + jnp.where(ids_buf[source, j:j + 1, :] == wanted, 1.0, 0.0)
        before = jnp.dot(count.astype(jnp.bfloat16), earlier, preferred_element_type=jnp.float32)
        slots_ref[source] = jnp.where(count > 0.0, before, -1.0)
        ids_ref[source] = ids_buf[source]
        return c

    lax.fori_loop(0, ids_buf.shape[0], table, 0)

    def arrive_x(m):
        landed(m, x_dev)
        landed_mate(m, 0)
        start(forward_y(m))
        to_mate(m, 0).start()

    def finish(m):
        landed_mate(m, 1)
        to_mate(m, 1).start()
        landed_mate(m, 2)
        to_mate(m, 2).start()
        local_w(m).wait()
        for source in (y_dev, dg_dev, mate, x_mate, yn * CORES + 1 - core, dg * CORES + 1 - core):
            landed(m, source)

    width = 256

    def project(m):
        def run(i, c):
            slot, n = i // (group // width), lax.rem(i, group // width)
            at = pl.ds(pl.multiple_of(n * width, width), width)
            out = jnp.dot(nbuf[slot], wbuf[m, :, :, at].reshape(dim, width), preferred_element_type=jnp.float32)
            qkv[m, slot, :, at] = out.astype(jnp.bfloat16)
            return c

        lax.fori_loop(0, seqs * (group // width), run, 0)

    arrive_x(0)
    start(over_y(2))
    n_copy(2).wait_recv()
    n_copy(3).start()
    finish(0)
    n_copy(1).wait_recv()
    n_copy(3).wait_recv()
    project(0)
    arrive_x(1)
    arrive_x(2)
    for slot, piece in enumerate((3, 0, 1, 2)):
        wo_y(slot, me, piece, wo_hbm.at[rows(piece)]).start()
    finish(1)
    project(1)
    finish(2)
    project(2)

    scale = 128 ** -0.5
    block = tok // 2
    pairs = group // 256

    def c_copy(slot, pair):
        at = pl.ds(pl.multiple_of(pair * 256, 256), 256)
        there = pl.ds(pl.multiple_of((2 * side + core) * group + pair * 256, 256), 256)
        src, dst = cbuf.at[slot, :, at], ctx.at[:, there]
        if slot == 0:
            return pltpu.make_async_copy(src, dst, c_own.at[pair])
        return remote(src, dst, c_send.at[slot - 1, pair], c_recv.at[slot - 1, pair], (mate, x_dev, x_mate)[slot - 1])

    def heads(pair, carry):
        def one_seq(slot, c):
            for h in range(2):
                at = pl.ds(pl.multiple_of(pair * 256 + h * 128, 128), 128)
                keys, values = qkv[1, slot, :, at], qkv[2, slot, :, at]
                for b in range(2):
                    query = qkv[0, slot, b * block:(b + 1) * block, at]
                    span = (b + 1) * block
                    s = lax.dot_general(query, keys[:span], (((1,), (1,)), ((), ())), preferred_element_type=jnp.float32) * scale
                    row = lax.broadcasted_iota(jnp.int32, (block, span), 0) + b * block
                    s = jnp.where(row >= lax.broadcasted_iota(jnp.int32, (block, span), 1), s, -jnp.inf)
                    e = jnp.exp(s - jnp.max(s, axis=-1, keepdims=True))
                    p = (e * (1.0 / jnp.sum(e, axis=-1, keepdims=True))).astype(jnp.bfloat16)
                    cbuf[slot, b * block:(b + 1) * block, at] = jnp.dot(p, values[:span], preferred_element_type=jnp.float32).astype(jnp.bfloat16)
            return c

        lax.fori_loop(0, seqs, one_seq, 0)
        for slot in (2, 3, 1, 0):
            c_copy(slot, pair).start()

        @pl.when(pair == 1)
        def _():
            for piece in range(PARTS):
                wo_landed(x_dev, piece)
                wo_mate(1, x_dev, piece, wfull_hbm.at[x_dev, rows(piece)]).start()
                if piece < 3:
                    wo_y(4 + piece, x_dev, piece, wfull_hbm.at[x_dev, rows(piece)]).start()

        return carry

    lax.fori_loop(0, pairs, heads, 0)
    finish_send(n_copy(slot) for slot in range(1, PARTS))
    total[...] = tok_ref[...].astype(jnp.float32)
    for piece in (3, 0, 1, 2):
        wo_landed(y_dev, piece)
        wo_mate(2, y_dev, piece, wfull_hbm.at[y_dev, rows(piece)]).start()
        if piece == 3:
            wo_x(4, y_dev, piece, wfull_hbm.at[y_dev, rows(piece)]).start()
    for slot in range(1, PARTS):
        for at in strips(group, TILE):
            remote(cbuf.at[0, :, at], ctx.at[:, at], c_send.at[0, 0], c_recv.at[slot - 1, at.start // TILE], mate).wait_recv()
    for pair in range(PARTS):
        c_copy(0, pair).wait()
    wo_own.wait()
    order = (me, x_dev, y_dev, mate, x_mate, yn * CORES + 1 - core, dg_dev, dg * CORES + 1 - core)

    def load(step):
        slot = step % CORES
        return pltpu.make_async_copy(wfull_hbm.at[order[step]], nbuf.at[CORES + slot], ring_sem.at[slot])

    def ready(step):
        if step == 6:
            for piece in range(PARTS):
                wo_landed(dg_dev, piece)
                wo_mate(3, dg_dev, piece, wfull_hbm.at[dg_dev, rows(piece)]).start()
        elif step > 2:
            for piece in range(PARTS):
                wo_landed(order[step], piece)
        load(step).start()

    ready(0)
    for step, source in enumerate(order):
        early = step + 1 < 6
        if early:
            ready(step + 1)
        load(step).wait()
        heads_at = pl.ds(pl.multiple_of(source * wo_hbm.shape[0], wo_hbm.shape[0]), wo_hbm.shape[0])

        def add(n, c, slot=step % CORES, heads_at=heads_at):
            at = pl.ds(pl.multiple_of(n * TILE, TILE), TILE)
            total[:, at] += jnp.dot(ctx[:, heads_at], nbuf[CORES + slot, :, at], preferred_element_type=jnp.float32)
            return c

        lax.fori_loop(0, dim // TILE, add, 0)
        if not early and step + 1 < len(order):
            ready(step + 1)
    nbuf[0] = total[...].astype(jnp.bfloat16)
    h_copy = pltpu.make_async_copy(nbuf.at[0], h_hbm, out_sem.at[0])
    h_copy.start()
    wide = nbuf[0].astype(jnp.float32)
    nbuf[1] = (wide * lax.rsqrt(jnp.mean(wide * wide, axis=-1, keepdims=True) + EPS)).astype(jnp.bfloat16)
    u_copy = pltpu.make_async_copy(nbuf.at[1], u_hbm, out_sem.at[1])
    u_copy.start()
    for slot in range(7):
        id_copy(slot, me).wait_send()
    for m in range(3):
        own_mate(m).wait_send()
        for copy in over_x(m) + over_y(m) + forward_y(m):
            copy.wait_send()
        for slot in range(3):
            to_mate(m, slot).wait_send()
    for pair in range(PARTS):
        finish_send(c_copy(slot, pair) for slot in range(1, PARTS))
    h_copy.wait()
    u_copy.wait()
    for slot in range(5):
        wo_x(slot, me, 0, wo_hbm.at[rows(0)]).wait_send()
    for slot in range(7):
        wo_y(slot, me, 0, wo_hbm.at[rows(0)]).wait_send()
    for order in range(PARTS):
        for piece in range(PARTS):
            wo_mate(order, me, piece, wo_hbm.at[rows(piece)]).wait_send()


def attend(tokens, ids, w_query, w_key, w_value, w_out):
    tok, dim = tokens.shape
    depth, width = w_query.shape
    devices, group = 8, width // 4
    dma = pltpu.SemaphoreType.DMA
    return pl.pallas_call(
        attend_kernel,
        out_shape=(jax.ShapeDtypeStruct((tok, dim), jnp.bfloat16), jax.ShapeDtypeStruct((tok, dim), jnp.bfloat16), jax.ShapeDtypeStruct((devices,) + w_out.shape, jnp.bfloat16), jax.ShapeDtypeStruct((devices, 32, tok), jnp.float32), jax.ShapeDtypeStruct((devices,) + ids.shape, jnp.int32)),
        in_specs=[WHOLE] + [ANY] * 5,
        out_specs=(ANY, ANY, ANY, WHOLE, WHOLE),
        scratch_shapes=[
            pltpu.VMEM((tok, width), jnp.bfloat16), pltpu.VMEM((tok, dim), jnp.float32), dma((2,)), dma((2,)),
            pltpu.VMEM((devices,) + ids.shape, jnp.int32), dma((7,)), dma((devices,)), dma,
            pltpu.VMEM((4, tok, dim), jnp.bfloat16),
            pltpu.VMEM((3, devices, depth, group), jnp.bfloat16),
            pltpu.VMEM((3, 3, depth, group), jnp.bfloat16),
            pltpu.VMEM((3, 4, tok, group), jnp.bfloat16),
            pltpu.VMEM((4, tok, group), jnp.bfloat16),
            dma((3,)), dma((3, 2)), dma((3, 2)), dma((3, 2)), dma((3,)), dma((3, 3)), dma((3, devices)), dma((3, 3)),
            dma((4,)), dma((4,)), dma((3, 4)), dma((3, 4)), dma((4,)),
            dma((5,)), dma((7,)), dma((4, 4)), dma((devices, 4)), dma,
        ],
        compiler_params=pltpu.CompilerParams(collective_id=3, has_side_effects=True, vmem_limit_bytes=VMEM_MAX),
        name='attend_heads',
    )(tokens, ids, w_query, w_key, w_value, w_out)


def spread_kernel(u_hbm, h_ref, router_ref, ids_ref, slot_ref, x_hbm, gall_hbm, g_own, ubuf, hbuf, xbuf, own_sem, gown_sem, out_sem, x_send, y_send, d_send, recv, g_send, g_recv):
    me, core, chip, xn, yn, dg = neighbours()
    mate = me + 1 - 2 * core
    tok = ubuf.shape[1]
    part = tok // 4
    local_experts = slot_ref.shape[1] // 2
    x_dev, y_dev, dg_dev = xn * CORES + core, yn * CORES + core, dg * CORES + core
    others = (x_dev, y_dev, mate, dg_dev, xn * CORES + 1 - core, yn * CORES + 1 - core, dg * CORES + 1 - core)
    greet(others)

    def rows(piece):
        return pl.ds(piece * part, part)

    def landed(source, piece):
        remote(ubuf.at[source, rows(piece)], ubuf.at[source, rows(piece)], d_send.at[0, 0], recv.at[source, piece], mate).wait_recv()

    def pass_on(order, source, piece):
        return remote(ubuf.at[source, rows(piece)], ubuf.at[source, rows(piece)], d_send.at[order, piece], recv.at[source, piece], mate)

    def across_x(slot, source, piece, src):
        return remote(src, ubuf.at[source, rows(piece)], x_send.at[slot], recv.at[source, piece], x_dev)

    def across_y(slot, source, piece, src):
        return remote(src, ubuf.at[source, rows(piece)], y_send.at[slot], recv.at[source, piece], y_dev)

    own = pltpu.make_async_copy(u_hbm, ubuf.at[me], own_sem)
    own.start()
    for slot in range(PARTS):
        across_x(slot, me, slot, u_hbm.at[rows(slot)]).start()
        across_y(slot, me, (slot + 2) % 4, u_hbm.at[rows((slot + 2) % 4)]).start()
    for piece in range(PARTS):
        remote(u_hbm.at[rows(piece)], ubuf.at[me, rows(piece)], d_send.at[0, piece], recv.at[me, piece], mate).start()
    wide = h_ref[...].astype(jnp.float32)
    wide = wide * lax.rsqrt(jnp.mean(wide * wide, axis=-1, keepdims=True) + EPS)
    logits = jnp.dot(wide, router_ref[...], precision=lax.Precision.HIGHEST, preferred_element_type=jnp.float32).T
    expert_at = lax.broadcasted_iota(jnp.int32, logits.shape, 0)
    for j in range(g_own.shape[0]):
        g_own[j:j + 1, :] = jnp.sum(jnp.where(ids_ref[j:j + 1, :] == expert_at, logits, 0.0), axis=0, keepdims=True)
    chosen = g_own[...]
    chosen = jnp.exp(chosen - jnp.max(chosen, axis=0, keepdims=True))
    g_own[...] = chosen / jnp.sum(chosen, axis=0, keepdims=True)
    gown = pltpu.make_async_copy(g_own, gall_hbm.at[me], gown_sem)
    gown.start()
    for slot, device in enumerate(others):
        remote(g_own, gall_hbm.at[me], g_send.at[slot], g_recv.at[me], device).start()
    own.wait()

    def out_copy(order, source):
        return pltpu.make_async_copy(xbuf.at[lax.rem(order, 2)], x_hbm.at[:, source], out_sem.at[lax.rem(order, 2)])

    def step(order, carry):
        kind = order // 2
        base = jnp.where(kind == 0, chip, jnp.where(kind == 1, xn, jnp.where(kind == 2, yn, dg)))
        odd = lax.rem(order, 2)
        source = base * 2 + core + odd * (1 - 2 * core)

        @pl.when(order == 2)
        def _():
            for piece in (0, 1):
                landed(x_dev, piece)
                across_y(4 + piece, x_dev, piece, ubuf.at[x_dev, rows(piece)]).start()
                pass_on(1, x_dev, piece).start()
                landed(y_dev, piece + 2)
                across_x(4 + piece, y_dev, piece + 2, ubuf.at[y_dev, rows(piece + 2)]).start()
                pass_on(2, y_dev, piece + 2).start()
            for piece in (0, 1):
                landed(x_dev, piece + 2)
                pass_on(1, x_dev, piece + 2).start()
                landed(y_dev, piece)
                pass_on(2, y_dev, piece).start()

        @pl.when(order == 6)
        def _():
            for piece in (0, 2, 1, 3):
                landed(dg_dev, piece)
                pass_on(3, dg_dev, piece).start()

        @pl.when(odd == 1)
        def _():
            for piece in range(PARTS):
                landed(source, piece)

        @pl.when(order >= 2)
        def _():
            out_copy(order, source).wait()

        spot = lax.broadcasted_iota(jnp.int32, (CAP, tok), 0).astype(jnp.float32)
        for expert in range(local_experts):
            hit = slot_ref[source, expert:expert + 1, :] == spot
            hbuf[expert * CAP:(expert + 1) * CAP, :] = jnp.where(hit, 1.0, 0.0).astype(jnp.bfloat16)
        width = 256

        def tile(n, c):
            cols = pl.ds(pl.multiple_of(n * width, width), width)
            picked = jnp.dot(hbuf[...], ubuf[source, :, cols], preferred_element_type=jnp.float32)
            xbuf[odd, :, :, cols] = picked.astype(jnp.bfloat16).reshape(local_experts, CAP, width)
            return c

        lax.fori_loop(0, ubuf.shape[2] // width, tile, 0)
        out_copy(order, source).start()
        return carry

    lax.fori_loop(0, 8, step, 0)
    out_copy(0, me).wait()
    out_copy(1, me).wait()
    gown.wait()
    for slot in range(PARTS):
        across_x(slot, me, slot, u_hbm.at[rows(slot)]).wait_send()
        across_y(slot, me, slot, u_hbm.at[rows(slot)]).wait_send()
    for piece in (0, 1):
        across_y(4 + piece, x_dev, piece, ubuf.at[x_dev, rows(piece)]).wait_send()
        across_x(4 + piece, y_dev, piece + 2, ubuf.at[y_dev, rows(piece + 2)]).wait_send()
    for order, source in enumerate((me, x_dev, y_dev, dg_dev)):
        for piece in range(PARTS):
            pass_on(order, source, piece).wait_send()
    for slot, device in enumerate(others):
        remote(g_own, gall_hbm.at[me], g_send.at[slot], g_recv.at[me], device).wait_send()
        remote(g_own, gall_hbm.at[device], g_send.at[slot], g_recv.at[device], device).wait_recv()


def spread(u, hidden, w_router, ids, slots):
    devices, pair_experts, tok = slots.shape
    local_experts = pair_experts // 2
    dim = u.shape[1]
    return pl.pallas_call(
        spread_kernel,
        out_shape=(jax.ShapeDtypeStruct((local_experts, devices, CAP, dim), jnp.bfloat16), jax.ShapeDtypeStruct((devices,) + ids.shape, jnp.float32)),
        in_specs=[ANY, WHOLE, WHOLE, WHOLE, WHOLE],
        out_specs=(ANY, ANY),
        scratch_shapes=[
            pltpu.VMEM(ids.shape, jnp.float32),
            pltpu.VMEM((devices, tok, dim), jnp.bfloat16),
            pltpu.VMEM((local_experts * CAP, tok), jnp.bfloat16),
            pltpu.VMEM((2, local_experts, CAP, dim), jnp.bfloat16),
            pltpu.SemaphoreType.DMA, pltpu.SemaphoreType.DMA, pltpu.SemaphoreType.DMA((2,)),
            pltpu.SemaphoreType.DMA((6,)), pltpu.SemaphoreType.DMA((6,)), pltpu.SemaphoreType.DMA((4, 4)),
            pltpu.SemaphoreType.DMA((devices, 4)), pltpu.SemaphoreType.DMA((7,)), pltpu.SemaphoreType.DMA((devices,)),
        ],
        compiler_params=pltpu.CompilerParams(collective_id=1, has_side_effects=True, vmem_limit_bytes=VMEM_MAX),
        name='spread_rows',
    )(u, hidden, w_router, ids, slots)


def ffn_kernel(units_ref, x_ref, w1_hbm, w3_hbm, w2_hbm, o_ref, packed, middle, done, w1_buf, w3_buf, w2_buf, w_sem):
    expert = pl.program_id(0)
    last = pl.num_programs(0)
    devices = x_ref.shape[1]
    depth = w1_buf.shape[0]
    ahead = depth - 1

    def fetch(e):
        slot = lax.rem(e, depth)
        moves = ((w1_hbm, w1_buf), (w3_hbm, w3_buf), (w2_hbm, w2_buf))
        return [pltpu.make_async_copy(src.at[e], dst.at[slot], w_sem.at[slot, i]) for i, (src, dst) in enumerate(moves)]

    @pl.when(expert == 0)
    def _():
        for e in range(ahead):
            start(fetch(e))
        packed[...] = jnp.zeros_like(packed)
        done[...] = jnp.zeros_like(done)

    @pl.when(expert + ahead < last)
    def _():
        start(fetch(expert + ahead))

    begins, counts = [], [units_ref[expert * devices + source] * UNIT for source in range(devices)]
    total = 0
    for source in range(devices):
        begins.append(pl.multiple_of(total, UNIT))
        packed[pl.ds(begins[-1], CAP), :] = x_ref[0, source]
        total = total + counts[source]
    for copy in fetch(expert):
        copy.wait()
    slot = lax.rem(expert, depth)
    small, big = LANES, TILE

    def run(begin, size):
        rows = pl.ds(pl.multiple_of(begin, small), size)
        for at in strips(w1_buf.shape[2], TILE):
            first = jnp.dot(packed[rows, :], w1_buf[slot, :, at], preferred_element_type=jnp.float32)
            third = jnp.dot(packed[rows, :], w3_buf[slot, :, at], preferred_element_type=jnp.float32)
            middle[:size, at] = (first * jax.nn.sigmoid(first) * third).astype(jnp.bfloat16)
        for at in strips(w2_buf.shape[2], 2 * TILE):
            done[rows, at] = jnp.dot(middle[:size], w2_buf[slot, :, at], preferred_element_type=jnp.float32).astype(jnp.bfloat16)

    full = (total + small - 1) // big

    def run_big(t, c):
        run(t * big, big)
        return c

    lax.fori_loop(0, full, run_big, 0)

    @pl.when(full * big < total)
    def _():
        run(full * big, small)

    spot = lax.broadcasted_iota(jnp.int32, (CAP, o_ref.shape[3]), 0)
    for source in range(devices):
        o_ref[0, source] = jnp.where(spot < counts[source], done[pl.ds(begins[source], CAP), :], jnp.zeros((), jnp.bfloat16))


def expert_ffn(units, x, w_one, w_three, w_two):
    experts, devices, _, dim = x.shape
    mid = w_one.shape[2]
    depth = 3
    block = pl.BlockSpec((1, devices, CAP, dim), lambda e, units: (e, 0, 0, 0))
    ring = [pltpu.VMEM((depth,) + w.shape[1:], jnp.bfloat16) for w in (w_one, w_three, w_two)]
    lines = pltpu.VMEM(((devices + 1) * CAP, dim), jnp.bfloat16)
    return pl.pallas_call(
        ffn_kernel,
        out_shape=jax.ShapeDtypeStruct(x.shape, jnp.bfloat16),
        grid_spec=pltpu.PrefetchScalarGridSpec(
            num_scalar_prefetch=1,
            grid=(experts,),
            in_specs=[block] + [ANY] * 3,
            out_specs=block,
            scratch_shapes=[lines, pltpu.VMEM((TILE, mid), jnp.bfloat16), lines] + ring + [pltpu.SemaphoreType.DMA((depth, 3))],
        ),
        compiler_params=pltpu.CompilerParams(dimension_semantics=('arbitrary',), vmem_limit_bytes=VMEM_MAX),
        name='expert_mlp',
    )(units, x, w_one, w_three, w_two)


def combine_kernel(o_hbm, slots_ref, ids_ref, gates_ref, h_hbm, y_ref, own, mate_rows, gate_tab, gate3, p_one, r_one, p_two, r_two, p_last, r_last, own_sem, h_sem, mate_send, mate_recv, one_send, one_recv, two_send, two_recv, last_send, last_recv):
    me, core, chip, xn, yn, dg = neighbours()
    mate = me + 1 - CORES * core
    near = xn + core * (yn - xn)
    far = yn + core * (xn - yn)
    near_dev, far_dev = near * CORES + core, far * CORES + core
    half = own.shape[3]
    rows_n = p_one.shape[1]
    experts = own.shape[1]
    greet((near_dev, far_dev, mate))
    my_cols = pl.ds(pl.multiple_of(core * half, half), half)
    mate_cols = pl.ds(pl.multiple_of((1 - core) * half, half), half)
    spot = lax.broadcasted_iota(jnp.int32, gate_tab.shape, 0)
    wanted = jnp.where(spot < experts, me * experts + spot, (mate - 1) * experts + spot)

    def dest(i, first, second, front):
        pair, odd = i // CORES, lax.rem(i, CORES)
        base = jnp.where(pair == 0, dg, jnp.where(pair == 1, first, jnp.where(pair == 2, second, chip)))
        return base * CORES + jnp.where(pair < 3, odd, front + odd * (1 - CORES * front))

    def my_dest(i):
        return dest(i, near, far, 1 - core)

    def to_mate(i):
        return remote(o_hbm.at[:, dest(i, far, near, core), :, mate_cols], mate_rows.at[i], mate_send.at[i], mate_recv.at[i], mate)

    def own_copy(i):
        slot = lax.rem(i, CORES)
        return pltpu.make_async_copy(o_hbm.at[:, my_dest(i), :, my_cols], own.at[slot], own_sem.at[slot])

    def one_copy(n):
        return remote(p_one.at[n], r_one.at[n], one_send.at[n], one_recv.at[n], near_dev)

    def two_copy(n):
        return remote(p_two.at[n], r_two.at[n], two_send.at[n], two_recv.at[n], far_dev)

    def last_copy(n):
        return remote(p_last.at[n], r_last.at[n], last_send.at[n], last_recv.at[n], mate)

    own_copy(0).start()
    for i in range(8):
        to_mate(i).start()
    residual = pltpu.make_async_copy(h_hbm, y_ref, h_sem)
    residual.start()

    def open_dest(i):
        gate = jnp.zeros(gate_tab.shape, jnp.float32)
        target = my_dest(i)
        for j in range(ids_ref.shape[1]):
            gate = gate + jnp.where(ids_ref[target, j:j + 1, :] == wanted, gates_ref[target, j:j + 1, :], 0.0)
        gate_tab[...] = gate
        own_copy(i).wait()
        to_mate(i).wait_recv()

        @pl.when(i < 7)
        def _():
            own_copy(i + 1).start()

    def weights(i, part):
        target = my_dest(i)
        cols = pl.ds(pl.multiple_of(part * rows_n, rows_n), rows_n)
        line = lax.broadcasted_iota(jnp.int32, (2 * CAP, rows_n), 0)
        low = line < CAP
        place = (line - jnp.where(low, 0, CAP)).astype(jnp.float32)
        for pair, where in enumerate(strips(gate3.shape[1], 2 * CAP)):
            one, two = slice(2 * pair, 2 * pair + 1), slice(2 * pair + 1, 2 * pair + 2)
            hit = jnp.where(low, slots_ref[target, one, cols], slots_ref[target, two, cols]) == place
            rest = jnp.where(hit, jnp.where(low, gate_tab[one, cols], gate_tab[two, cols]), 0.0).T
            for rows in strips(gate3.shape[0], rows_n):
                term = rest.astype(jnp.bfloat16)
                gate3[rows, where] = term
                rest = rest - term.astype(jnp.float32)

    def products(i, part, sink):
        @pl.when(part == 0)
        def _():
            open_dest(i)

        weights(i, part)
        slot = lax.rem(i, CORES)
        depth = experts * CAP

        def tile(n, c):
            cols = pl.ds(pl.multiple_of(n * TILE, TILE), TILE)
            mine = own[slot, :, :, cols].reshape(depth, TILE)
            other = mate_rows[i, :, :, cols].reshape(depth, TILE)
            out = jnp.dot(gate3[:, :depth], mine, preferred_element_type=jnp.float32) + jnp.dot(gate3[:, depth:], other, preferred_element_type=jnp.float32)
            sink[:, cols] = sum(out[rows] for rows in strips(out.shape[0], rows_n))
            return c

        lax.fori_loop(0, half // TILE, tile, 0)

    lead, pair_n, part_n = p_one.shape[0], p_two.shape[0], p_two.shape[0] // CORES

    def phase_one(step, c):
        products(step // part_n, lax.rem(step, part_n), p_one.at[step])
        one_copy(step).start()
        return c

    lax.fori_loop(0, lead, phase_one, 0)

    def phase_two(step, c):
        products(4 + step // part_n, lax.rem(step, part_n), p_two.at[step])
        one_copy(step).wait_recv()
        p_two[step] = p_two[step] + r_one[step]
        two_copy(step).start()
        return c

    lax.fori_loop(0, pair_n, phase_two, 0)
    residual.wait()

    def phase_three(step, c):
        part = lax.rem(step, part_n)
        products(6 + step // part_n, part, p_last.at[step])
        n = jnp.where(step < part_n, 1 - core, core) * part_n + part
        one_copy(pair_n + n).wait_recv()
        two_copy(n).wait_recv()
        p_last[step] = p_last[step] + (r_one[pair_n + n] + r_two[n])

        @pl.when(step < part_n)
        def _():
            last_copy(step).start()

        @pl.when(step >= part_n)
        def _():
            rows = pl.ds(pl.multiple_of(part * rows_n, rows_n), rows_n)
            y_ref[rows, my_cols] = (y_ref[rows, my_cols].astype(jnp.float32) + p_last[step]).astype(jnp.bfloat16)

        return c

    lax.fori_loop(0, pair_n, phase_three, 0)
    for n in range(part_n):
        rows = pl.ds(n * rows_n, rows_n)
        last_copy(n).wait_recv()
        y_ref[rows, mate_cols] = (y_ref[rows, mate_cols].astype(jnp.float32) + r_last[n]).astype(jnp.bfloat16)
    finish_send(to_mate(n) for n in range(8))
    finish_send(one_copy(n) for n in range(lead))
    finish_send(two_copy(n) for n in range(pair_n))
    finish_send(last_copy(n) for n in range(part_n))


def combine(done, slots, ids, gates, hidden):
    experts, devices, _, dim = done.shape
    tok = hidden.shape[0]
    half, part = dim // CORES, tok // PARTS
    pair_n = CORES * PARTS
    dma = pltpu.SemaphoreType.DMA
    floats = lambda n: pltpu.VMEM((n, part, half), jnp.float32)
    rows = lambda n: pltpu.VMEM((n, experts, CAP, half), jnp.bfloat16)
    sizes = [CORES * pair_n, CORES * pair_n, pair_n, pair_n, pair_n, PARTS]
    sems = [dma((n,)) for n in (devices, devices, 2 * pair_n, 2 * pair_n, pair_n, pair_n, PARTS, PARTS)]
    return pl.pallas_call(
        combine_kernel,
        out_shape=jax.ShapeDtypeStruct((tok, dim), jnp.bfloat16),
        in_specs=[ANY, WHOLE, WHOLE, WHOLE, ANY],
        out_specs=WHOLE,
        scratch_shapes=[rows(CORES), rows(devices), pltpu.VMEM(slots.shape[1:], jnp.float32), pltpu.VMEM((3 * part, CORES * experts * CAP), jnp.bfloat16)] + [floats(n) for n in sizes] + [dma((CORES,)), dma] + sems,
        compiler_params=pltpu.CompilerParams(collective_id=2, has_side_effects=True, vmem_limit_bytes=VMEM_MAX),
        name='combine_rows',
    )(done, slots, ids, gates, hidden)


def solution(mesh):
    tok_spec = P(('dp', 'ep'))
    row_spec = P('ep')

    def local_layer(tokens, w_query, w_key, w_value, w_out, w_router, w_one, w_three, w_two, expert_ids):
        seq_count, seq_len, model_dim = tokens.shape
        choices = expert_ids.shape[2]
        local_experts = w_one.shape[0]
        tok_count = seq_count * seq_len
        ids_t = expert_ids.reshape(tok_count, choices).T
        flat = tokens.reshape(tok_count, model_dim)
        w_flat = [w.reshape(w.shape[0], -1) for w in (w_query, w_key, w_value)]
        hidden, normed, _, slot, all_ids = attend(flat, ids_t, *w_flat, w_out)
        units = ((jnp.max(slot[:, :local_experts], axis=2).astype(jnp.int32) + UNIT) // UNIT).T.reshape(-1)
        x, all_gates = spread(normed, hidden, w_router, ids_t, slot)
        done = expert_ffn(units, x, w_one, w_three, w_two)
        layer_out = combine(done, slot, all_ids, all_gates, hidden)
        return layer_out.reshape(seq_count, seq_len, model_dim)

    return jax.shard_map(local_layer, mesh=mesh, in_specs=(tok_spec, row_spec, row_spec, row_spec, row_spec, P(), row_spec, row_spec, row_spec, tok_spec), out_specs=tok_spec, check_vma=False)
```

```python
import functools

import jax
import jax.numpy as jnp
from jax import lax
from jax.experimental import pallas as pl
from jax.experimental.pallas import tpu as pltpu
from jax.sharding import PartitionSpec as P

EPS = 1e-6
CAP = 64
UNIT = 16
VMEM_MAX = 67043328
LANES = 128
TILE = 256
CORES = 2
PARTS = 4
ANY = pl.BlockSpec(memory_space=pl.ANY)
WHOLE = pl.BlockSpec(memory_space=pltpu.VMEM)


def strips(size, width):
    return [slice(at, at + width) for at in range(0, size, width)]


def start(copies):
    for copy in copies:
        copy.start()


def finish_send(copies):
    for copy in copies:
        copy.wait_send()


def neighbours():
    me = lax.axis_index('ep')
    core, chip = lax.rem(me, 2), me // 2
    side, up = lax.rem(chip, 2), chip // 2
    return me, core, chip, 1 - side + 2 * up, side + 2 * (1 - up), 3 - chip


def greet(devices):
    barrier = pltpu.get_barrier_semaphore()
    for device in devices:
        pl.semaphore_signal(barrier, inc=1, device_id={'ep': device}, device_id_type=pl.DeviceIdType.MESH)
    pl.semaphore_wait(barrier, len(devices))


def remote(src, dst, send_sem, recv_sem, device):
    return pltpu.make_async_remote_copy(src_ref=src, dst_ref=dst, send_sem=send_sem, recv_sem=recv_sem, device_id={'ep': device}, device_id_type=pl.DeviceIdType.MESH)


def attend_kernel(tok_ref, ids_hbm, wq_hbm, wk_hbm, wv_hbm, wo_hbm, h_hbm, u_hbm, wfull_hbm, slots_ref, ids_ref, ctx, total, out_sem, ring_sem, ids_buf, i_send, i_recv, i_own, nbuf, wbuf, wmate, qkv, cbuf, loc_sem, a_send, b_send, f_send, m_send, mf_send, w_recv, wm_recv, n_send, n_recv, c_send, c_recv, c_own, ox_send, oy_send, od_send, o_recv, o_own):
    me, core, chip, xn, yn, dg = neighbours()
    side = lax.rem(chip, 2)
    mate = me + 1 - 2 * core
    x_dev, y_dev, dg_dev, x_mate = xn * CORES + core, yn * CORES + core, dg * CORES + core, xn * CORES + 1 - core
    weights = (wq_hbm, wk_hbm, wv_hbm)
    seqs, tok, dim = nbuf.shape
    group = wbuf.shape[3]
    part = tok // 4
    others = (x_dev, y_dev, mate, x_mate, dg_dev, yn * CORES + 1 - core, dg * CORES + 1 - core)
    greet(others)

    def cols(on_side, on_core):
        return pl.ds(pl.multiple_of((2 * on_side + on_core) * group, group), group)

    def local_w(m):
        return pltpu.make_async_copy(weights[m].at[:, cols(side, core)], wbuf.at[m, me], loc_sem.at[m])

    def own_mate(m):
        return remote(weights[m].at[:, cols(side, 1 - core)], wbuf.at[m, me], m_send.at[m], w_recv.at[m, me], mate)

    def over_x(m):
        return (remote(weights[m].at[:, cols(1 - side, core)], wbuf.at[m, me], a_send.at[m, 0], w_recv.at[m, me], x_dev),
                remote(weights[m].at[:, cols(1 - side, 1 - core)], wmate.at[m, 0], a_send.at[m, 1], wm_recv.at[m, 0], x_dev))

    def over_y(m):
        return (remote(weights[m].at[:, cols(side, core)], wbuf.at[m, me], b_send.at[m, 0], w_recv.at[m, me], y_dev),
                remote(weights[m].at[:, cols(side, 1 - core)], wmate.at[m, 1], b_send.at[m, 1], wm_recv.at[m, 1], y_dev))

    def forward_y(m):
        return (remote(wbuf.at[m, x_dev], wbuf.at[m, x_dev], f_send.at[m, 0], w_recv.at[m, x_dev], y_dev),
                remote(wmate.at[m, 0], wmate.at[m, 2], f_send.at[m, 1], wm_recv.at[m, 2], y_dev))

    def to_mate(m, slot):
        source = (x_dev, y_dev, dg_dev)[slot]
        return remote(wmate.at[m, slot], wbuf.at[m, source], mf_send.at[m, slot], w_recv.at[m, source], mate)

    def landed(m, source):
        remote(wbuf.at[m, source], wbuf.at[m, source], m_send.at[m], w_recv.at[m, source], mate).wait_recv()

    def landed_mate(m, slot):
        to = wmate.at[m, slot]
        remote(to, to, m_send.at[m], wm_recv.at[m, slot], mate).wait_recv()

    def n_copy(slot):
        source, device = (0, 0, 0, 2)[slot], (mate, mate, x_dev, mate)[slot]
        return remote(nbuf.at[source], nbuf.at[slot], n_send.at[slot], n_recv.at[slot], device)

    def id_copy(slot, owner):
        return remote(ids_hbm, ids_buf.at[owner], i_send.at[slot], i_recv.at[owner], others[slot])

    def rows(piece):
        return pl.ds(piece * part, part)

    def wo_x(slot, source, piece, src):
        return remote(src, wfull_hbm.at[source, rows(piece)], ox_send.at[slot], o_recv.at[source, piece], x_dev)

    def wo_y(slot, source, piece, src):
        return remote(src, wfull_hbm.at[source, rows(piece)], oy_send.at[slot], o_recv.at[source, piece], y_dev)

    def wo_mate(order, source, piece, src):
        return remote(src, wfull_hbm.at[source, rows(piece)], od_send.at[order, piece], o_recv.at[source, piece], mate)

    def wo_landed(source, piece):
        to = wfull_hbm.at[source, rows(piece)]
        remote(to, to, od_send.at[0, 0], o_recv.at[source, piece], mate).wait_recv()

    for slot in range(7):
        id_copy(slot, me).start()
    id_own = pltpu.make_async_copy(ids_hbm, ids_buf.at[me], i_own)
    id_own.start()
    start(over_x(0))
    start(over_y(0))
    for m in range(3):
        local_w(m).start()
        own_mate(m).start()
    start(over_y(1))
    wide = tok_ref[...].astype(jnp.float32)
    nbuf[0] = (wide * lax.rsqrt(jnp.mean(wide * wide, axis=-1, keepdims=True) + EPS)).astype(jnp.bfloat16)
    n_copy(2).start()
    n_copy(1).start()
    start(over_x(1))
    start(over_x(2))
    for piece in range(PARTS):
        wo_x(piece, me, piece, wo_hbm.at[rows(piece)]).start()
    for piece in range(PARTS):
        wo_mate(0, me, piece, wo_hbm.at[rows(piece)]).start()
    wo_own = pltpu.make_async_copy(wo_hbm, wfull_hbm.at[me], o_own)
    wo_own.start()

    id_own.wait()
    for slot in range(7):
        id_copy(slot, others[slot]).wait_recv()
    order = lax.broadcasted_iota(jnp.int32, (tok, tok), 0) < lax.broadcasted_iota(jnp.int32, (tok, tok), 1)
    earlier = jnp.where(order, 1.0, 0.0).astype(jnp.bfloat16)
    experts = slots_ref.shape[1]
    spot = lax.broadcasted_iota(jnp.int32, (experts, tok), 0)
    local = experts // 2
    wanted = jnp.where(spot < local, me * local + spot, (mate - 1) * local + spot)

    def table(source, c):
        count = jnp.zeros((experts, tok), jnp.float32)
        for j in range(ids_buf.shape[1]):
            count = count + jnp.where(ids_buf[source, j:j + 1, :] == wanted, 1.0, 0.0)
        before = jnp.dot(count.astype(jnp.bfloat16), earlier, preferred_element_type=jnp.float32)
        slots_ref[source] = jnp.where(count > 0.0, before, -1.0)
        ids_ref[source] = ids_buf[source]
        return c

    lax.fori_loop(0, ids_buf.shape[0], table, 0)

    def arrive_x(m):
        landed(m, x_dev)
        landed_mate(m, 0)
        start(forward_y(m))
        to_mate(m, 0).start()

    def finish(m):
        landed_mate(m, 1)
        to_mate(m, 1).start()
        landed_mate(m, 2)
        to_mate(m, 2).start()
        local_w(m).wait()
        for source in (y_dev, dg_dev, mate, x_mate, yn * CORES + 1 - core, dg * CORES + 1 - core):
            landed(m, source)

    width = 256

    def project(m):
        def run(i, c):
            slot, n = i // (group // width), lax.rem(i, group // width)
            at = pl.ds(pl.multiple_of(n * width, width), width)
            out = jnp.dot(nbuf[slot], wbuf[m, :, :, at].reshape(dim, width), preferred_element_type=jnp.float32)
            qkv[m, slot, :, at] = out.astype(jnp.bfloat16)
            return c

        lax.fori_loop(0, seqs * (group // width), run, 0)

    arrive_x(0)
    start(over_y(2))
    n_copy(2).wait_recv()
    n_copy(3).start()
    finish(0)
    n_copy(1).wait_recv()
    n_copy(3).wait_recv()
    project(0)
    arrive_x(1)
    arrive_x(2)
    for slot, piece in enumerate((3, 0, 1, 2)):
        wo_y(slot, me, piece, wo_hbm.at[rows(piece)]).start()
    finish(1)
    project(1)
    finish(2)
    project(2)

    scale = 128 ** -0.5
    block = tok // 2
    pairs = group // 256

    def c_copy(slot, pair):
        at = pl.ds(pl.multiple_of(pair * 256, 256), 256)
        there = pl.ds(pl.multiple_of((2 * side + core) * group + pair * 256, 256), 256)
        src, dst = cbuf.at[slot, :, at], ctx.at[:, there]
        if slot == 0:
            return pltpu.make_async_copy(src, dst, c_own.at[pair])
        return remote(src, dst, c_send.at[slot - 1, pair], c_recv.at[slot - 1, pair], (mate, x_dev, x_mate)[slot - 1])

    def heads(pair, carry):
        def one_seq(slot, c):
            for h in range(2):
                at = pl.ds(pl.multiple_of(pair * 256 + h * 128, 128), 128)
                keys, values = qkv[1, slot, :, at], qkv[2, slot, :, at]
                for b in range(2):
                    query = qkv[0, slot, b * block:(b + 1) * block, at]
                    span = (b + 1) * block
                    s = lax.dot_general(query, keys[:span], (((1,), (1,)), ((), ())), preferred_element_type=jnp.float32) * scale
                    row = lax.broadcasted_iota(jnp.int32, (block, span), 0) + b * block
                    s = jnp.where(row >= lax.broadcasted_iota(jnp.int32, (block, span), 1), s, -jnp.inf)
                    e = jnp.exp(s - jnp.max(s, axis=-1, keepdims=True))
                    p = (e * (1.0 / jnp.sum(e, axis=-1, keepdims=True))).astype(jnp.bfloat16)
                    cbuf[slot, b * block:(b + 1) * block, at] = jnp.dot(p, values[:span], preferred_element_type=jnp.float32).astype(jnp.bfloat16)
            return c

        lax.fori_loop(0, seqs, one_seq, 0)
        for slot in (2, 3, 1, 0):
            c_copy(slot, pair).start()

        @pl.when(pair == 1)
        def _():
            for piece in range(PARTS):
                wo_landed(x_dev, piece)
                wo_mate(1, x_dev, piece, wfull_hbm.at[x_dev, rows(piece)]).start()
                if piece < 3:
                    wo_y(4 + piece, x_dev, piece, wfull_hbm.at[x_dev, rows(piece)]).start()

        return carry

    lax.fori_loop(0, pairs, heads, 0)
    finish_send(n_copy(slot) for slot in range(1, PARTS))
    total[...] = tok_ref[...].astype(jnp.float32)
    for piece in (3, 0, 1, 2):
        wo_landed(y_dev, piece)
        wo_mate(2, y_dev, piece, wfull_hbm.at[y_dev, rows(piece)]).start()
        if piece == 3:
            wo_x(4, y_dev, piece, wfull_hbm.at[y_dev, rows(piece)]).start()
    for slot in range(1, PARTS):
        for at in strips(group, TILE):
            remote(cbuf.at[0, :, at], ctx.at[:, at], c_send.at[0, 0], c_recv.at[slot - 1, at.start // TILE], mate).wait_recv()
    for pair in range(PARTS):
        c_copy(0, pair).wait()
    wo_own.wait()
    order = (me, x_dev, y_dev, mate, x_mate, yn * CORES + 1 - core, dg_dev, dg * CORES + 1 - core)

    def load(step):
        slot = step % CORES
        return pltpu.make_async_copy(wfull_hbm.at[order[step]], nbuf.at[CORES + slot], ring_sem.at[slot])

    def ready(step):
        if step == 6:
            for piece in range(PARTS):
                wo_landed(dg_dev, piece)
                wo_mate(3, dg_dev, piece, wfull_hbm.at[dg_dev, rows(piece)]).start()
        elif step > 2:
            for piece in range(PARTS):
                wo_landed(order[step], piece)
        load(step).start()

    ready(0)
    for step, source in enumerate(order):
        early = step + 1 < 6
        if early:
            ready(step + 1)
        load(step).wait()
        heads_at = pl.ds(pl.multiple_of(source * wo_hbm.shape[0], wo_hbm.shape[0]), wo_hbm.shape[0])

        def add(n, c, slot=step % CORES, heads_at=heads_at):
            at = pl.ds(pl.multiple_of(n * TILE, TILE), TILE)
            total[:, at] += jnp.dot(ctx[:, heads_at], nbuf[CORES + slot, :, at], preferred_element_type=jnp.float32)
            return c

        lax.fori_loop(0, dim // TILE, add, 0)
        if not early and step + 1 < len(order):
            ready(step + 1)
    nbuf[0] = total[...].astype(jnp.bfloat16)
    h_copy = pltpu.make_async_copy(nbuf.at[0], h_hbm, out_sem.at[0])
    h_copy.start()
    wide = nbuf[0].astype(jnp.float32)
    nbuf[1] = (wide * lax.rsqrt(jnp.mean(wide * wide, axis=-1, keepdims=True) + EPS)).astype(jnp.bfloat16)
    u_copy = pltpu.make_async_copy(nbuf.at[1], u_hbm, out_sem.at[1])
    u_copy.start()
    for slot in range(7):
        id_copy(slot, me).wait_send()
    for m in range(3):
        own_mate(m).wait_send()
        for copy in over_x(m) + over_y(m) + forward_y(m):
            copy.wait_send()
        for slot in range(3):
            to_mate(m, slot).wait_send()
    for pair in range(PARTS):
        finish_send(c_copy(slot, pair) for slot in range(1, PARTS))
    h_copy.wait()
    u_copy.wait()
    for slot in range(5):
        wo_x(slot, me, 0, wo_hbm.at[rows(0)]).wait_send()
    for slot in range(7):
        wo_y(slot, me, 0, wo_hbm.at[rows(0)]).wait_send()
    for order in range(PARTS):
        for piece in range(PARTS):
            wo_mate(order, me, piece, wo_hbm.at[rows(piece)]).wait_send()


def attend(tokens, ids, w_query, w_key, w_value, w_out):
    tok, dim = tokens.shape
    depth, width = w_query.shape
    devices, group = 8, width // 4
    dma = pltpu.SemaphoreType.DMA
    return pl.pallas_call(
        attend_kernel,
        out_shape=(jax.ShapeDtypeStruct((tok, dim), jnp.bfloat16), jax.ShapeDtypeStruct((tok, dim), jnp.bfloat16), jax.ShapeDtypeStruct((devices,) + w_out.shape, jnp.bfloat16), jax.ShapeDtypeStruct((devices, 32, tok), jnp.float32), jax.ShapeDtypeStruct((devices,) + ids.shape, jnp.int32)),
        in_specs=[WHOLE] + [ANY] * 5,
        out_specs=(ANY, ANY, ANY, WHOLE, WHOLE),
        scratch_shapes=[
            pltpu.VMEM((tok, width), jnp.bfloat16), pltpu.VMEM((tok, dim), jnp.float32), dma((2,)), dma((2,)),
            pltpu.VMEM((devices,) + ids.shape, jnp.int32), dma((7,)), dma((devices,)), dma,
            pltpu.VMEM((4, tok, dim), jnp.bfloat16),
            pltpu.VMEM((3, devices, depth, group), jnp.bfloat16),
            pltpu.VMEM((3, 3, depth, group), jnp.bfloat16),
            pltpu.VMEM((3, 4, tok, group), jnp.bfloat16),
            pltpu.VMEM((4, tok, group), jnp.bfloat16),
            dma((3,)), dma((3, 2)), dma((3, 2)), dma((3, 2)), dma((3,)), dma((3, 3)), dma((3, devices)), dma((3, 3)),
            dma((4,)), dma((4,)), dma((3, 4)), dma((3, 4)), dma((4,)),
            dma((5,)), dma((7,)), dma((4, 4)), dma((devices, 4)), dma,
        ],
        compiler_params=pltpu.CompilerParams(collective_id=3, has_side_effects=True, vmem_limit_bytes=VMEM_MAX),
        name='attend_heads',
    )(tokens, ids, w_query, w_key, w_value, w_out)


def spread_kernel(u_hbm, h_ref, router_ref, ids_ref, slot_ref, x_hbm, gall_hbm, g_own, ubuf, hbuf, xbuf, own_sem, gown_sem, out_sem, x_send, y_send, d_send, recv, g_send, g_recv):
    me, core, chip, xn, yn, dg = neighbours()
    mate = me + 1 - 2 * core
    tok = ubuf.shape[1]
    part = tok // 4
    local_experts = slot_ref.shape[1] // 2
    x_dev, y_dev, dg_dev = xn * CORES + core, yn * CORES + core, dg * CORES + core
    others = (x_dev, y_dev, mate, dg_dev, xn * CORES + 1 - core, yn * CORES + 1 - core, dg * CORES + 1 - core)
    greet(others)

    def rows(piece):
        return pl.ds(piece * part, part)

    def landed(source, piece):
        remote(ubuf.at[source, rows(piece)], ubuf.at[source, rows(piece)], d_send.at[0, 0], recv.at[source, piece], mate).wait_recv()

    def pass_on(order, source, piece):
        return remote(ubuf.at[source, rows(piece)], ubuf.at[source, rows(piece)], d_send.at[order, piece], recv.at[source, piece], mate)

    def across_x(slot, source, piece, src):
        return remote(src, ubuf.at[source, rows(piece)], x_send.at[slot], recv.at[source, piece], x_dev)

    def across_y(slot, source, piece, src):
        return remote(src, ubuf.at[source, rows(piece)], y_send.at[slot], recv.at[source, piece], y_dev)

    own = pltpu.make_async_copy(u_hbm, ubuf.at[me], own_sem)
    own.start()
    for slot in range(PARTS):
        across_x(slot, me, slot, u_hbm.at[rows(slot)]).start()
        across_y(slot, me, (slot + 2) % 4, u_hbm.at[rows((slot + 2) % 4)]).start()
    for piece in range(PARTS):
        remote(u_hbm.at[rows(piece)], ubuf.at[me, rows(piece)], d_send.at[0, piece], recv.at[me, piece], mate).start()
    wide = h_ref[...].astype(jnp.float32)
    wide = wide * lax.rsqrt(jnp.mean(wide * wide, axis=-1, keepdims=True) + EPS)
    logits = jnp.dot(wide, router_ref[...], precision=lax.Precision.HIGHEST, preferred_element_type=jnp.float32).T
    expert_at = lax.broadcasted_iota(jnp.int32, logits.shape, 0)
    for j in range(g_own.shape[0]):
        g_own[j:j + 1, :] = jnp.sum(jnp.where(ids_ref[j:j + 1, :] == expert_at, logits, 0.0), axis=0, keepdims=True)
    chosen = g_own[...]
    chosen = jnp.exp(chosen - jnp.max(chosen, axis=0, keepdims=True))
    g_own[...] = chosen / jnp.sum(chosen, axis=0, keepdims=True)
    gown = pltpu.make_async_copy(g_own, gall_hbm.at[me], gown_sem)
    gown.start()
    for slot, device in enumerate(others):
        remote(g_own, gall_hbm.at[me], g_send.at[slot], g_recv.at[me], device).start()
    own.wait()

    def out_copy(order, source):
        return pltpu.make_async_copy(xbuf.at[lax.rem(order, 2)], x_hbm.at[:, source], out_sem.at[lax.rem(order, 2)])

    def step(order, carry):
        kind = order // 2
        base = jnp.where(kind == 0, chip, jnp.where(kind == 1, xn, jnp.where(kind == 2, yn, dg)))
        odd = lax.rem(order, 2)
        source = base * 2 + core + odd * (1 - 2 * core)

        @pl.when(order == 2)
        def _():
            for piece in (0, 1):
                landed(x_dev, piece)
                across_y(4 + piece, x_dev, piece, ubuf.at[x_dev, rows(piece)]).start()
                pass_on(1, x_dev, piece).start()
                landed(y_dev, piece + 2)
                across_x(4 + piece, y_dev, piece + 2, ubuf.at[y_dev, rows(piece + 2)]).start()
                pass_on(2, y_dev, piece + 2).start()
            for piece in (0, 1):
                landed(x_dev, piece + 2)
                pass_on(1, x_dev, piece + 2).start()
                landed(y_dev, piece)
                pass_on(2, y_dev, piece).start()

        @pl.when(order == 6)
        def _():
            for piece in (0, 2, 1, 3):
                landed(dg_dev, piece)
                pass_on(3, dg_dev, piece).start()

        @pl.when(odd == 1)
        def _():
            for piece in range(PARTS):
                landed(source, piece)

        @pl.when(order >= 2)
        def _():
            out_copy(order, source).wait()

        spot = lax.broadcasted_iota(jnp.int32, (CAP, tok), 0).astype(jnp.float32)
        for expert in range(local_experts):
            hit = slot_ref[source, expert:expert + 1, :] == spot
            hbuf[expert * CAP:(expert + 1) * CAP, :] = jnp.where(hit, 1.0, 0.0).astype(jnp.bfloat16)
        width = 256

        def tile(n, c):
            cols = pl.ds(pl.multiple_of(n * width, width), width)
            picked = jnp.dot(hbuf[...], ubuf[source, :, cols], preferred_element_type=jnp.float32)
            xbuf[odd, :, :, cols] = picked.astype(jnp.bfloat16).reshape(local_experts, CAP, width)
            return c

        lax.fori_loop(0, ubuf.shape[2] // width, tile, 0)
        out_copy(order, source).start()
        return carry

    lax.fori_loop(0, 8, step, 0)
    out_copy(0, me).wait()
    out_copy(1, me).wait()
    gown.wait()
    for slot in range(PARTS):
        across_x(slot, me, slot, u_hbm.at[rows(slot)]).wait_send()
        across_y(slot, me, slot, u_hbm.at[rows(slot)]).wait_send()
    for piece in (0, 1):
        across_y(4 + piece, x_dev, piece, ubuf.at[x_dev, rows(piece)]).wait_send()
        across_x(4 + piece, y_dev, piece + 2, ubuf.at[y_dev, rows(piece + 2)]).wait_send()
    for order, source in enumerate((me, x_dev, y_dev, dg_dev)):
        for piece in range(PARTS):
            pass_on(order, source, piece).wait_send()
    for slot, device in enumerate(others):
        remote(g_own, gall_hbm.at[me], g_send.at[slot], g_recv.at[me], device).wait_send()
        remote(g_own, gall_hbm.at[device], g_send.at[slot], g_recv.at[device], device).wait_recv()


def spread(u, hidden, w_router, ids, slots):
    devices, pair_experts, tok = slots.shape
    local_experts = pair_experts // 2
    dim = u.shape[1]
    return pl.pallas_call(
        spread_kernel,
        out_shape=(jax.ShapeDtypeStruct((local_experts, devices, CAP, dim), jnp.bfloat16), jax.ShapeDtypeStruct((devices,) + ids.shape, jnp.float32)),
        in_specs=[ANY, WHOLE, WHOLE, WHOLE, WHOLE],
        out_specs=(ANY, ANY),
        scratch_shapes=[
            pltpu.VMEM(ids.shape, jnp.float32),
            pltpu.VMEM((devices, tok, dim), jnp.bfloat16),
            pltpu.VMEM((local_experts * CAP, tok), jnp.bfloat16),
            pltpu.VMEM((2, local_experts, CAP, dim), jnp.bfloat16),
            pltpu.SemaphoreType.DMA, pltpu.SemaphoreType.DMA, pltpu.SemaphoreType.DMA((2,)),
            pltpu.SemaphoreType.DMA((6,)), pltpu.SemaphoreType.DMA((6,)), pltpu.SemaphoreType.DMA((4, 4)),
            pltpu.SemaphoreType.DMA((devices, 4)), pltpu.SemaphoreType.DMA((7,)), pltpu.SemaphoreType.DMA((devices,)),
        ],
        compiler_params=pltpu.CompilerParams(collective_id=1, has_side_effects=True, vmem_limit_bytes=VMEM_MAX),
        name='spread_rows',
    )(u, hidden, w_router, ids, slots)


def ffn_kernel(units_ref, x_ref, w1_hbm, w3_hbm, w2_hbm, o_ref, packed, middle, done, w1_buf, w3_buf, w2_buf, w_sem):
    expert = pl.program_id(0)
    last = pl.num_programs(0)
    devices = x_ref.shape[1]
    depth = w1_buf.shape[0]
    ahead = depth - 1

    def fetch(e):
        slot = lax.rem(e, depth)
        moves = ((w1_hbm, w1_buf), (w3_hbm, w3_buf), (w2_hbm, w2_buf))
        return [pltpu.make_async_copy(src.at[e], dst.at[slot], w_sem.at[slot, i]) for i, (src, dst) in enumerate(moves)]

    @pl.when(expert == 0)
    def _():
        for e in range(ahead):
            start(fetch(e))
        packed[...] = jnp.zeros_like(packed)
        done[...] = jnp.zeros_like(done)

    @pl.when(expert + ahead < last)
    def _():
        start(fetch(expert + ahead))

    begins, counts = [], [units_ref[expert * devices + source] * UNIT for source in range(devices)]
    total = 0
    for source in range(devices):
        begins.append(pl.multiple_of(total, UNIT))
        packed[pl.ds(begins[-1], CAP), :] = x_ref[0, source]
        total = total + counts[source]
    for copy in fetch(expert):
        copy.wait()
    slot = lax.rem(expert, depth)
    small, big = LANES, TILE

    def run(begin, size):
        rows = pl.ds(pl.multiple_of(begin, small), size)
        for at in strips(w1_buf.shape[2], TILE):
            first = jnp.dot(packed[rows, :], w1_buf[slot, :, at], preferred_element_type=jnp.float32)
            third = jnp.dot(packed[rows, :], w3_buf[slot, :, at], preferred_element_type=jnp.float32)
            middle[:size, at] = (first * jax.nn.sigmoid(first) * third).astype(jnp.bfloat16)
        for at in strips(w2_buf.shape[2], 2 * TILE):
            done[rows, at] = jnp.dot(middle[:size], w2_buf[slot, :, at], preferred_element_type=jnp.float32).astype(jnp.bfloat16)

    full = (total + small - 1) // big

    def run_big(t, c):
        run(t * big, big)
        return c

    lax.fori_loop(0, full, run_big, 0)

    @pl.when(full * big < total)
    def _():
        run(full * big, small)

    spot = lax.broadcasted_iota(jnp.int32, (CAP, o_ref.shape[3]), 0)
    for source in range(devices):
        o_ref[0, source] = jnp.where(spot < counts[source], done[pl.ds(begins[source], CAP), :], jnp.zeros((), jnp.bfloat16))


def expert_ffn(units, x, w_one, w_three, w_two):
    experts, devices, _, dim = x.shape
    mid = w_one.shape[2]
    depth = 3
    block = pl.BlockSpec((1, devices, CAP, dim), lambda e, units: (e, 0, 0, 0))
    ring = [pltpu.VMEM((depth,) + w.shape[1:], jnp.bfloat16) for w in (w_one, w_three, w_two)]
    lines = pltpu.VMEM(((devices + 1) * CAP, dim), jnp.bfloat16)
    return pl.pallas_call(
        ffn_kernel,
        out_shape=jax.ShapeDtypeStruct(x.shape, jnp.bfloat16),
        grid_spec=pltpu.PrefetchScalarGridSpec(
            num_scalar_prefetch=1,
            grid=(experts,),
            in_specs=[block] + [ANY] * 3,
            out_specs=block,
            scratch_shapes=[lines, pltpu.VMEM((TILE, mid), jnp.bfloat16), lines] + ring + [pltpu.SemaphoreType.DMA((depth, 3))],
        ),
        compiler_params=pltpu.CompilerParams(dimension_semantics=('arbitrary',), vmem_limit_bytes=VMEM_MAX),
        name='expert_mlp',
    )(units, x, w_one, w_three, w_two)


def combine_kernel(o_hbm, slots_ref, ids_ref, gates_ref, h_hbm, y_ref, own, mate_rows, gate_tab, gate3, p_one, r_one, p_two, r_two, p_last, r_last, own_sem, h_sem, mate_send, mate_recv, one_send, one_recv, two_send, two_recv, last_send, last_recv):
    me, core, chip, xn, yn, dg = neighbours()
    mate = me + 1 - CORES * core
    near = xn + core * (yn - xn)
    far = yn + core * (xn - yn)
    near_dev, far_dev = near * CORES + core, far * CORES + core
    half = own.shape[3]
    rows_n = p_one.shape[1]
    experts = own.shape[1]
    greet((near_dev, far_dev, mate))
    my_cols = pl.ds(pl.multiple_of(core * half, half), half)
    mate_cols = pl.ds(pl.multiple_of((1 - core) * half, half), half)
    spot = lax.broadcasted_iota(jnp.int32, gate_tab.shape, 0)
    wanted = jnp.where(spot < experts, me * experts + spot, (mate - 1) * experts + spot)

    def dest(i, first, second, front):
        pair, odd = i // CORES, lax.rem(i, CORES)
        base = jnp.where(pair == 0, dg, jnp.where(pair == 1, first, jnp.where(pair == 2, second, chip)))
        return base * CORES + jnp.where(pair < 3, odd, front + odd * (1 - CORES * front))

    def my_dest(i):
        return dest(i, near, far, 1 - core)

    def to_mate(i):
        return remote(o_hbm.at[:, dest(i, far, near, core), :, mate_cols], mate_rows.at[i], mate_send.at[i], mate_recv.at[i], mate)

    def own_copy(i):
        slot = lax.rem(i, CORES)
        return pltpu.make_async_copy(o_hbm.at[:, my_dest(i), :, my_cols], own.at[slot], own_sem.at[slot])

    def one_copy(n):
        return remote(p_one.at[n], r_one.at[n], one_send.at[n], one_recv.at[n], near_dev)

    def two_copy(n):
        return remote(p_two.at[n], r_two.at[n], two_send.at[n], two_recv.at[n], far_dev)

    def last_copy(n):
        return remote(p_last.at[n], r_last.at[n], last_send.at[n], last_recv.at[n], mate)

    own_copy(0).start()
    for i in range(8):
        to_mate(i).start()
    residual = pltpu.make_async_copy(h_hbm, y_ref, h_sem)
    residual.start()

    def open_dest(i):
        gate = jnp.zeros(gate_tab.shape, jnp.float32)
        target = my_dest(i)
        for j in range(ids_ref.shape[1]):
            gate = gate + jnp.where(ids_ref[target, j:j + 1, :] == wanted, gates_ref[target, j:j + 1, :], 0.0)
        gate_tab[...] = gate

    def open_rows(i):
        own_copy(i).wait()
        to_mate(i).wait_recv()

        @pl.when(i < 7)
        def _():
            own_copy(i + 1).start()

    def weights(i, part):
        target = my_dest(i)
        cols = pl.ds(pl.multiple_of(part * rows_n, rows_n), rows_n)
        line = lax.broadcasted_iota(jnp.int32, (2 * CAP, rows_n), 0)
        low = line < CAP
        place = (line - jnp.where(low, 0, CAP)).astype(jnp.float32)
        for pair, where in enumerate(strips(gate3.shape[1], 2 * CAP)):
            one, two = slice(2 * pair, 2 * pair + 1), slice(2 * pair + 1, 2 * pair + 2)
            hit = jnp.where(low, slots_ref[target, one, cols], slots_ref[target, two, cols]) == place
            rest = jnp.where(hit, jnp.where(low, gate_tab[one, cols], gate_tab[two, cols]), 0.0).T
            for rows in strips(gate3.shape[0], rows_n):
                term = rest.astype(jnp.bfloat16)
                gate3[rows, where] = term
                rest = rest - term.astype(jnp.float32)

    def products(i, part, sink):
        @pl.when(part == 0)
        def _():
            open_dest(i)

        weights(i, part)

        @pl.when(part == 0)
        def _():
            open_rows(i)

        slot = lax.rem(i, CORES)
        depth = experts * CAP

        def tile(n, c):
            cols = pl.ds(pl.multiple_of(n * TILE, TILE), TILE)
            mine = own[slot, :, :, cols].reshape(depth, TILE)
            other = mate_rows[i, :, :, cols].reshape(depth, TILE)
            out = jnp.dot(gate3[:, :depth], mine, preferred_element_type=jnp.float32) + jnp.dot(gate3[:, depth:], other, preferred_element_type=jnp.float32)
            sink[:, cols] = sum(out[rows] for rows in strips(out.shape[0], rows_n))
            return c

        lax.fori_loop(0, half // TILE, tile, 0)

    lead, pair_n, part_n = p_one.shape[0], p_two.shape[0], p_two.shape[0] // CORES

    def phase_one(step, c):
        products(step // part_n, lax.rem(step, part_n), p_one.at[step])
        one_copy(step).start()
        return c

    lax.fori_loop(0, lead, phase_one, 0)

    def phase_two(step, c):
        products(4 + step // part_n, lax.rem(step, part_n), p_two.at[step])
        one_copy(step).wait_recv()
        p_two[step] = p_two[step] + r_one[step]
        two_copy(step).start()
        return c

    lax.fori_loop(0, pair_n, phase_two, 0)
    residual.wait()

    def phase_three(step, c):
        products(6 + step // part_n, lax.rem(step, part_n), p_last.at[step])
        return c

    lax.fori_loop(0, pair_n, phase_three, 0)

    def close(step, c):
        part = lax.rem(step, part_n)
        n = jnp.where(step < part_n, 1 - core, core) * part_n + part
        one_copy(pair_n + n).wait_recv()
        two_copy(n).wait_recv()
        p_last[step] = p_last[step] + (r_one[pair_n + n] + r_two[n])

        @pl.when(step < part_n)
        def _():
            last_copy(step).start()

        @pl.when(step >= part_n)
        def _():
            rows = pl.ds(pl.multiple_of(part * rows_n, rows_n), rows_n)
            y_ref[rows, my_cols] = (y_ref[rows, my_cols].astype(jnp.float32) + p_last[step]).astype(jnp.bfloat16)

        return c

    lax.fori_loop(0, pair_n, close, 0)
    for n in range(part_n):
        rows = pl.ds(n * rows_n, rows_n)
        last_copy(n).wait_recv()
        y_ref[rows, mate_cols] = (y_ref[rows, mate_cols].astype(jnp.float32) + r_last[n]).astype(jnp.bfloat16)
    finish_send(to_mate(n) for n in range(8))
    finish_send(one_copy(n) for n in range(lead))
    finish_send(two_copy(n) for n in range(pair_n))
    finish_send(last_copy(n) for n in range(part_n))


def combine(done, slots, ids, gates, hidden):
    experts, devices, _, dim = done.shape
    tok = hidden.shape[0]
    half, part = dim // CORES, tok // PARTS
    pair_n = CORES * PARTS
    dma = pltpu.SemaphoreType.DMA
    floats = lambda n: pltpu.VMEM((n, part, half), jnp.float32)
    rows = lambda n: pltpu.VMEM((n, experts, CAP, half), jnp.bfloat16)
    sizes = [CORES * pair_n, CORES * pair_n, pair_n, pair_n, pair_n, PARTS]
    sems = [dma((n,)) for n in (devices, devices, 2 * pair_n, 2 * pair_n, pair_n, pair_n, PARTS, PARTS)]
    return pl.pallas_call(
        combine_kernel,
        out_shape=jax.ShapeDtypeStruct((tok, dim), jnp.bfloat16),
        in_specs=[ANY, WHOLE, WHOLE, WHOLE, ANY],
        out_specs=WHOLE,
        scratch_shapes=[rows(CORES), rows(devices), pltpu.VMEM(slots.shape[1:], jnp.float32), pltpu.VMEM((3 * part, CORES * experts * CAP), jnp.bfloat16)] + [floats(n) for n in sizes] + [dma((CORES,)), dma] + sems,
        compiler_params=pltpu.CompilerParams(collective_id=2, has_side_effects=True, vmem_limit_bytes=VMEM_MAX),
        name='combine_rows',
    )(done, slots, ids, gates, hidden)


def solution(mesh):
    tok_spec = P(('dp', 'ep'))
    row_spec = P('ep')

    def local_layer(tokens, w_query, w_key, w_value, w_out, w_router, w_one, w_three, w_two, expert_ids):
        seq_count, seq_len, model_dim = tokens.shape
        choices = expert_ids.shape[2]
        local_experts = w_one.shape[0]
        tok_count = seq_count * seq_len
        ids_t = expert_ids.reshape(tok_count, choices).T
        flat = tokens.reshape(tok_count, model_dim)
        w_flat = [w.reshape(w.shape[0], -1) for w in (w_query, w_key, w_value)]
        hidden, normed, _, slot, all_ids = attend(flat, ids_t, *w_flat, w_out)
        units = ((jnp.max(slot[:, :local_experts], axis=2).astype(jnp.int32) + UNIT) // UNIT).T.reshape(-1)
        x, all_gates = spread(normed, hidden, w_router, ids_t, slot)
        done = expert_ffn(units, x, w_one, w_three, w_two)
        layer_out = combine(done, slot, all_ids, all_gates, hidden)
        return layer_out.reshape(seq_count, seq_len, model_dim)

    return jax.shard_map(local_layer, mesh=mesh, in_specs=(tok_spec, row_spec, row_spec, row_spec, row_spec, P(), row_spec, row_spec, row_spec, tok_spec), out_specs=tok_spec, check_vma=False)
```

```python
import functools

import jax
import jax.numpy as jnp
from jax import lax
from jax.experimental import pallas as pl
from jax.experimental.pallas import tpu as pltpu
from jax.sharding import PartitionSpec as P

EPS = 1e-6
CAP = 64
UNIT = 16
VMEM_MAX = 67043328
LANES = 128
TILE = 256
CORES = 2
PARTS = 4
ANY = pl.BlockSpec(memory_space=pl.ANY)
WHOLE = pl.BlockSpec(memory_space=pltpu.VMEM)


def strips(size, width):
    return [slice(at, at + width) for at in range(0, size, width)]


def start(copies):
    for copy in copies:
        copy.start()


def finish_send(copies):
    for copy in copies:
        copy.wait_send()


def neighbours():
    me = lax.axis_index('ep')
    core, chip = lax.rem(me, 2), me // 2
    side, up = lax.rem(chip, 2), chip // 2
    return me, core, chip, 1 - side + 2 * up, side + 2 * (1 - up), 3 - chip


def greet(devices):
    barrier = pltpu.get_barrier_semaphore()
    for device in devices:
        pl.semaphore_signal(barrier, inc=1, device_id={'ep': device}, device_id_type=pl.DeviceIdType.MESH)
    pl.semaphore_wait(barrier, len(devices))


def remote(src, dst, send_sem, recv_sem, device):
    return pltpu.make_async_remote_copy(src_ref=src, dst_ref=dst, send_sem=send_sem, recv_sem=recv_sem, device_id={'ep': device}, device_id_type=pl.DeviceIdType.MESH)


def attend_kernel(tok_ref, ids_hbm, wq_hbm, wk_hbm, wv_hbm, wo_hbm, h_hbm, u_hbm, wfull_hbm, slots_ref, ids_ref, ctx, total, out_sem, ring_sem, ids_buf, i_send, i_recv, i_own, nbuf, wbuf, wmate, qkv, cbuf, loc_sem, a_send, b_send, f_send, m_send, mf_send, w_recv, wm_recv, n_send, n_recv, c_send, c_recv, c_own, ox_send, oy_send, od_send, o_recv, o_own):
    me, core, chip, xn, yn, dg = neighbours()
    side = lax.rem(chip, 2)
    mate = me + 1 - 2 * core
    x_dev, y_dev, dg_dev, x_mate = xn * CORES + core, yn * CORES + core, dg * CORES + core, xn * CORES + 1 - core
    weights = (wq_hbm, wk_hbm, wv_hbm)
    seqs, tok, dim = nbuf.shape
    group = wbuf.shape[3]
    part = tok // 4
    others = (x_dev, y_dev, mate, x_mate, dg_dev, yn * CORES + 1 - core, dg * CORES + 1 - core)
    greet(others)

    def cols(on_side, on_core):
        return pl.ds(pl.multiple_of((2 * on_side + on_core) * group, group), group)

    def local_w(m):
        return pltpu.make_async_copy(weights[m].at[:, cols(side, core)], wbuf.at[m, me], loc_sem.at[m])

    def own_mate(m):
        return remote(weights[m].at[:, cols(side, 1 - core)], wbuf.at[m, me], m_send.at[m], w_recv.at[m, me], mate)

    def over_x(m):
        return (remote(weights[m].at[:, cols(1 - side, core)], wbuf.at[m, me], a_send.at[m, 0], w_recv.at[m, me], x_dev),
                remote(weights[m].at[:, cols(1 - side, 1 - core)], wmate.at[m, 0], a_send.at[m, 1], wm_recv.at[m, 0], x_dev))

    def over_y(m):
        return (remote(weights[m].at[:, cols(side, core)], wbuf.at[m, me], b_send.at[m, 0], w_recv.at[m, me], y_dev),
                remote(weights[m].at[:, cols(side, 1 - core)], wmate.at[m, 1], b_send.at[m, 1], wm_recv.at[m, 1], y_dev))

    def forward_y(m):
        return (remote(wbuf.at[m, x_dev], wbuf.at[m, x_dev], f_send.at[m, 0], w_recv.at[m, x_dev], y_dev),
                remote(wmate.at[m, 0], wmate.at[m, 2], f_send.at[m, 1], wm_recv.at[m, 2], y_dev))

    def to_mate(m, slot):
        source = (x_dev, y_dev, dg_dev)[slot]
        return remote(wmate.at[m, slot], wbuf.at[m, source], mf_send.at[m, slot], w_recv.at[m, source], mate)

    def landed(m, source):
        remote(wbuf.at[m, source], wbuf.at[m, source], m_send.at[m], w_recv.at[m, source], mate).wait_recv()

    def landed_mate(m, slot):
        to = wmate.at[m, slot]
        remote(to, to, m_send.at[m], wm_recv.at[m, slot], mate).wait_recv()

    def n_copy(slot):
        source, device = (0, 0, 0, 2)[slot], (mate, mate, x_dev, mate)[slot]
        return remote(nbuf.at[source], nbuf.at[slot], n_send.at[slot], n_recv.at[slot], device)

    def id_copy(slot, owner):
        return remote(ids_hbm, ids_buf.at[owner], i_send.at[slot], i_recv.at[owner], others[slot])

    def rows(piece):
        return pl.ds(piece * part, part)

    def wo_x(slot, source, piece, src):
        return remote(src, wfull_hbm.at[source, rows(piece)], ox_send.at[slot], o_recv.at[source, piece], x_dev)

    def wo_y(slot, source, piece, src):
        return remote(src, wfull_hbm.at[source, rows(piece)], oy_send.at[slot], o_recv.at[source, piece], y_dev)

    def wo_mate(order, source, piece, src):
        return remote(src, wfull_hbm.at[source, rows(piece)], od_send.at[order, piece], o_recv.at[source, piece], mate)

    def wo_landed(source, piece):
        to = wfull_hbm.at[source, rows(piece)]
        remote(to, to, od_send.at[0, 0], o_recv.at[source, piece], mate).wait_recv()

    for slot in range(7):
        id_copy(slot, me).start()
    id_own = pltpu.make_async_copy(ids_hbm, ids_buf.at[me], i_own)
    id_own.start()
    start(over_x(0))
    start(over_y(0))
    for m in range(3):
        local_w(m).start()
        own_mate(m).start()
    start(over_y(1))
    wide = tok_ref[...].astype(jnp.float32)
    nbuf[0] = (wide * lax.rsqrt(jnp.mean(wide * wide, axis=-1, keepdims=True) + EPS)).astype(jnp.bfloat16)
    n_copy(2).start()
    n_copy(1).start()
    start(over_x(1))
    start(over_x(2))
    for piece in range(PARTS):
        wo_x(piece, me, piece, wo_hbm.at[rows(piece)]).start()
    for piece in range(PARTS):
        wo_mate(0, me, piece, wo_hbm.at[rows(piece)]).start()
    wo_own = pltpu.make_async_copy(wo_hbm, wfull_hbm.at[me], o_own)
    wo_own.start()

    id_own.wait()
    for slot in range(7):
        id_copy(slot, others[slot]).wait_recv()
    order = lax.broadcasted_iota(jnp.int32, (tok, tok), 0) < lax.broadcasted_iota(jnp.int32, (tok, tok), 1)
    earlier = jnp.where(order, 1.0, 0.0).astype(jnp.bfloat16)
    experts = slots_ref.shape[1]
    spot = lax.broadcasted_iota(jnp.int32, (experts, tok), 0)
    local = experts // 2
    wanted = jnp.where(spot < local, me * local + spot, (mate - 1) * local + spot)

    def table(source, c):
        count = jnp.zeros((experts, tok), jnp.float32)
        for j in range(ids_buf.shape[1]):
            count = count + jnp.where(ids_buf[source, j:j + 1, :] == wanted, 1.0, 0.0)
        before = jnp.dot(count.astype(jnp.bfloat16), earlier, preferred_element_type=jnp.float32)
        slots_ref[source] = jnp.where(count > 0.0, before, -1.0)
        ids_ref[source] = ids_buf[source]
        return c

    lax.fori_loop(0, ids_buf.shape[0], table, 0)

    def arrive_x(m):
        landed(m, x_dev)
        landed_mate(m, 0)
        start(forward_y(m))
        to_mate(m, 0).start()

    def finish(m):
        landed_mate(m, 1)
        to_mate(m, 1).start()
        landed_mate(m, 2)
        to_mate(m, 2).start()
        local_w(m).wait()
        for source in (y_dev, dg_dev, mate, x_mate, yn * CORES + 1 - core, dg * CORES + 1 - core):
            landed(m, source)

    width = 256

    def project(m):
        def run(i, c):
            slot, n = i // (group // width), lax.rem(i, group // width)
            at = pl.ds(pl.multiple_of(n * width, width), width)
            out = jnp.dot(nbuf[slot], wbuf[m, :, :, at].reshape(dim, width), preferred_element_type=jnp.float32)
            qkv[m, slot, :, at] = out.astype(jnp.bfloat16)
            return c

        lax.fori_loop(0, seqs * (group // width), run, 0)

    arrive_x(0)
    start(over_y(2))
    n_copy(2).wait_recv()
    n_copy(3).start()
    finish(0)
    n_copy(1).wait_recv()
    n_copy(3).wait_recv()
    project(0)
    arrive_x(1)
    arrive_x(2)
    for slot, piece in enumerate((3, 0, 1, 2)):
        wo_y(slot, me, piece, wo_hbm.at[rows(piece)]).start()
    finish(1)
    project(1)
    finish(2)
    project(2)

    scale = 128 ** -0.5
    block = tok // 2
    pairs = group // 256

    def c_copy(slot, pair):
        at = pl.ds(pl.multiple_of(pair * 256, 256), 256)
        there = pl.ds(pl.multiple_of((2 * side + core) * group + pair * 256, 256), 256)
        src, dst = cbuf.at[slot, :, at], ctx.at[:, there]
        if slot == 0:
            return pltpu.make_async_copy(src, dst, c_own.at[pair])
        return remote(src, dst, c_send.at[slot - 1, pair], c_recv.at[slot - 1, pair], (mate, x_dev, x_mate)[slot - 1])

    def heads(pair, carry):
        def one_seq(slot, c):
            for h in range(2):
                at = pl.ds(pl.multiple_of(pair * 256 + h * 128, 128), 128)
                keys, values = qkv[1, slot, :, at], qkv[2, slot, :, at]
                for b in range(2):
                    query = qkv[0, slot, b * block:(b + 1) * block, at]
                    span = (b + 1) * block
                    s = lax.dot_general(query, keys[:span], (((1,), (1,)), ((), ())), preferred_element_type=jnp.float32) * scale
                    row = lax.broadcasted_iota(jnp.int32, (block, span), 0) + b * block
                    s = jnp.where(row >= lax.broadcasted_iota(jnp.int32, (block, span), 1), s, -jnp.inf)
                    e = jnp.exp(s - jnp.max(s, axis=-1, keepdims=True))
                    p = (e * (1.0 / jnp.sum(e, axis=-1, keepdims=True))).astype(jnp.bfloat16)
                    cbuf[slot, b * block:(b + 1) * block, at] = jnp.dot(p, values[:span], preferred_element_type=jnp.float32).astype(jnp.bfloat16)
            return c

        lax.fori_loop(0, seqs, one_seq, 0)
        for slot in (2, 3, 1, 0):
            c_copy(slot, pair).start()

        @pl.when(pair == 1)
        def _():
            for piece in range(PARTS):
                wo_landed(x_dev, piece)
                wo_mate(1, x_dev, piece, wfull_hbm.at[x_dev, rows(piece)]).start()
                if piece < 3:
                    wo_y(4 + piece, x_dev, piece, wfull_hbm.at[x_dev, rows(piece)]).start()

        return carry

    lax.fori_loop(0, pairs, heads, 0)
    finish_send(n_copy(slot) for slot in range(1, PARTS))
    total[...] = tok_ref[...].astype(jnp.float32)
    for piece in (3, 0, 1, 2):
        wo_landed(y_dev, piece)
        wo_mate(2, y_dev, piece, wfull_hbm.at[y_dev, rows(piece)]).start()
        if piece == 3:
            wo_x(4, y_dev, piece, wfull_hbm.at[y_dev, rows(piece)]).start()
    for slot in range(1, PARTS):
        for at in strips(group, TILE):
            remote(cbuf.at[0, :, at], ctx.at[:, at], c_send.at[0, 0], c_recv.at[slot - 1, at.start // TILE], mate).wait_recv()
    for pair in range(PARTS):
        c_copy(0, pair).wait()
    wo_own.wait()
    order = (me, x_dev, y_dev, mate, x_mate, yn * CORES + 1 - core, dg_dev, dg * CORES + 1 - core)

    def load(step):
        slot = step % CORES
        return pltpu.make_async_copy(wfull_hbm.at[order[step]], nbuf.at[CORES + slot], ring_sem.at[slot])

    def ready(step):
        if step == 6:
            for piece in range(PARTS):
                wo_landed(dg_dev, piece)
                wo_mate(3, dg_dev, piece, wfull_hbm.at[dg_dev, rows(piece)]).start()
        elif step > 2:
            for piece in range(PARTS):
                wo_landed(order[step], piece)
        load(step).start()

    ready(0)
    for step, source in enumerate(order):
        early = step + 1 < 6
        if early:
            ready(step + 1)
        load(step).wait()
        heads_at = pl.ds(pl.multiple_of(source * wo_hbm.shape[0], wo_hbm.shape[0]), wo_hbm.shape[0])

        def add(n, c, slot=step % CORES, heads_at=heads_at):
            at = pl.ds(pl.multiple_of(n * TILE, TILE), TILE)
            total[:, at] += jnp.dot(ctx[:, heads_at], nbuf[CORES + slot, :, at], preferred_element_type=jnp.float32)
            return c

        lax.fori_loop(0, dim // TILE, add, 0)
        if not early and step + 1 < len(order):
            ready(step + 1)
    nbuf[0] = total[...].astype(jnp.bfloat16)
    h_copy = pltpu.make_async_copy(nbuf.at[0], h_hbm, out_sem.at[0])
    h_copy.start()
    wide = nbuf[0].astype(jnp.float32)
    nbuf[1] = (wide * lax.rsqrt(jnp.mean(wide * wide, axis=-1, keepdims=True) + EPS)).astype(jnp.bfloat16)
    u_copy = pltpu.make_async_copy(nbuf.at[1], u_hbm, out_sem.at[1])
    u_copy.start()
    for slot in range(7):
        id_copy(slot, me).wait_send()
    for m in range(3):
        own_mate(m).wait_send()
        for copy in over_x(m) + over_y(m) + forward_y(m):
            copy.wait_send()
        for slot in range(3):
            to_mate(m, slot).wait_send()
    for pair in range(PARTS):
        finish_send(c_copy(slot, pair) for slot in range(1, PARTS))
    h_copy.wait()
    u_copy.wait()
    for slot in range(5):
        wo_x(slot, me, 0, wo_hbm.at[rows(0)]).wait_send()
    for slot in range(7):
        wo_y(slot, me, 0, wo_hbm.at[rows(0)]).wait_send()
    for order in range(PARTS):
        for piece in range(PARTS):
            wo_mate(order, me, piece, wo_hbm.at[rows(piece)]).wait_send()


def attend(tokens, ids, w_query, w_key, w_value, w_out):
    tok, dim = tokens.shape
    depth, width = w_query.shape
    devices, group = 8, width // 4
    dma = pltpu.SemaphoreType.DMA
    return pl.pallas_call(
        attend_kernel,
        out_shape=(jax.ShapeDtypeStruct((tok, dim), jnp.bfloat16), jax.ShapeDtypeStruct((tok, dim), jnp.bfloat16), jax.ShapeDtypeStruct((devices,) + w_out.shape, jnp.bfloat16), jax.ShapeDtypeStruct((devices, 32, tok), jnp.float32), jax.ShapeDtypeStruct((devices,) + ids.shape, jnp.int32)),
        in_specs=[WHOLE] + [ANY] * 5,
        out_specs=(ANY, ANY, ANY, WHOLE, WHOLE),
        scratch_shapes=[
            pltpu.VMEM((tok, width), jnp.bfloat16), pltpu.VMEM((tok, dim), jnp.float32), dma((2,)), dma((2,)),
            pltpu.VMEM((devices,) + ids.shape, jnp.int32), dma((7,)), dma((devices,)), dma,
            pltpu.VMEM((4, tok, dim), jnp.bfloat16),
            pltpu.VMEM((3, devices, depth, group), jnp.bfloat16),
            pltpu.VMEM((3, 3, depth, group), jnp.bfloat16),
            pltpu.VMEM((3, 4, tok, group), jnp.bfloat16),
            pltpu.VMEM((4, tok, group), jnp.bfloat16),
            dma((3,)), dma((3, 2)), dma((3, 2)), dma((3, 2)), dma((3,)), dma((3, 3)), dma((3, devices)), dma((3, 3)),
            dma((4,)), dma((4,)), dma((3, 4)), dma((3, 4)), dma((4,)),
            dma((5,)), dma((7,)), dma((4, 4)), dma((devices, 4)), dma,
        ],
        compiler_params=pltpu.CompilerParams(collective_id=3, has_side_effects=True, vmem_limit_bytes=VMEM_MAX),
        name='attend_heads',
    )(tokens, ids, w_query, w_key, w_value, w_out)


def spread_kernel(u_hbm, h_ref, router_ref, ids_ref, slot_ref, x_hbm, gall_hbm, g_own, ubuf, hbuf, xbuf, own_sem, gown_sem, out_sem, x_send, y_send, d_send, recv, g_send, g_recv):
    me, core, chip, xn, yn, dg = neighbours()
    mate = me + 1 - 2 * core
    tok = ubuf.shape[1]
    part = tok // 4
    local_experts = slot_ref.shape[1] // 2
    x_dev, y_dev, dg_dev = xn * CORES + core, yn * CORES + core, dg * CORES + core
    others = (x_dev, y_dev, mate, dg_dev, xn * CORES + 1 - core, yn * CORES + 1 - core, dg * CORES + 1 - core)
    greet(others)

    def rows(piece):
        return pl.ds(piece * part, part)

    def landed(source, piece):
        remote(ubuf.at[source, rows(piece)], ubuf.at[source, rows(piece)], d_send.at[0, 0], recv.at[source, piece], mate).wait_recv()

    def pass_on(order, source, piece):
        return remote(ubuf.at[source, rows(piece)], ubuf.at[source, rows(piece)], d_send.at[order, piece], recv.at[source, piece], mate)

    def across_x(slot, source, piece, src):
        return remote(src, ubuf.at[source, rows(piece)], x_send.at[slot], recv.at[source, piece], x_dev)

    def across_y(slot, source, piece, src):
        return remote(src, ubuf.at[source, rows(piece)], y_send.at[slot], recv.at[source, piece], y_dev)

    own = pltpu.make_async_copy(u_hbm, ubuf.at[me], own_sem)
    own.start()
    for slot in range(PARTS):
        across_x(slot, me, slot, u_hbm.at[rows(slot)]).start()
        across_y(slot, me, (slot + 2) % 4, u_hbm.at[rows((slot + 2) % 4)]).start()
    for piece in range(PARTS):
        remote(u_hbm.at[rows(piece)], ubuf.at[me, rows(piece)], d_send.at[0, piece], recv.at[me, piece], mate).start()
    wide = h_ref[...].astype(jnp.float32)
    wide = wide * lax.rsqrt(jnp.mean(wide * wide, axis=-1, keepdims=True) + EPS)
    logits = jnp.dot(wide, router_ref[...], precision=lax.Precision.HIGHEST, preferred_element_type=jnp.float32).T
    expert_at = lax.broadcasted_iota(jnp.int32, logits.shape, 0)
    for j in range(g_own.shape[0]):
        g_own[j:j + 1, :] = jnp.sum(jnp.where(ids_ref[j:j + 1, :] == expert_at, logits, 0.0), axis=0, keepdims=True)
    chosen = g_own[...]
    chosen = jnp.exp(chosen - jnp.max(chosen, axis=0, keepdims=True))
    g_own[...] = chosen / jnp.sum(chosen, axis=0, keepdims=True)
    gown = pltpu.make_async_copy(g_own, gall_hbm.at[me], gown_sem)
    gown.start()
    for slot, device in enumerate(others):
        remote(g_own, gall_hbm.at[me], g_send.at[slot], g_recv.at[me], device).start()
    own.wait()

    def out_copy(order, source):
        return pltpu.make_async_copy(xbuf.at[lax.rem(order, 2)], x_hbm.at[:, source], out_sem.at[lax.rem(order, 2)])

    def step(order, carry):
        kind = order // 2
        base = jnp.where(kind == 0, chip, jnp.where(kind == 1, xn, jnp.where(kind == 2, yn, dg)))
        odd = lax.rem(order, 2)
        source = base * 2 + core + odd * (1 - 2 * core)

        @pl.when(order == 2)
        def _():
            for piece in (0, 1):
                landed(x_dev, piece)
                across_y(4 + piece, x_dev, piece, ubuf.at[x_dev, rows(piece)]).start()
                pass_on(1, x_dev, piece).start()
                landed(y_dev, piece + 2)
                across_x(4 + piece, y_dev, piece + 2, ubuf.at[y_dev, rows(piece + 2)]).start()
                pass_on(2, y_dev, piece + 2).start()
            for piece in (0, 1):
                landed(x_dev, piece + 2)
                pass_on(1, x_dev, piece + 2).start()
                landed(y_dev, piece)
                pass_on(2, y_dev, piece).start()

        @pl.when(order == 6)
        def _():
            for piece in (0, 2, 1, 3):
                landed(dg_dev, piece)
                pass_on(3, dg_dev, piece).start()

        @pl.when(odd == 1)
        def _():
            for piece in range(PARTS):
                landed(source, piece)

        @pl.when(order >= 2)
        def _():
            out_copy(order, source).wait()

        spot = lax.broadcasted_iota(jnp.int32, (CAP, tok), 0).astype(jnp.float32)
        for expert in range(local_experts):
            hit = slot_ref[source, expert:expert + 1, :] == spot
            hbuf[expert * CAP:(expert + 1) * CAP, :] = jnp.where(hit, 1.0, 0.0).astype(jnp.bfloat16)
        width = 4 * TILE

        def tile(n, c):
            cols = pl.ds(pl.multiple_of(n * width, width), width)
            picked = jnp.dot(hbuf[...], ubuf[source, :, cols], preferred_element_type=jnp.float32)
            xbuf[odd, :, :, cols] = picked.astype(jnp.bfloat16).reshape(local_experts, CAP, width)
            return c

        lax.fori_loop(0, ubuf.shape[2] // width, tile, 0)
        out_copy(order, source).start()
        return carry

    lax.fori_loop(0, 8, step, 0)
    out_copy(0, me).wait()
    out_copy(1, me).wait()
    gown.wait()
    for slot in range(PARTS):
        across_x(slot, me, slot, u_hbm.at[rows(slot)]).wait_send()
        across_y(slot, me, slot, u_hbm.at[rows(slot)]).wait_send()
    for piece in (0, 1):
        across_y(4 + piece, x_dev, piece, ubuf.at[x_dev, rows(piece)]).wait_send()
        across_x(4 + piece, y_dev, piece + 2, ubuf.at[y_dev, rows(piece + 2)]).wait_send()
    for order, source in enumerate((me, x_dev, y_dev, dg_dev)):
        for piece in range(PARTS):
            pass_on(order, source, piece).wait_send()
    for slot, device in enumerate(others):
        remote(g_own, gall_hbm.at[me], g_send.at[slot], g_recv.at[me], device).wait_send()
        remote(g_own, gall_hbm.at[device], g_send.at[slot], g_recv.at[device], device).wait_recv()


def spread(u, hidden, w_router, ids, slots):
    devices, pair_experts, tok = slots.shape
    local_experts = pair_experts // 2
    dim = u.shape[1]
    return pl.pallas_call(
        spread_kernel,
        out_shape=(jax.ShapeDtypeStruct((local_experts, devices, CAP, dim), jnp.bfloat16), jax.ShapeDtypeStruct((devices,) + ids.shape, jnp.float32)),
        in_specs=[ANY, WHOLE, WHOLE, WHOLE, WHOLE],
        out_specs=(ANY, ANY),
        scratch_shapes=[
            pltpu.VMEM(ids.shape, jnp.float32),
            pltpu.VMEM((devices, tok, dim), jnp.bfloat16),
            pltpu.VMEM((local_experts * CAP, tok), jnp.bfloat16),
            pltpu.VMEM((2, local_experts, CAP, dim), jnp.bfloat16),
            pltpu.SemaphoreType.DMA, pltpu.SemaphoreType.DMA, pltpu.SemaphoreType.DMA((2,)),
            pltpu.SemaphoreType.DMA((6,)), pltpu.SemaphoreType.DMA((6,)), pltpu.SemaphoreType.DMA((4, 4)),
            pltpu.SemaphoreType.DMA((devices, 4)), pltpu.SemaphoreType.DMA((7,)), pltpu.SemaphoreType.DMA((devices,)),
        ],
        compiler_params=pltpu.CompilerParams(collective_id=1, has_side_effects=True, vmem_limit_bytes=VMEM_MAX),
        name='spread_rows',
    )(u, hidden, w_router, ids, slots)


def ffn_kernel(units_ref, x_ref, w1_hbm, w3_hbm, w2_hbm, o_ref, packed, middle, done, w1_buf, w3_buf, w2_buf, w_sem):
    expert = pl.program_id(0)
    last = pl.num_programs(0)
    devices = x_ref.shape[1]
    depth = w1_buf.shape[0]
    ahead = depth - 1

    def fetch(e):
        slot = lax.rem(e, depth)
        moves = ((w1_hbm, w1_buf), (w3_hbm, w3_buf), (w2_hbm, w2_buf))
        return [pltpu.make_async_copy(src.at[e], dst.at[slot], w_sem.at[slot, i]) for i, (src, dst) in enumerate(moves)]

    @pl.when(expert == 0)
    def _():
        for e in range(ahead):
            start(fetch(e))
        packed[...] = jnp.zeros_like(packed)
        done[...] = jnp.zeros_like(done)

    @pl.when(expert + ahead < last)
    def _():
        start(fetch(expert + ahead))

    begins, counts = [], [units_ref[expert * devices + source] * UNIT for source in range(devices)]
    total = 0
    for source in range(devices):
        begins.append(pl.multiple_of(total, UNIT))
        packed[pl.ds(begins[-1], CAP), :] = x_ref[0, source]
        total = total + counts[source]
    for copy in fetch(expert):
        copy.wait()
    slot = lax.rem(expert, depth)
    small, big = LANES, TILE

    def run(begin, size):
        rows = pl.ds(pl.multiple_of(begin, small), size)
        for at in strips(w1_buf.shape[2], TILE):
            first = jnp.dot(packed[rows, :], w1_buf[slot, :, at], preferred_element_type=jnp.float32)
            third = jnp.dot(packed[rows, :], w3_buf[slot, :, at], preferred_element_type=jnp.float32)
            middle[:size, at] = (first * jax.nn.sigmoid(first) * third).astype(jnp.bfloat16)
        for at in strips(w2_buf.shape[2], 2 * TILE):
            done[rows, at] = jnp.dot(middle[:size], w2_buf[slot, :, at], preferred_element_type=jnp.float32).astype(jnp.bfloat16)

    full = (total + small - 1) // big

    def run_big(t, c):
        run(t * big, big)
        return c

    lax.fori_loop(0, full, run_big, 0)

    @pl.when(full * big < total)
    def _():
        run(full * big, small)

    spot = lax.broadcasted_iota(jnp.int32, (CAP, o_ref.shape[3]), 0)
    for source in range(devices):
        o_ref[0, source] = jnp.where(spot < counts[source], done[pl.ds(begins[source], CAP), :], jnp.zeros((), jnp.bfloat16))


def expert_ffn(units, x, w_one, w_three, w_two):
    experts, devices, _, dim = x.shape
    mid = w_one.shape[2]
    depth = 3
    block = pl.BlockSpec((1, devices, CAP, dim), lambda e, units: (e, 0, 0, 0))
    ring = [pltpu.VMEM((depth,) + w.shape[1:], jnp.bfloat16) for w in (w_one, w_three, w_two)]
    lines = pltpu.VMEM(((devices + 1) * CAP, dim), jnp.bfloat16)
    return pl.pallas_call(
        ffn_kernel,
        out_shape=jax.ShapeDtypeStruct(x.shape, jnp.bfloat16),
        grid_spec=pltpu.PrefetchScalarGridSpec(
            num_scalar_prefetch=1,
            grid=(experts,),
            in_specs=[block] + [ANY] * 3,
            out_specs=block,
            scratch_shapes=[lines, pltpu.VMEM((TILE, mid), jnp.bfloat16), lines] + ring + [pltpu.SemaphoreType.DMA((depth, 3))],
        ),
        compiler_params=pltpu.CompilerParams(dimension_semantics=('arbitrary',), vmem_limit_bytes=VMEM_MAX),
        name='expert_mlp',
    )(units, x, w_one, w_three, w_two)


def combine_kernel(o_hbm, slots_ref, ids_ref, gates_ref, h_hbm, y_ref, own, mate_rows, gate_tab, gate3, p_one, r_one, p_two, r_two, p_last, r_last, own_sem, h_sem, mate_send, mate_recv, one_send, one_recv, two_send, two_recv, last_send, last_recv):
    me, core, chip, xn, yn, dg = neighbours()
    mate = me + 1 - CORES * core
    near = xn + core * (yn - xn)
    far = yn + core * (xn - yn)
    near_dev, far_dev = near * CORES + core, far * CORES + core
    half = own.shape[3]
    rows_n = p_one.shape[1]
    experts = own.shape[1]
    greet((near_dev, far_dev, mate))
    my_cols = pl.ds(pl.multiple_of(core * half, half), half)
    mate_cols = pl.ds(pl.multiple_of((1 - core) * half, half), half)
    spot = lax.broadcasted_iota(jnp.int32, gate_tab.shape, 0)
    wanted = jnp.where(spot < experts, me * experts + spot, (mate - 1) * experts + spot)

    def dest(i, first, second, front):
        pair, odd = i // CORES, lax.rem(i, CORES)
        base = jnp.where(pair == 0, dg, jnp.where(pair == 1, first, jnp.where(pair == 2, second, chip)))
        return base * CORES + jnp.where(pair < 3, odd, front + odd * (1 - CORES * front))

    def my_dest(i):
        return dest(i, near, far, 1 - core)

    def to_mate(i):
        return remote(o_hbm.at[:, dest(i, far, near, core), :, mate_cols], mate_rows.at[i], mate_send.at[i], mate_recv.at[i], mate)

    def own_copy(i):
        slot = lax.rem(i, CORES)
        return pltpu.make_async_copy(o_hbm.at[:, my_dest(i), :, my_cols], own.at[slot], own_sem.at[slot])

    def one_copy(n):
        return remote(p_one.at[n], r_one.at[n], one_send.at[n], one_recv.at[n], near_dev)

    def two_copy(n):
        return remote(p_two.at[n], r_two.at[n], two_send.at[n], two_recv.at[n], far_dev)

    def last_copy(n):
        return remote(p_last.at[n], r_last.at[n], last_send.at[n], last_recv.at[n], mate)

    own_copy(0).start()
    for i in range(8):
        to_mate(i).start()
    residual = pltpu.make_async_copy(h_hbm, y_ref, h_sem)
    residual.start()

    def open_dest(i):
        gate = jnp.zeros(gate_tab.shape, jnp.float32)
        target = my_dest(i)
        for j in range(ids_ref.shape[1]):
            gate = gate + jnp.where(ids_ref[target, j:j + 1, :] == wanted, gates_ref[target, j:j + 1, :], 0.0)
        gate_tab[...] = gate

    def open_rows(i):
        own_copy(i).wait()
        to_mate(i).wait_recv()

        @pl.when(i < 7)
        def _():
            own_copy(i + 1).start()

    def weights(i, part):
        target = my_dest(i)
        cols = pl.ds(pl.multiple_of(part * rows_n, rows_n), rows_n)
        line = lax.broadcasted_iota(jnp.int32, (2 * CAP, rows_n), 0)
        low = line < CAP
        place = (line - jnp.where(low, 0, CAP)).astype(jnp.float32)
        for pair, where in enumerate(strips(gate3.shape[1], 2 * CAP)):
            one, two = slice(2 * pair, 2 * pair + 1), slice(2 * pair + 1, 2 * pair + 2)
            hit = jnp.where(low, slots_ref[target, one, cols], slots_ref[target, two, cols]) == place
            rest = jnp.where(hit, jnp.where(low, gate_tab[one, cols], gate_tab[two, cols]), 0.0).T
            for rows in strips(gate3.shape[0], rows_n):
                term = rest.astype(jnp.bfloat16)
                gate3[rows, where] = term
                rest = rest - term.astype(jnp.float32)

    def products(i, part, sink):
        @pl.when(part == 0)
        def _():
            open_dest(i)

        weights(i, part)

        @pl.when(part == 0)
        def _():
            open_rows(i)

        slot = lax.rem(i, CORES)
        depth = experts * CAP

        wide = CORES * TILE

        def tile(n, c):
            cols = pl.ds(pl.multiple_of(n * wide, wide), wide)
            mine = own[slot, :, :, cols].reshape(depth, wide)
            other = mate_rows[i, :, :, cols].reshape(depth, wide)
            out = jnp.dot(gate3[:, :depth], mine, preferred_element_type=jnp.float32) + jnp.dot(gate3[:, depth:], other, preferred_element_type=jnp.float32)
            sink[:, cols] = sum(out[rows] for rows in strips(out.shape[0], rows_n))
            return c

        lax.fori_loop(0, half // wide, tile, 0)

    lead, pair_n, part_n = p_one.shape[0], p_two.shape[0], p_two.shape[0] // CORES

    def phase_one(step, c):
        products(step // part_n, lax.rem(step, part_n), p_one.at[step])
        one_copy(step).start()
        return c

    lax.fori_loop(0, lead, phase_one, 0)

    def phase_two(step, c):
        products(4 + step // part_n, lax.rem(step, part_n), p_two.at[step])
        one_copy(step).wait_recv()
        p_two[step] = p_two[step] + r_one[step]
        two_copy(step).start()
        return c

    lax.fori_loop(0, pair_n, phase_two, 0)
    residual.wait()

    def phase_three(step, c):
        products(6 + step // part_n, lax.rem(step, part_n), p_last.at[step])
        return c

    lax.fori_loop(0, pair_n, phase_three, 0)

    def close(step, c):
        part = lax.rem(step, part_n)
        n = jnp.where(step < part_n, 1 - core, core) * part_n + part
        one_copy(pair_n + n).wait_recv()
        two_copy(n).wait_recv()
        p_last[step] = p_last[step] + (r_one[pair_n + n] + r_two[n])

        @pl.when(step < part_n)
        def _():
            last_copy(step).start()

        @pl.when(step >= part_n)
        def _():
            rows = pl.ds(pl.multiple_of(part * rows_n, rows_n), rows_n)
            y_ref[rows, my_cols] = (y_ref[rows, my_cols].astype(jnp.float32) + p_last[step]).astype(jnp.bfloat16)

        return c

    lax.fori_loop(0, pair_n, close, 0)
    for n in range(part_n):
        rows = pl.ds(n * rows_n, rows_n)
        last_copy(n).wait_recv()
        y_ref[rows, mate_cols] = (y_ref[rows, mate_cols].astype(jnp.float32) + r_last[n]).astype(jnp.bfloat16)
    finish_send(to_mate(n) for n in range(8))
    finish_send(one_copy(n) for n in range(lead))
    finish_send(two_copy(n) for n in range(pair_n))
    finish_send(last_copy(n) for n in range(part_n))


def combine(done, slots, ids, gates, hidden):
    experts, devices, _, dim = done.shape
    tok = hidden.shape[0]
    half, part = dim // CORES, tok // PARTS
    pair_n = CORES * PARTS
    dma = pltpu.SemaphoreType.DMA
    floats = lambda n: pltpu.VMEM((n, part, half), jnp.float32)
    rows = lambda n: pltpu.VMEM((n, experts, CAP, half), jnp.bfloat16)
    sizes = [CORES * pair_n, CORES * pair_n, pair_n, pair_n, pair_n, PARTS]
    sems = [dma((n,)) for n in (devices, devices, 2 * pair_n, 2 * pair_n, pair_n, pair_n, PARTS, PARTS)]
    return pl.pallas_call(
        combine_kernel,
        out_shape=jax.ShapeDtypeStruct((tok, dim), jnp.bfloat16),
        in_specs=[ANY, WHOLE, WHOLE, WHOLE, ANY],
        out_specs=WHOLE,
        scratch_shapes=[rows(CORES), rows(devices), pltpu.VMEM(slots.shape[1:], jnp.float32), pltpu.VMEM((3 * part, CORES * experts * CAP), jnp.bfloat16)] + [floats(n) for n in sizes] + [dma((CORES,)), dma] + sems,
        compiler_params=pltpu.CompilerParams(collective_id=2, has_side_effects=True, vmem_limit_bytes=VMEM_MAX),
        name='combine_rows',
    )(done, slots, ids, gates, hidden)


def solution(mesh):
    tok_spec = P(('dp', 'ep'))
    row_spec = P('ep')

    def local_layer(tokens, w_query, w_key, w_value, w_out, w_router, w_one, w_three, w_two, expert_ids):
        seq_count, seq_len, model_dim = tokens.shape
        choices = expert_ids.shape[2]
        local_experts = w_one.shape[0]
        tok_count = seq_count * seq_len
        ids_t = expert_ids.reshape(tok_count, choices).T
        flat = tokens.reshape(tok_count, model_dim)
        w_flat = [w.reshape(w.shape[0], -1) for w in (w_query, w_key, w_value)]
        hidden, normed, _, slot, all_ids = attend(flat, ids_t, *w_flat, w_out)
        units = ((jnp.max(slot[:, :local_experts], axis=2).astype(jnp.int32) + UNIT) // UNIT).T.reshape(-1)
        x, all_gates = spread(normed, hidden, w_router, ids_t, slot)
        done = expert_ffn(units, x, w_one, w_three, w_two)
        layer_out = combine(done, slot, all_ids, all_gates, hidden)
        return layer_out.reshape(seq_count, seq_len, model_dim)

    return jax.shard_map(local_layer, mesh=mesh, in_specs=(tok_spec, row_spec, row_spec, row_spec, row_spec, P(), row_spec, row_spec, row_spec, tok_spec), out_specs=tok_spec, check_vma=False)
```
